32 devices in a mesh: dp: 16 (over z, x, core), fsdp: 2 (over y).
Axes of the slice: x: 2, y: 2, z: 4, core: 2. Of those that a mesh axis runs over, the one named last changes fastest.
Arguments:
- hidden: bfloat16 [64, 512, 768], P(('dp', 'fsdp')), may hold values from -7 to 7
- lengths: int32 [64], P(('dp', 'fsdp')), may hold values from 1 to 512, 20480 in all
- in_weight: bfloat16 [768, 1536], P(('dp', 'fsdp')), may hold values from -0.21875 to 0.21875
- depth_kernel: bfloat16 [9, 768], P(None, ('dp', 'fsdp')), may hold values from -2 to 2
- point_weight: bfloat16 [768, 384], P(('dp', 'fsdp')), may hold values from -0.21875 to 0.21875
- kernel_weight: bfloat16 [9, 2304], P(None, ('dp', 'fsdp')), may hold values from -0.3125 to 0.3125
- out_weight: bfloat16 [768, 768], P(('dp', 'fsdp')), may hold values from -0.875 to 0.875
- up_weight: bfloat16 [2, 384, 1536], P(None, None, ('dp', 'fsdp')), may hold values from -0.3125 to 0.3125
- down_weight: bfloat16 [2, 1536, 384], P(None, ('dp', 'fsdp')), may hold values from -0.15625 to 0.15625
- norm_gains: bfloat16 [2, 768], P(None, ('dp', 'fsdp')), may hold values from 0.25 to 1.75
- norm_biases: bfloat16 [2, 768], P(None, ('dp', 'fsdp')), may hold values from -3 to 3
- out_grad: bfloat16 [64, 512, 768], P(('dp', 'fsdp')), may hold values from -6 to 6
Outputs:
- output: bfloat16 [64, 512, 768], P(('dp', 'fsdp'))
- input_grad: bfloat16 [64, 512, 768], P(('dp', 'fsdp'))
- grad_in_weight: float32 [768, 1536], P(('dp', 'fsdp'))
- grad_depth_kernel: float32 [9, 768], P(None, ('dp', 'fsdp'))
- grad_point_weight: float32 [768, 384], P(('dp', 'fsdp'))
- grad_kernel_weight: float32 [9, 2304], P(None, ('dp', 'fsdp'))
- grad_out_weight: float32 [768, 768], P(('dp', 'fsdp'))
- grad_up_weight: float32 [2, 384, 1536], P(None, None, ('dp', 'fsdp'))
- grad_down_weight: float32 [2, 1536, 384], P(None, ('dp', 'fsdp'))
- grad_norm_gains: float32 [2, 768], P(None, ('dp', 'fsdp'))
- grad_norm_biases: float32 [2, 768], P(None, ('dp', 'fsdp'))
- rms: float32 [4], replicated
The draws below stay inside these ranges and needn't reach their ends.
All inputs are finite; a program needn't handle non-finite values. No bound on the sum of `lengths` on one device may be relied on, other than what follows from the above.
Results may differ from the reference program's by a relative error of at most 0.015.
Values may be sent and summed in bfloat16 or wider, within the bound.
A program may use at most 192 MiB of HBM per device.

```python
import math
import jax
import jax.numpy as jnp
import numpy as np
from jax import lax

D = 768
HEADS = 6
HD = 64
FF = 3072
G = 2
K = 9
SEQ = 512
AW = 384
ROWS = 64


def draw_hidden(key, part):
    row_index = jnp.arange(ROWS, dtype=jnp.float32) / max(ROWS - 1, 1)
    row_scale = jnp.exp(0.5 * math.log(3.0) * row_index)[:, None, None]
    base = jax.random.truncated_normal(key, -4.0, 4.0, (ROWS, SEQ, D), jnp.float32)
    return (base * row_scale).astype(jnp.bfloat16)


def levels(key, shape, cuts, least, top_value):
    factor_of = 1.0
    for position, blocks in cuts:
        heights = jax.random.uniform(jax.random.fold_in(jax.random.fold_in(key, 6), position), (blocks,), jnp.float32, least / len(cuts), top_value / len(cuts))
        factor_of = factor_of * jnp.repeat(jnp.exp(heights), shape[position] // blocks).reshape((-1,) + (1,) * (len(shape) - 1 - position))
    return factor_of


def split_up(amount, total, reach, lean):
    loads = [(1 << 20) // math.isqrt(grade ** lean) + 1 for grade in range(2, amount + 1)]
    surplus, holding = total - reach - (amount - 1), [1] * (amount - 1)
    while surplus > 0:
        movable = [i for i in range(amount - 1) if holding[i] < reach]
        whole, left = sum([loads[i] for i in movable]), surplus
        for i in movable:
            addition = min(reach - holding[i], max(1, left * loads[i] // whole), surplus)
            holding[i] = holding[i] + addition
            surplus = surplus - addition
    return np.array([reach] + holding)


def uneven(rng, count, total, limit, lean):
    if count == 2:
        one = jax.random.randint(rng, (), max(1, total - limit), min(limit, total - 1) + 1)
        return jnp.stack([one, total - one])
    sizes = jnp.asarray(split_up(count, total, limit, lean), jnp.int32)
    couples = (count - 1) // 2
    giver, receiver = sizes[1:1 + 2 * couples:2], sizes[2:2 + 2 * couples:2]
    slack = jnp.minimum(giver - 1, limit - receiver)
    passed = jax.random.randint(jax.random.fold_in(rng, 1), (couples,), 0, 1 << 20) % (slack + 1)
    sizes = sizes.at[1:1 + 2 * couples:2].set(giver - passed).at[2:2 + 2 * couples:2].set(receiver + passed)
    return sizes[jax.random.permutation(jax.random.fold_in(rng, 2), count)]


def scatter_about(stream_key, shape, spread, limit, pieces=(), kind=jnp.bfloat16):
    values = jax.random.normal(stream_key, shape, jnp.float32) * spread
    if len(pieces) > 0:
        values = levels(stream_key, shape, pieces, -0.22, 0.18) * values
    return jnp.clip(values, min=-limit, max=limit).astype(kind)


def setup_inputs(seed: int = 0) -> dict:
    streams_of = jax.random.split(jax.random.key(seed), 13)
    hidden = draw_hidden(jax.random.fold_in(streams_of[12], 71), 0)
    lengths = uneven(streams_of[1], ROWS, ROWS * SEQ * 5 // 8, SEQ, 2).astype(jnp.int32)
    in_weight = scatter_about(streams_of[2], (D, 4 * AW), D ** -0.5, 0.21875, ((0, 32),))
    depth_kernel = scatter_about(streams_of[3], (K, D), K ** -0.5, 2.0, ((1, 32),))
    point_weight = scatter_about(streams_of[4], (D, AW), D ** -0.5, 0.21875, ((0, 32),))
    kernel_weight = scatter_about(streams_of[5], (K, AW * HEADS), AW ** -0.5, 0.3125, ((1, 32),))
    out_weight = scatter_about(streams_of[6], (D, D), (D // 16) ** -0.5, 0.875, ((0, 32),))
    up_weight = scatter_about(streams_of[7], (G, D // G, FF // G), (D // G) ** -0.5, 0.3125, ((2, 32),))
    down_weight = scatter_about(streams_of[8], (G, FF // G, D // G), (FF // G) ** -0.5, 0.15625, ((1, 32),))
    norm_gains = jnp.clip(1.0 + 0.15 * jax.random.normal(streams_of[9], (2, D), jnp.float32), 0.25, 1.75).astype(jnp.bfloat16)
    norm_biases = scatter_about(streams_of[10], (2, D), 0.5, 3.0, ((1, 32),))
    out_grad = scatter_about(streams_of[11], (ROWS, SEQ, D), 1.0, 6.0, ((0, 32),))
    return dict(hidden=hidden, lengths=lengths, in_weight=in_weight, depth_kernel=depth_kernel, point_weight=point_weight, kernel_weight=kernel_weight, out_weight=out_weight, up_weight=up_weight, down_weight=down_weight, norm_gains=norm_gains, norm_biases=norm_biases, out_grad=out_grad)


@jax.custom_vjp
def low(v):
    return lax.optimization_barrier(v.astype(jnp.bfloat16)).astype(jnp.float32)

@jax.custom_vjp
def low_back(v):
    return v

def low_keep(v):
    return (low(v), None)

def low_pass(kept, grad):
    return (grad,)

def back_keep(v):
    return (v, None)

def back_low(kept, grad):
    return (low(grad),)
low.defvjp(low_keep, low_pass)
low_back.defvjp(back_keep, back_low)
HIGHEST = lax.Precision.HIGHEST
EPSILON = 1e-06

def normalize(values, gain, bias):
    average = lax.optimization_barrier(jnp.mean(values, axis=-1, keepdims=True))
    centered = values - average
    variance = lax.optimization_barrier(jnp.mean(centered * centered, axis=-1, keepdims=True))
    return centered * lax.rsqrt(variance + EPSILON) * gain + bias

def activation(values):
    return jax.nn.gelu(values, approximate=False)

def padded_seq(values):
    border = K // 2
    return jnp.pad(values, ((0, 0), (border, border), (0, 0)))

def forward(hidden_f, lengths, in_weight, depth_kernel, point_weight, kernel_weight, out_weight, up_weight, down_weight, norm_gains, norm_biases):
    row_count = hidden_f.shape[0]
    att_width = HEADS * HD
    positions = jnp.arange(SEQ, dtype=jnp.int32)
    valid_mask = (positions[None, :] < lengths[:, None]).astype(jnp.float32)
    inputs = hidden_f * valid_mask[:, :, None]
    projected = low(low_back(jnp.einsum('rtd,de->rte', inputs, in_weight, precision=HIGHEST)))
    query = projected[:, :, :att_width]
    key_part = projected[:, :, att_width:2 * att_width]
    value_part = projected[:, :, 2 * att_width:3 * att_width]
    span_value = projected[:, :, 3 * att_width:]
    padded_in = padded_seq(inputs)
    depthwise = jnp.zeros_like(inputs)
    for offset in range(K):
        depthwise = depthwise + padded_in[:, offset:offset + SEQ] * depth_kernel[offset]
    key_conv = low_back(jnp.einsum('rtd,de->rte', low(depthwise), point_weight, precision=HIGHEST))
    mixed_key = low(key_conv * query)
    kernel_matrix = jnp.transpose(kernel_weight.reshape(K, att_width, HEADS), (1, 2, 0)).reshape(att_width, HEADS * K)
    logits = low_back(jnp.einsum('rtc,ce->rte', mixed_key, kernel_matrix, precision=HIGHEST))
    span_weights = jax.nn.softmax(logits.reshape(row_count, SEQ, HEADS, K), axis=-1)
    padded_value = padded_seq(span_value).reshape(row_count, SEQ + 2 * (K // 2), HEADS, HD)
    conv_out = jnp.zeros((row_count, SEQ, HEADS, HD), jnp.float32)
    for offset in range(K):
        conv_out = conv_out + span_weights[:, :, :, offset:offset + 1] * padded_value[:, offset:offset + SEQ]
    queries = query.reshape(row_count, SEQ, HEADS, HD)
    keys_all = key_part.reshape(row_count, SEQ, HEADS, HD)
    values_all = value_part.reshape(row_count, SEQ, HEADS, HD)
    scores = low_back(jnp.einsum('rqhe,rkhe->rhqk', queries, keys_all, precision=HIGHEST) * (1.0 / math.sqrt(HD)))
    scores = jnp.where(valid_mask[:, None, None, :] > 0.5, scores, -1e+30)
    attn_probs = low(jax.nn.softmax(scores, axis=-1))
    attended = jnp.einsum('rhqk,rkhe->rqhe', attn_probs, values_all, precision=HIGHEST)
    context = low(low_back(jnp.concatenate([attended.reshape(row_count, SEQ, att_width), conv_out.reshape(row_count, SEQ, att_width)], axis=-1)))
    mixer_out = low_back(jnp.einsum('rtc,cd->rtd', context, out_weight, precision=HIGHEST))
    first = normalize(inputs + mixer_out, norm_gains[0], norm_biases[0])
    grouped = low(first).reshape(row_count, SEQ, G, D // G)
    pre_act = low_back(jnp.einsum('rtgi,gij->rtgj', grouped, up_weight, precision=HIGHEST))
    activated = low(activation(pre_act))
    ffn_out = low_back(jnp.einsum('rtgj,gjo->rtgo', activated, down_weight, precision=HIGHEST).reshape(row_count, SEQ, D))
    layer_y = normalize(first + ffn_out, norm_gains[1], norm_biases[1]) * valid_mask[:, :, None]
    return (layer_y, (inputs, mixer_out, ffn_out, valid_mask))

def reference(hidden, lengths, in_weight, depth_kernel, point_weight, kernel_weight, out_weight, up_weight, down_weight, norm_gains, norm_biases, out_grad):
    params = tuple((weight.astype(jnp.float32) for weight in (in_weight, depth_kernel, point_weight, kernel_weight, out_weight, up_weight, down_weight, norm_gains, norm_biases)))
    row_count = hidden.shape[0]
    group_rows = math.gcd(row_count, max(1, 4096 // SEQ))
    step_count = row_count // group_rows
    hidden_groups = hidden.reshape(step_count, group_rows, SEQ, D)
    length_groups = lengths.reshape(step_count, group_rows)
    grad_groups = out_grad.reshape(step_count, group_rows, SEQ, D)

    def one_group(carry, block):
        grad_sums, square_sums, count_sum = carry
        hidden_block, length_block, cotangent = block

        def local_forward(hidden_f, *weights):
            return forward(hidden_f, length_block, *weights)
        layer_y, pullback, extras = jax.vjp(local_forward, hidden_block.astype(jnp.float32), *params, has_aux=True)
        pulled = pullback(cotangent.astype(jnp.float32))
        inputs, mixer_out, ffn_out, valid_mask = extras
        weight_mask = valid_mask[:, :, None]
        squares = jnp.stack([jnp.sum(inputs * inputs), jnp.sum(weight_mask * mixer_out * mixer_out), jnp.sum(weight_mask * ffn_out * ffn_out), jnp.sum(layer_y * layer_y)])
        new_sums = tuple((total + extra for total, extra in zip(grad_sums, pulled[1:])))
        return ((new_sums, square_sums + squares, count_sum + jnp.sum(valid_mask)), (layer_y.astype(jnp.bfloat16), pulled[0].astype(jnp.bfloat16)))
    start = (tuple((jnp.zeros(weight.shape, jnp.float32) for weight in params)), jnp.zeros((4,), jnp.float32), jnp.zeros((), jnp.float32))
    final, stacked = lax.scan(one_group, start, (hidden_groups, length_groups, grad_groups))
    grad_sums, square_sums, count_sum = final
    outputs, input_grads = stacked
    rms = jnp.sqrt(square_sums / (count_sum * D))
    return (outputs.reshape(row_count, SEQ, D), input_grads.reshape(row_count, SEQ, D), grad_sums[0], grad_sums[1], grad_sums[2], grad_sums[3], grad_sums[4], grad_sums[5], grad_sums[6], grad_sums[7], grad_sums[8], rms)
```

```python
import functools
import math

import jax
import jax.numpy as jnp
from jax import lax
from jax.experimental import pallas as pl
from jax.experimental.pallas import tpu as pltpu
from jax.sharding import PartitionSpec as P

D = 768
HEADS = 6
HD = 64
G = 2
K = 9
SEQ = 512


EPSILON = 1e-06


def product(left_op, right_op):
    return jnp.dot(left_op, right_op, preferred_element_type=jnp.float32)


def product_tn(left_op, right_op):
    return lax.dot_general(
        left_op, right_op, (((0,), (0,)), ((), ())), preferred_element_type=jnp.float32
    )


def product_nt(left_op, right_op):
    return lax.dot_general(
        left_op, right_op, (((1,), (1,)), ((), ())), preferred_element_type=jnp.float32
    )


def layer_norm(values, gain, bias):
    average = jnp.mean(values, axis=-1, keepdims=True)
    centered = values - average
    variance = jnp.mean(centered * centered, axis=-1, keepdims=True)
    inverse = lax.rsqrt(variance + EPSILON)
    normed = centered * inverse
    return (normed * gain + bias, normed, inverse)


def norm_backward(grad_in, normed, inverse, gain):
    scaled = grad_in * gain
    return inverse * (
        scaled
        - jnp.mean(scaled, axis=-1, keepdims=True)
        - normed * jnp.mean(scaled * normed, axis=-1, keepdims=True)
    )


def activation(values):
    return jax.nn.gelu(values, approximate=False)


def pad_rows(values, before, after):
    return jnp.pad(values, ((0, 0), (before, after)) + ((0, 0),) * (values.ndim - 2))


MESH = pl.DeviceIdType.MESH
BLOCKS = 16
HALF = BLOCKS // 2


def place():
    dp, y = lax.axis_index("dp"), lax.axis_index("fsdp")
    return dp, dp // 4, (dp // 2) % 2, dp % 2, y


def partners(dp, x, core, y):
    return (dp + 1 - 2 * core, y), (dp + 2 - 4 * x, y), (dp, 1 - y)


def meet(peers, others):
    barrier = pltpu.get_barrier_semaphore()
    for peer in peers:
        pl.semaphore_signal(barrier, inc=1, device_id=peer, device_id_type=MESH)
    count = len(peers)
    for there, peer in others:

        @pl.when(there)
        def _():
            pl.semaphore_signal(barrier, inc=1, device_id=peer, device_id_type=MESH)

        count = count + there.astype(jnp.int32)
    pl.semaphore_wait(barrier, count)


def send(src, dst, send_sem, recv_sem, device):
    return pltpu.make_async_remote_copy(
        src_ref=src,
        dst_ref=dst,
        send_sem=send_sem,
        recv_sem=recv_sem,
        device_id=device,
        device_id_type=MESH,
    )


def gather_kernel(
    depth, p_ref, g_ref, own_sem, zs, zr, xs, xr, ys, yr, ds, dr, cs, cr
):
    dp, z, x, core, y = place()
    c_dev, x_dev, y_dev = partners(dp, x, core, y)
    up_dev, down_dev = (dp + 4, y), (dp - 4, y)
    own = pltpu.make_async_copy(p_ref, g_ref.at[:, z, x, core, y], own_sem)
    own.start()
    meet((c_dev, x_dev, y_dev), ((z + 1 < depth, up_dev), (z > 0, down_dev)))
    own.wait()
    steps = 2 * depth - 1

    def target(q):
        return z + ((q + 1) // 2) * (1 - 2 * (q % 2))

    def z_copy(j, way, device):
        slab = g_ref.at[:, j, x, core, y]
        return send(slab, slab, zs.at[way, j], zr.at[j], device)

    def x_copy(j):
        slab = g_ref.at[:, j, x, core, y]
        return send(slab, slab, xs.at[j], xr.at[j], x_dev)

    def y_copy(j):
        slab = g_ref.at[:, j, x, core, y]
        return send(slab, slab, ys.at[j], yr.at[j], y_dev)

    def d_copy(j, half):
        if half == 0:
            slab = g_ref.at[pl.ds(0, HALF), j, 1 - x, core, y]
            return send(slab, slab, ds.at[0, j], dr.at[0, j], y_dev)
        slab = g_ref.at[pl.ds(HALF, HALF), j, x, core, 1 - y]
        return send(slab, slab, ds.at[1, j], dr.at[1, j], x_dev)

    def c_copy(j, a, b):
        slab = g_ref.at[:, j, (x + a) % 2, core, (y + b) % 2]
        return send(slab, slab, cs.at[2 * a + b, j], cr.at[2 * a + b, j], c_dev)

    def c_arrival(j, a, b):
        slab = g_ref.at[:, j, (x + a) % 2, 1 - core, (y + b) % 2]
        return send(slab, slab, cs.at[2 * a + b, j], cr.at[2 * a + b, j], c_dev)

    def x_arrival(j):
        slab = g_ref.at[:, j, 1 - x, core, y]
        return send(slab, slab, xs.at[j], xr.at[j], x_dev)

    def y_arrival(j):
        slab = g_ref.at[:, j, x, core, 1 - y]
        return send(slab, slab, ys.at[j], yr.at[j], y_dev)

    def d_arrival(j, half):
        slab = g_ref.at[pl.ds(half * HALF, HALF), j, 1 - x, core, 1 - y]
        return send(slab, slab, ds.at[half, j], dr.at[half, j], y_dev if half == 0 else x_dev)

    def first(j):
        @pl.when(j != z)
        def _():
            z_copy(j, 0, up_dev).wait_recv()

        @pl.when((j <= z) & (z + 1 < depth))
        def _():
            z_copy(j, 0, up_dev).start()

        @pl.when((j >= z) & (z > 0))
        def _():
            z_copy(j, 1, down_dev).start()

        x_copy(j).start()
        y_copy(j).start()
        c_copy(j, 0, 0).start()

    def second(j):
        x_arrival(j).wait_recv()
        d_copy(j, 0).start()
        c_copy(j, 1, 0).start()
        y_arrival(j).wait_recv()
        d_copy(j, 1).start()
        c_copy(j, 0, 1).start()

    def third(j):
        d_arrival(j, 0).wait_recv()
        d_arrival(j, 1).wait_recv()
        c_copy(j, 1, 1).start()

    def stage(q, work):
        j = target(q)

        @pl.when((q >= 0) & (q < steps) & (j >= 0) & (j < depth))
        def _():
            work(j)

    def step(q, carry):
        stage(q, first)
        stage(q - 1, second)
        stage(q - 2, third)
        return carry

    lax.fori_loop(0, steps + 2, step, 0)

    def finish(j, carry):
        for a in range(2):
            for b in range(2):
                c_arrival(j, a, b).wait_recv()
                c_copy(j, a, b).wait_send()
        x_copy(j).wait_send()
        y_copy(j).wait_send()
        d_copy(j, 0).wait_send()
        d_copy(j, 1).wait_send()

        @pl.when((j <= z) & (z + 1 < depth))
        def _():
            z_copy(j, 0, up_dev).wait_send()

        @pl.when((j >= z) & (z > 0))
        def _():
            z_copy(j, 1, down_dev).wait_send()

        return carry

    lax.fori_loop(0, depth, finish, 0)


def gather_all(packed, mesh):
    dp, fsdp = mesh.shape["dp"], mesh.shape["fsdp"]
    _, rows, width = packed.shape
    if fsdp != 2 or dp % 4:
        full = lax.all_gather(packed, ("dp", "fsdp"), axis=1, tiled=False)
        return full.reshape(BLOCKS, dp * fsdp * rows, width)
    depth = dp // 4
    dma = pltpu.SemaphoreType.DMA
    full = pl.pallas_call(
        functools.partial(gather_kernel, depth),
        out_shape=jax.ShapeDtypeStruct((BLOCKS, depth, 2, 2, 2, rows, width), packed.dtype),
        in_specs=[pl.BlockSpec(memory_space=pltpu.VMEM)],
        out_specs=pl.BlockSpec(memory_space=pl.ANY),
        scratch_shapes=[
            dma(()),
            dma((2, depth)),
            dma((depth,)),
            dma((depth,)),
            dma((depth,)),
            dma((depth,)),
            dma((depth,)),
            dma((2, depth)),
            dma((2, depth)),
            dma((4, depth)),
            dma((4, depth)),
        ],
        compiler_params=pltpu.CompilerParams(collective_id=0, has_side_effects=True),
        name="gather_all",
    )(packed)
    return full.reshape(BLOCKS, dp * fsdp * rows, width)


def scatter_kernel(
    depth,
    l_ref,
    t_ref,
    o_ref,
    u_ref,
    acc,
    rc,
    ry1,
    rx1,
    rx2,
    ry2,
    rup,
    rdn,
    tiny,
    got,
    load_sem,
    cs,
    cr,
    ss,
    sr,
    zs,
    zr,
    ts,
    tr,
):
    dp, z, x, core, y = place()
    c_dev, x_dev, y_dev = partners(dp, x, core, y)
    up_dev, down_dev = (dp + 4, y), (dp - 4, y)
    steps = 2 * depth - 1
    bf16, f32 = jnp.bfloat16, jnp.float32

    def target(q):
        return z + (depth - 1 - q // 2) * (1 - 2 * (q % 2))

    def valid(q):
        j = target(q)
        return (q >= 0) & (q < steps) & (j >= 0) & (j < depth)

    def load(j):
        return pltpu.make_async_copy(l_ref.at[:, j, :, core, :], acc.at[j], load_sem.at[j])

    def c_copy(j):
        return send(l_ref.at[:, j, :, 1 - core, :], rc.at[j], cs.at[j], cr.at[j], c_dev)

    def y1_copy(j):
        return send(acc.at[j, pl.ds(0, HALF), :, 1 - y], ry1.at[j], ss.at[0, j], sr.at[0, j], y_dev)

    def x1_copy(j):
        return send(acc.at[j, pl.ds(HALF, HALF), 1 - x], rx1.at[j], ss.at[1, j], sr.at[1, j], x_dev)

    def x2_copy(j):
        return send(acc.at[j, pl.ds(0, HALF), 1 - x, y], rx2.at[j], ss.at[2, j], sr.at[2, j], x_dev)

    def y2_copy(j):
        return send(acc.at[j, pl.ds(HALF, HALF), x, 1 - y], ry2.at[j], ss.at[3, j], sr.at[3, j], y_dev)

    def up_copy(j):
        return send(acc.at[j, :, x, y], rup.at[j], zs.at[j], zr.at[0, j], up_dev)

    def down_copy(j):
        return send(acc.at[j, :, x, y], rdn.at[j], zs.at[j], zr.at[1, j], down_dev)

    def issue(q, carry):
        @pl.when(valid(q))
        def _():
            load(target(q)).start()

        return carry

    lax.fori_loop(0, steps, issue, 0)
    lines = tuple((z >= d, (dp - 4 * d, y)) for d in range(1, depth)) + tuple(
        (z + d < depth, (dp + 4 * d, y)) for d in range(1, depth)
    )
    meet((c_dev, x_dev, y_dev), lines)

    def issue_core(q, carry):
        @pl.when(valid(q))
        def _():
            c_copy(target(q)).start()

        return carry

    lax.fori_loop(0, steps, issue_core, 0)

    tiny[0] = t_ref[...]

    def t_copy(k):
        return send(tiny.at[k], got.at[k], ts.at[k], tr.at[k], (c_dev, x_dev, y_dev)[k])

    def t_line(d, way):
        return send(
            tiny.at[3],
            got.at[3 + z],
            ts.at[2 + d if way > 0 else 1 + depth + d],
            tr.at[3 + z],
            (dp + 4 * d * way, y),
        )

    def t_arrival(level):
        return send(tiny.at[3], got.at[3 + level], ts.at[0], tr.at[3 + level], c_dev)

    t_copy(0).start()

    def add(into, other):
        return (into.astype(f32) + other.astype(f32)).astype(bf16)

    def first(j):
        load(j).wait()
        c_copy(j).wait_recv()

        def block(b, carry):
            acc[j, b] = add(acc[j, b], rc[j, b])
            return carry

        lax.fori_loop(0, BLOCKS, block, 0)
        y1_copy(j).start()
        x1_copy(j).start()

    def second(j):
        y1_copy(j).wait_recv()

        def low(b, carry):
            for a in range(2):
                acc[j, b, a, y] = add(acc[j, b, a, y], ry1[j, b, a])
            return carry

        lax.fori_loop(0, HALF, low, 0)
        x2_copy(j).start()
        x1_copy(j).wait_recv()

        def high(b, carry):
            for a in range(2):
                acc[j, HALF + b, x, a] = add(acc[j, HALF + b, x, a], rx1[j, b, a])
            return carry

        lax.fori_loop(0, HALF, high, 0)
        y2_copy(j).start()

    def third(j):
        x2_copy(j).wait_recv()
        y2_copy(j).wait_recv()

        @pl.when((j >= z) & (z > 0))
        def _():
            up_copy(j).wait_recv()

        @pl.when((j <= z) & (z + 1 < depth))
        def _():
            down_copy(j).wait_recv()

        def block(b, carry):
            for part, other in ((0, rx2), (HALF, ry2)):
                total = acc[j, part + b, x, y].astype(f32) + other[j, b].astype(f32)

                @pl.when(j == z)
                def _():
                    o_ref[part + b] = total

                @pl.when(j != z)
                def _():
                    acc[j, part + b, x, y] = total.astype(bf16)

            return carry

        lax.fori_loop(0, HALF, block, 0)

        def more(ref, low_precision):
            def block(b, carry):
                if low_precision:
                    acc[j, b, x, y] = add(acc[j, b, x, y], ref[j, b])
                else:
                    o_ref[b] = o_ref[b] + ref[j, b].astype(f32)
                return carry

            lax.fori_loop(0, BLOCKS, block, 0)

        @pl.when((j > z) & (z > 0))
        def _():
            more(rup, True)

        @pl.when((j < z) & (z + 1 < depth))
        def _():
            more(rdn, True)

        @pl.when((j == z) & (z > 0))
        def _():
            more(rup, False)

        @pl.when((j == z) & (z + 1 < depth))
        def _():
            more(rdn, False)

        @pl.when(j > z)
        def _():
            up_copy(j).start()

        @pl.when(j < z)
        def _():
            down_copy(j).start()

    def stage(q, work):
        @pl.when(valid(q))
        def _():
            work(target(q))

    def step(q, carry):
        stage(q, first)
        stage(q - 1, second)
        stage(q - 2, third)
        return carry

    lax.fori_loop(0, steps + 2, step, 0)

    for k in range(3):
        t_copy(k).wait_recv()
        tiny[k + 1] = tiny[k] + got[k]
        if k < 2:
            t_copy(k + 1).start()
    for d in range(1, depth):

        @pl.when(z + d < depth)
        def _():
            t_line(d, 1).start()

        @pl.when(z >= d)
        def _():
            t_line(d, -1).start()

    for level in range(depth):

        @pl.when(z == level)
        def _():
            got[3 + level] = tiny[3]

        @pl.when(z != level)
        def _():
            t_arrival(level).wait_recv()

    total = got[3]
    for level in range(1, depth):
        total = total + got[3 + level]
    u_ref[...] = total

    for d in range(1, depth):

        @pl.when(z + d < depth)
        def _():
            t_line(d, 1).wait_send()

        @pl.when(z >= d)
        def _():
            t_line(d, -1).wait_send()

    for k in range(3):
        t_copy(k).wait_send()

    def finish(j, carry):
        c_copy(j).wait_send()
        y1_copy(j).wait_send()
        x1_copy(j).wait_send()
        x2_copy(j).wait_send()
        y2_copy(j).wait_send()

        @pl.when(j > z)
        def _():
            up_copy(j).wait_send()

        @pl.when(j < z)
        def _():
            down_copy(j).wait_send()

        return carry

    lax.fori_loop(0, depth, finish, 0)


def scatter_all(local, tiny, mesh):
    dp, fsdp = mesh.shape["dp"], mesh.shape["fsdp"]
    _, total, width = local.shape
    rows = total // (dp * fsdp)
    if fsdp != 2 or dp % 4:
        shard = lax.psum_scatter(
            local.reshape(BLOCKS, dp * fsdp, rows, width),
            ("dp", "fsdp"),
            scatter_dimension=1,
            tiled=False,
        )
        return shard.astype(jnp.float32), lax.psum(tiny, ("dp", "fsdp"))
    depth = dp // 4
    dma = pltpu.SemaphoreType.DMA
    bf16 = jnp.bfloat16
    return pl.pallas_call(
        functools.partial(scatter_kernel, depth),
        out_shape=(
            jax.ShapeDtypeStruct((BLOCKS, rows, width), jnp.float32),
            jax.ShapeDtypeStruct((8, 128), jnp.float32),
        ),
        in_specs=[pl.BlockSpec(memory_space=pl.ANY), pl.BlockSpec(memory_space=pltpu.VMEM)],
        out_specs=(
            pl.BlockSpec(memory_space=pltpu.VMEM),
            pl.BlockSpec(memory_space=pltpu.VMEM),
        ),
        scratch_shapes=[
            pltpu.VMEM((depth, BLOCKS, 2, 2, rows, width), bf16),
            pltpu.VMEM((depth, BLOCKS, 2, 2, rows, width), bf16),
            pltpu.VMEM((depth, HALF, 2, rows, width), bf16),
            pltpu.VMEM((depth, HALF, 2, rows, width), bf16),
            pltpu.VMEM((depth, HALF, rows, width), bf16),
            pltpu.VMEM((depth, HALF, rows, width), bf16),
            pltpu.VMEM((depth, BLOCKS, rows, width), bf16),
            pltpu.VMEM((depth, BLOCKS, rows, width), bf16),
            pltpu.VMEM((4, 8, 128), jnp.float32),
            pltpu.VMEM((3 + depth, 8, 128), jnp.float32),
            dma((depth,)),
            dma((depth,)),
            dma((depth,)),
            dma((4, depth)),
            dma((4, depth)),
            dma((depth,)),
            dma((2, depth)),
            dma((1 + 2 * depth,)),
            dma((3 + depth,)),
        ],
        compiler_params=pltpu.CompilerParams(
            collective_id=1, has_side_effects=True, vmem_limit_bytes=60 * 1024 * 1024
        ),
        name="scatter_all",
    )(local.reshape(BLOCKS, depth, 2, 2, 2, rows, width), tiny)


def pack(in_weight, depth_kernel, point_weight, kernel_weight, out_weight, up_weight, down_weight, norm_gains, norm_biases):
    rows = in_weight.shape[0]
    width = D // G

    def halves(grouped):
        return grouped.reshape(G * 2, rows, width)

    kernel = kernel_weight.reshape(K, rows, 3).transpose(1, 0, 2).reshape(rows, 3 * K)
    small = jnp.concatenate([depth_kernel.T, kernel, norm_gains.T, norm_biases.T], axis=1)
    small = jnp.pad(small, ((0, 0), (0, width - small.shape[1])))
    return jnp.concatenate(
        [
            in_weight.reshape(rows, 4, width).transpose(1, 0, 2),
            point_weight[None],
            out_weight.reshape(rows, 2, width).transpose(1, 0, 2),
            halves(down_weight),
            halves(up_weight.transpose(0, 2, 1)),
            small[None],
        ],
        axis=0,
    )


def unpack(shard):
    rows, width = shard.shape[1], shard.shape[2]
    small = shard[15]
    kernel = small[:, K : 4 * K].reshape(rows, K, 3).transpose(1, 0, 2).reshape(K, 3 * rows)
    return (
        shard[0:4].transpose(1, 0, 2).reshape(rows, 4 * width),
        small[:, :K].T,
        shard[4],
        kernel,
        shard[5:7].transpose(1, 0, 2).reshape(rows, 2 * width),
        shard[11:15].reshape(G, 2 * rows, width).transpose(0, 2, 1),
        shard[7:11].reshape(G, 2 * rows, width),
        small[:, 4 * K : 4 * K + 2].T,
        small[:, 4 * K + 2 : 4 * K + 4].T,
    )


def body(
    mesh,
    hidden,
    lengths,
    in_weight,
    depth_kernel,
    point_weight,
    kernel_weight,
    out_weight,
    up_weight,
    down_weight,
    norm_gains,
    norm_biases,
    out_grad,
):
    full = gather_all(
        pack(
            in_weight,
            depth_kernel,
            point_weight,
            kernel_weight,
            out_weight,
            up_weight,
            down_weight,
            norm_gains,
            norm_biases,
        ),
        mesh,
    )
    small = full[15]
    in_full = full[0:4].transpose(1, 0, 2).reshape(D, 4 * (D // G))
    depth_full = small[:, :K].T
    point_full = full[4]
    kernel_full = small[:, K : 4 * K].reshape(D, K, 3).transpose(1, 0, 2).reshape(K, 3 * D)
    out_full = full[5:7].transpose(1, 0, 2).reshape(D, D)
    down_full = full[7:11].reshape(G, 4 * (D // G) , D // G)
    up_full = full[11:15].reshape(G, 4 * (D // G), D // G)
    gains_full = small[:, 4 * K : 4 * K + 2].T.astype(jnp.float32)
    biases_full = small[:, 4 * K + 2 : 4 * K + 4].T.astype(jnp.float32)
    row_count = hidden.shape[0]
    tokens = row_count * SEQ
    att_width = HEADS * HD
    half_span = K // 2
    score_scale = 1.0 / math.sqrt(HD)
    positions = jnp.arange(SEQ, dtype=jnp.int32)
    valid_mask = positions[None, :] < lengths[:, None]
    mask_flat = valid_mask.reshape(tokens, 1).astype(jnp.float32)
    inputs = jnp.where(valid_mask[:, :, None], hidden, jnp.zeros_like(hidden))
    flat_in = inputs.reshape(tokens, D)
    projected = product(flat_in, in_full).astype(jnp.bfloat16)
    padded_in = pad_rows(inputs, half_span, half_span)
    depth_weights = depth_full.astype(jnp.float32)
    depthwise = jnp.zeros((row_count, SEQ, D), jnp.float32)
    for offset in range(K):
        depthwise = (
            depthwise
            + padded_in[:, offset : offset + SEQ].astype(jnp.float32) * depth_weights[offset]
        )
    depth_low = depthwise.reshape(tokens, D).astype(jnp.bfloat16)
    key_conv = product(depth_low, point_full)
    query_f = projected[:, :att_width].astype(jnp.float32)
    mixed_key = (key_conv * query_f).astype(jnp.bfloat16)
    kernel_matrix = jnp.transpose(kernel_full.reshape(K, att_width, HEADS), (1, 2, 0)).reshape(
        att_width, HEADS * K
    )
    logits = product(mixed_key, kernel_matrix).reshape(row_count, SEQ, HEADS, K)
    span_weights = jax.nn.softmax(logits, axis=-1)
    padded_value = pad_rows(
        projected[:, 3 * att_width :].reshape(row_count, SEQ, HEADS, HD), half_span, half_span
    )
    conv_out = jnp.zeros((row_count, SEQ, HEADS, HD), jnp.float32)
    for offset in range(K):
        conv_out = conv_out + span_weights[:, :, :, offset : offset + 1] * padded_value[
            :, offset : offset + SEQ
        ].astype(jnp.float32)
    heads_all = projected[:, : 3 * att_width].reshape(row_count, SEQ, 3, HEADS, HD)

    def row_scores(row_qkv, row_valid):
        scores = (
            jnp.einsum(
                "qhe,khe->hqk", row_qkv[:, 0], row_qkv[:, 1], preferred_element_type=jnp.float32
            )
            * score_scale
        )
        return jnp.where(row_valid[None, None, :], scores, -1e30)

    def attend(row_input):
        row_qkv, row_valid = row_input
        scores = row_scores(row_qkv, row_valid)
        row_peak = jnp.max(scores, axis=-1, keepdims=True)
        exponent = jnp.exp(scores - row_peak)
        row_total = jnp.sum(exponent, axis=-1, keepdims=True)
        attn_probs = (exponent / row_total).astype(jnp.bfloat16)
        result = jnp.einsum(
            "hqk,khe->qhe", attn_probs, row_qkv[:, 2], preferred_element_type=jnp.float32
        )
        return (result, row_peak + jnp.log(row_total))

    attended, log_sums = lax.map(attend, (heads_all, valid_mask))
    context = jnp.concatenate(
        [attended.reshape(tokens, att_width), conv_out.reshape(tokens, att_width)], axis=-1
    ).astype(jnp.bfloat16)
    mixer_out = product(context, out_full)
    inputs_f = flat_in.astype(jnp.float32)
    first, normed_one, inverse_one = layer_norm(inputs_f + mixer_out, gains_full[0], biases_full[0])
    grouped = first.astype(jnp.bfloat16).reshape(tokens, G, D // G)
    pre_act = jnp.einsum("tgi,gji->tgj", grouped, up_full, preferred_element_type=jnp.float32)
    activated = activation(pre_act).astype(jnp.bfloat16)
    ffn_out = jnp.einsum(
        "tgj,gjo->tgo", activated, down_full, preferred_element_type=jnp.float32
    ).reshape(tokens, D)
    second, normed_two, inverse_two = layer_norm(first + ffn_out, gains_full[1], biases_full[1])
    layer_y = second * mask_flat
    squares = jnp.stack(
        [
            jnp.sum(inputs_f * inputs_f),
            jnp.sum(mask_flat * mixer_out * mixer_out),
            jnp.sum(mask_flat * ffn_out * ffn_out),
            jnp.sum(layer_y * layer_y),
        ]
    )
    valid_count = jnp.sum(mask_flat)
    in_back, depth_back, point_back, out_back = in_full, depth_full.astype(jnp.float32), point_full, out_full
    kernel_back, up_back, down_back, gains_back = kernel_matrix, up_full, down_full, gains_full
    grad_layer = out_grad.reshape(tokens, D).astype(jnp.float32) * mask_flat
    gain_grad_two = jnp.sum(grad_layer * normed_two, axis=0)
    bias_grad_two = jnp.sum(grad_layer, axis=0)
    grad_res_two = norm_backward(grad_layer, normed_two, inverse_two, gains_back[1])
    grad_ffn = grad_res_two.astype(jnp.bfloat16).reshape(tokens, G, D // G)
    grad_down = jnp.einsum("tgj,tgo->gjo", activated, grad_ffn, preferred_element_type=jnp.float32)
    grad_act = jnp.einsum("tgo,gjo->tgj", grad_ffn, down_back, preferred_element_type=jnp.float32)
    act_value, act_pull = jax.vjp(activation, pre_act)
    grad_pre = act_pull(grad_act)[0].astype(jnp.bfloat16)
    grad_up = jnp.einsum("tgj,tgi->gji", grad_pre, grouped, preferred_element_type=jnp.float32)
    grad_first = grad_res_two + jnp.einsum(
        "tgj,gji->tgi", grad_pre, up_back, preferred_element_type=jnp.float32
    ).reshape(tokens, D)
    gain_grad_one = jnp.sum(grad_first * normed_one, axis=0)
    bias_grad_one = jnp.sum(grad_first, axis=0)
    grad_res_one = norm_backward(grad_first, normed_one, inverse_one, gains_back[0])
    grad_mixer = grad_res_one.astype(jnp.bfloat16)
    grad_out_w = product_tn(context, grad_mixer)
    grad_context = product_nt(grad_mixer, out_back).astype(jnp.bfloat16)
    grad_conv = grad_context[:, att_width:].reshape(row_count, SEQ, HEADS, HD).astype(jnp.float32)
    span_grads = []
    grad_value_pad = jnp.zeros((row_count, SEQ + 2 * half_span, HEADS, HD), jnp.float32)
    for offset in range(K):
        window = padded_value[:, offset : offset + SEQ].astype(jnp.float32)
        span_grads.append(jnp.sum(grad_conv * window, axis=-1))
        grad_value_pad = grad_value_pad + pad_rows(
            span_weights[:, :, :, offset : offset + 1] * grad_conv, offset, 2 * half_span - offset
        )
    grad_spans = jnp.stack(span_grads, axis=-1)
    grad_value = grad_value_pad[:, half_span : half_span + SEQ].reshape(tokens, att_width)
    grad_logits = (
        (span_weights * (grad_spans - jnp.sum(span_weights * grad_spans, axis=-1, keepdims=True)))
        .reshape(tokens, HEADS * K)
        .astype(jnp.bfloat16)
    )
    grad_kernel_mat = product_tn(mixed_key, grad_logits)
    grad_kernel = jnp.transpose(grad_kernel_mat.reshape(att_width, HEADS, K), (2, 0, 1)).reshape(
        K, att_width * HEADS
    )
    grad_mixed = product_nt(grad_logits, kernel_back)
    grad_key_conv = (grad_mixed * query_f).astype(jnp.bfloat16)
    grad_query_conv = grad_mixed * key_conv
    grad_point = product_tn(depth_low, grad_key_conv)
    grad_depthwise = product_nt(grad_key_conv, point_back).reshape(row_count, SEQ, D)
    kernel_grads = []
    grad_input_pad = jnp.zeros((row_count, SEQ + 2 * half_span, D), jnp.float32)
    for offset in range(K):
        window_in = padded_in[:, offset : offset + SEQ].astype(jnp.float32)
        kernel_grads.append(jnp.sum(window_in * grad_depthwise, axis=(0, 1)))
        grad_input_pad = grad_input_pad + pad_rows(
            grad_depthwise * depth_back[offset], offset, 2 * half_span - offset
        )
    grad_depth_k = jnp.stack(kernel_grads, axis=0)
    grad_input_conv = grad_input_pad[:, half_span : half_span + SEQ].reshape(tokens, D)

    def attend_back(row_input):
        row_qkv, row_valid, row_lse, row_grad = row_input
        scores = row_scores(row_qkv, row_valid)
        probs_f = jnp.exp(scores - row_lse)
        grad_probs = jnp.einsum(
            "qhe,khe->hqk", row_grad, row_qkv[:, 2], preferred_element_type=jnp.float32
        )
        correction = jnp.sum(probs_f * grad_probs, axis=-1, keepdims=True)
        grad_scores = (probs_f * (grad_probs - correction)).astype(jnp.bfloat16)
        grad_query = (
            jnp.einsum(
                "hqk,khe->qhe", grad_scores, row_qkv[:, 1], preferred_element_type=jnp.float32
            )
            * score_scale
        )
        grad_key = (
            jnp.einsum(
                "hqk,qhe->khe", grad_scores, row_qkv[:, 0], preferred_element_type=jnp.float32
            )
            * score_scale
        )
        grad_value_att = jnp.einsum(
            "hqk,qhe->khe",
            probs_f.astype(jnp.bfloat16),
            row_grad,
            preferred_element_type=jnp.float32,
        )
        return jnp.stack([grad_query, grad_key, grad_value_att], axis=1)

    grad_heads = lax.map(
        attend_back,
        (
            heads_all,
            valid_mask,
            log_sums,
            grad_context[:, :att_width].reshape(row_count, SEQ, HEADS, HD),
        ),
    )
    grad_qkv = grad_heads.reshape(tokens, 3 * att_width)
    grad_projected = jnp.concatenate(
        [grad_qkv[:, :att_width] + grad_query_conv, grad_qkv[:, att_width:], grad_value], axis=-1
    ).astype(jnp.bfloat16)
    grad_in_w = product_tn(flat_in, grad_projected)
    grad_inputs = grad_res_one + product_nt(grad_projected, in_back) + grad_input_conv
    input_grad = (grad_inputs * mask_flat).reshape(row_count, SEQ, D).astype(jnp.bfloat16)
    grad_gains = jnp.stack([gain_grad_one, gain_grad_two], axis=0)
    grad_biases = jnp.stack([bias_grad_one, bias_grad_two], axis=0)
    low = jnp.bfloat16
    width = D // G
    grad_small = jnp.concatenate(
        [
            grad_depth_k.T,
            grad_kernel.reshape(K, D, 3).transpose(1, 0, 2).reshape(D, 3 * K),
            grad_gains.T,
            grad_biases.T,
        ],
        axis=1,
    )
    grad_small = jnp.pad(grad_small, ((0, 0), (0, width - grad_small.shape[1])))
    local = jnp.concatenate(
        [
            grad_in_w.reshape(D, 4, width).transpose(1, 0, 2).astype(low),
            grad_point[None].astype(low),
            grad_out_w.reshape(D, 2, width).transpose(1, 0, 2).astype(low),
            grad_down.reshape(4, D, width).astype(low),
            grad_up.reshape(4, D, width).astype(low),
            grad_small[None].astype(low),
        ],
        axis=0,
    )
    sums = jnp.concatenate([squares, valid_count[None]])
    tiny = jnp.broadcast_to(jnp.pad(sums, (0, 123))[None], (8, 128))
    shard, totals = scatter_all(local, tiny, mesh)
    rms = jnp.sqrt(totals[0, :4] / (totals[0, 4] * D))
    summed = unpack(shard)
    output = layer_y.reshape(row_count, SEQ, D).astype(jnp.bfloat16)
    return (
        output,
        input_grad,
        summed[0],
        summed[1],
        summed[2],
        summed[3],
        summed[4],
        summed[5],
        summed[6],
        summed[7],
        summed[8],
        rms,
    )


def solution(mesh):
    in_specs = (
        P(("dp", "fsdp"), None, None),
        P(("dp", "fsdp")),
        P(("dp", "fsdp"), None),
        P(None, ("dp", "fsdp")),
        P(("dp", "fsdp"), None),
        P(None, ("dp", "fsdp")),
        P(("dp", "fsdp"), None),
        P(None, None, ("dp", "fsdp")),
        P(None, ("dp", "fsdp"), None),
        P(None, ("dp", "fsdp")),
        P(None, ("dp", "fsdp")),
        P(("dp", "fsdp"), None, None),
    )
    out_specs = (
        P(("dp", "fsdp"), None, None),
        P(("dp", "fsdp"), None, None),
        P(("dp", "fsdp"), None),
        P(None, ("dp", "fsdp")),
        P(("dp", "fsdp"), None),
        P(None, ("dp", "fsdp")),
        P(("dp", "fsdp"), None),
        P(None, None, ("dp", "fsdp")),
        P(None, ("dp", "fsdp"), None),
        P(None, ("dp", "fsdp")),
        P(None, ("dp", "fsdp")),
        P(),
    )
    return jax.shard_map(functools.partial(body, mesh), mesh=mesh, in_specs=in_specs, out_specs=out_specs, check_vma=False)
```

```python
import functools
import math

import jax
import jax.numpy as jnp
from jax import lax
from jax.experimental import pallas as pl
from jax.experimental.pallas import tpu as pltpu
from jax.sharding import PartitionSpec as P

D = 768
HEADS = 6
HD = 64
G = 2
K = 9
SEQ = 512


EPSILON = 1e-06
MESH = pl.DeviceIdType.MESH
BLOCKS = 16
HALF = BLOCKS // 2


def place():
    dp, y = lax.axis_index("dp"), lax.axis_index("fsdp")
    return dp, dp // 4, (dp // 2) % 2, dp % 2, y


def partners(dp, x, core, y):
    return (dp + 1 - 2 * core, y), (dp + 2 - 4 * x, y), (dp, 1 - y)


def meet(peers, others):
    barrier = pltpu.get_barrier_semaphore()
    for peer in peers:
        pl.semaphore_signal(barrier, inc=1, device_id=peer, device_id_type=MESH)
    count = len(peers)
    for there, peer in others:

        @pl.when(there)
        def _():
            pl.semaphore_signal(barrier, inc=1, device_id=peer, device_id_type=MESH)

        count = count + there.astype(jnp.int32)
    pl.semaphore_wait(barrier, count)


def send(src, dst, send_sem, recv_sem, device):
    return pltpu.make_async_remote_copy(
        src_ref=src,
        dst_ref=dst,
        send_sem=send_sem,
        recv_sem=recv_sem,
        device_id=device,
        device_id_type=MESH,
    )


def gather_kernel(
    depth, p_ref, g_ref, own_sem, zs, zr, xs, xr, ys, yr, ds, dr, cs, cr
):
    dp, z, x, core, y = place()
    c_dev, x_dev, y_dev = partners(dp, x, core, y)
    up_dev, down_dev = (dp + 4, y), (dp - 4, y)
    own = pltpu.make_async_copy(p_ref, g_ref.at[:, z, x, core, y], own_sem)
    own.start()
    meet((c_dev, x_dev, y_dev), ((z + 1 < depth, up_dev), (z > 0, down_dev)))
    own.wait()
    steps = 2 * depth - 1

    def target(q):
        return z + ((q + 1) // 2) * (1 - 2 * (q % 2))

    def z_copy(j, way, device):
        slab = g_ref.at[:, j, x, core, y]
        return send(slab, slab, zs.at[way, j], zr.at[j], device)

    def x_copy(j):
        slab = g_ref.at[:, j, x, core, y]
        return send(slab, slab, xs.at[j], xr.at[j], x_dev)

    def y_copy(j):
        slab = g_ref.at[:, j, x, core, y]
        return send(slab, slab, ys.at[j], yr.at[j], y_dev)

    def d_copy(j, half):
        if half == 0:
            slab = g_ref.at[pl.ds(0, HALF), j, 1 - x, core, y]
            return send(slab, slab, ds.at[0, j], dr.at[0, j], y_dev)
        slab = g_ref.at[pl.ds(HALF, HALF), j, x, core, 1 - y]
        return send(slab, slab, ds.at[1, j], dr.at[1, j], x_dev)

    def c_copy(j, a, b):
        slab = g_ref.at[:, j, (x + a) % 2, core, (y + b) % 2]
        return send(slab, slab, cs.at[2 * a + b, j], cr.at[2 * a + b, j], c_dev)

    def c_arrival(j, a, b):
        slab = g_ref.at[:, j, (x + a) % 2, 1 - core, (y + b) % 2]
        return send(slab, slab, cs.at[2 * a + b, j], cr.at[2 * a + b, j], c_dev)

    def x_arrival(j):
        slab = g_ref.at[:, j, 1 - x, core, y]
        return send(slab, slab, xs.at[j], xr.at[j], x_dev)

    def y_arrival(j):
        slab = g_ref.at[:, j, x, core, 1 - y]
        return send(slab, slab, ys.at[j], yr.at[j], y_dev)

    def d_arrival(j, half):
        slab = g_ref.at[pl.ds(half * HALF, HALF), j, 1 - x, core, 1 - y]
        return send(slab, slab, ds.at[half, j], dr.at[half, j], y_dev if half == 0 else x_dev)

    def first(j):
        @pl.when(j != z)
        def _():
            z_copy(j, 0, up_dev).wait_recv()

        @pl.when((j <= z) & (z + 1 < depth))
        def _():
            z_copy(j, 0, up_dev).start()

        @pl.when((j >= z) & (z > 0))
        def _():
            z_copy(j, 1, down_dev).start()

        x_copy(j).start()
        y_copy(j).start()
        c_copy(j, 0, 0).start()

    def second(j):
        x_arrival(j).wait_recv()
        d_copy(j, 0).start()
        c_copy(j, 1, 0).start()
        y_arrival(j).wait_recv()
        d_copy(j, 1).start()
        c_copy(j, 0, 1).start()

    def third(j):
        d_arrival(j, 0).wait_recv()
        d_arrival(j, 1).wait_recv()
        c_copy(j, 1, 1).start()

    def stage(q, work):
        j = target(q)

        @pl.when((q >= 0) & (q < steps) & (j >= 0) & (j < depth))
        def _():
            work(j)

    def step(q, carry):
        stage(q, first)
        stage(q - 1, second)
        stage(q - 2, third)
        return carry

    lax.fori_loop(0, steps + 2, step, 0)

    def finish(j, carry):
        for a in range(2):
            for b in range(2):
                c_arrival(j, a, b).wait_recv()
                c_copy(j, a, b).wait_send()
        x_copy(j).wait_send()
        y_copy(j).wait_send()
        d_copy(j, 0).wait_send()
        d_copy(j, 1).wait_send()

        @pl.when((j <= z) & (z + 1 < depth))
        def _():
            z_copy(j, 0, up_dev).wait_send()

        @pl.when((j >= z) & (z > 0))
        def _():
            z_copy(j, 1, down_dev).wait_send()

        return carry

    lax.fori_loop(0, depth, finish, 0)


def gather_all(packed, mesh):
    dp, fsdp = mesh.shape["dp"], mesh.shape["fsdp"]
    _, rows, width = packed.shape
    if fsdp != 2 or dp % 4:
        full = lax.all_gather(packed, ("dp", "fsdp"), axis=1, tiled=False)
        return full.reshape(BLOCKS, dp * fsdp * rows, width)
    depth = dp // 4
    dma = pltpu.SemaphoreType.DMA
    full = pl.pallas_call(
        functools.partial(gather_kernel, depth),
        out_shape=jax.ShapeDtypeStruct((BLOCKS, depth, 2, 2, 2, rows, width), packed.dtype),
        in_specs=[pl.BlockSpec(memory_space=pltpu.VMEM)],
        out_specs=pl.BlockSpec(memory_space=pl.ANY),
        scratch_shapes=[
            dma(()),
            dma((2, depth)),
            dma((depth,)),
            dma((depth,)),
            dma((depth,)),
            dma((depth,)),
            dma((depth,)),
            dma((2, depth)),
            dma((2, depth)),
            dma((4, depth)),
            dma((4, depth)),
        ],
        compiler_params=pltpu.CompilerParams(collective_id=0, has_side_effects=True),
        name="gather_all",
    )(packed)
    return full.reshape(BLOCKS, dp * fsdp * rows, width)


def scatter_kernel(
    depth,
    l_ref,
    t_ref,
    o_ref,
    u_ref,
    acc,
    rc,
    ry1,
    rx1,
    rx2,
    ry2,
    rup,
    rdn,
    tiny,
    got,
    load_sem,
    cs,
    cr,
    ss,
    sr,
    zs,
    zr,
    ts,
    tr,
):
    dp, z, x, core, y = place()
    c_dev, x_dev, y_dev = partners(dp, x, core, y)
    up_dev, down_dev = (dp + 4, y), (dp - 4, y)
    steps = 2 * depth - 1
    bf16, f32 = jnp.bfloat16, jnp.float32

    def target(q):
        return z + (depth - 1 - q // 2) * (1 - 2 * (q % 2))

    def valid(q):
        j = target(q)
        return (q >= 0) & (q < steps) & (j >= 0) & (j < depth)

    def load(j):
        return pltpu.make_async_copy(l_ref.at[:, j, :, core, :], acc.at[j], load_sem.at[j])

    def c_copy(j):
        return send(l_ref.at[:, j, :, 1 - core, :], rc.at[j], cs.at[j], cr.at[j], c_dev)

    def y1_copy(j):
        return send(acc.at[j, pl.ds(0, HALF), :, 1 - y], ry1.at[j], ss.at[0, j], sr.at[0, j], y_dev)

    def x1_copy(j):
        return send(acc.at[j, pl.ds(HALF, HALF), 1 - x], rx1.at[j], ss.at[1, j], sr.at[1, j], x_dev)

    def x2_copy(j):
        return send(acc.at[j, pl.ds(0, HALF), 1 - x, y], rx2.at[j], ss.at[2, j], sr.at[2, j], x_dev)

    def y2_copy(j):
        return send(acc.at[j, pl.ds(HALF, HALF), x, 1 - y], ry2.at[j], ss.at[3, j], sr.at[3, j], y_dev)

    def up_copy(j):
        return send(acc.at[j, :, x, y], rup.at[j], zs.at[j], zr.at[0, j], up_dev)

    def down_copy(j):
        return send(acc.at[j, :, x, y], rdn.at[j], zs.at[j], zr.at[1, j], down_dev)

    def issue(q, carry):
        @pl.when(valid(q))
        def _():
            load(target(q)).start()

        return carry

    lax.fori_loop(0, steps, issue, 0)
    lines = tuple((z >= d, (dp - 4 * d, y)) for d in range(1, depth)) + tuple(
        (z + d < depth, (dp + 4 * d, y)) for d in range(1, depth)
    )
    meet((c_dev, x_dev, y_dev), lines)

    def issue_core(q, carry):
        @pl.when(valid(q))
        def _():
            c_copy(target(q)).start()

        return carry

    lax.fori_loop(0, steps, issue_core, 0)

    tiny[0] = t_ref[...]

    def t_copy(k):
        return send(tiny.at[k], got.at[k], ts.at[k], tr.at[k], (c_dev, x_dev, y_dev)[k])

    def t_line(d, way):
        return send(
            tiny.at[3],
            got.at[3 + z],
            ts.at[2 + d if way > 0 else 1 + depth + d],
            tr.at[3 + z],
            (dp + 4 * d * way, y),
        )

    def t_arrival(level):
        return send(tiny.at[3], got.at[3 + level], ts.at[0], tr.at[3 + level], c_dev)

    t_copy(0).start()

    def add(into, other):
        return (into.astype(f32) + other.astype(f32)).astype(bf16)

    def first(j):
        load(j).wait()
        c_copy(j).wait_recv()

        def block(b, carry):
            acc[j, b] = add(acc[j, b], rc[j, b])
            return carry

        lax.fori_loop(0, BLOCKS, block, 0)
        y1_copy(j).start()
        x1_copy(j).start()

    def second(j):
        y1_copy(j).wait_recv()

        def low(b, carry):
            for a in range(2):
                acc[j, b, a, y] = add(acc[j, b, a, y], ry1[j, b, a])
            return carry

        lax.fori_loop(0, HALF, low, 0)
        x2_copy(j).start()
        x1_copy(j).wait_recv()

        def high(b, carry):
            for a in range(2):
                acc[j, HALF + b, x, a] = add(acc[j, HALF + b, x, a], rx1[j, b, a])
            return carry

        lax.fori_loop(0, HALF, high, 0)
        y2_copy(j).start()

    def third(j):
        x2_copy(j).wait_recv()
        y2_copy(j).wait_recv()

        @pl.when((j >= z) & (z > 0))
        def _():
            up_copy(j).wait_recv()

        @pl.when((j <= z) & (z + 1 < depth))
        def _():
            down_copy(j).wait_recv()

        def block(b, carry):
            for part, other in ((0, rx2), (HALF, ry2)):
                total = acc[j, part + b, x, y].astype(f32) + other[j, b].astype(f32)

                @pl.when(j == z)
                def _():
                    o_ref[part + b] = total

                @pl.when(j != z)
                def _():
                    acc[j, part + b, x, y] = total.astype(bf16)

            return carry

        lax.fori_loop(0, HALF, block, 0)

        def more(ref, low_precision):
            def block(b, carry):
                if low_precision:
                    acc[j, b, x, y] = add(acc[j, b, x, y], ref[j, b])
                else:
                    o_ref[b] = o_ref[b] + ref[j, b].astype(f32)
                return carry

            lax.fori_loop(0, BLOCKS, block, 0)

        @pl.when((j > z) & (z > 0))
        def _():
            more(rup, True)

        @pl.when((j < z) & (z + 1 < depth))
        def _():
            more(rdn, True)

        @pl.when((j == z) & (z > 0))
        def _():
            more(rup, False)

        @pl.when((j == z) & (z + 1 < depth))
        def _():
            more(rdn, False)

        @pl.when(j > z)
        def _():
            up_copy(j).start()

        @pl.when(j < z)
        def _():
            down_copy(j).start()

    def stage(q, work):
        @pl.when(valid(q))
        def _():
            work(target(q))

    def step(q, carry):
        stage(q, first)
        stage(q - 1, second)
        stage(q - 2, third)
        return carry

    lax.fori_loop(0, steps + 2, step, 0)

    for k in range(3):
        t_copy(k).wait_recv()
        tiny[k + 1] = tiny[k] + got[k]
        if k < 2:
            t_copy(k + 1).start()
    for d in range(1, depth):

        @pl.when(z + d < depth)
        def _():
            t_line(d, 1).start()

        @pl.when(z >= d)
        def _():
            t_line(d, -1).start()

    for level in range(depth):

        @pl.when(z == level)
        def _():
            got[3 + level] = tiny[3]

        @pl.when(z != level)
        def _():
            t_arrival(level).wait_recv()

    total = got[3]
    for level in range(1, depth):
        total = total + got[3 + level]
    u_ref[...] = total

    for d in range(1, depth):

        @pl.when(z + d < depth)
        def _():
            t_line(d, 1).wait_send()

        @pl.when(z >= d)
        def _():
            t_line(d, -1).wait_send()

    for k in range(3):
        t_copy(k).wait_send()

    def finish(j, carry):
        c_copy(j).wait_send()
        y1_copy(j).wait_send()
        x1_copy(j).wait_send()
        x2_copy(j).wait_send()
        y2_copy(j).wait_send()

        @pl.when(j > z)
        def _():
            up_copy(j).wait_send()

        @pl.when(j < z)
        def _():
            down_copy(j).wait_send()

        return carry

    lax.fori_loop(0, depth, finish, 0)


def scatter_all(local, tiny, mesh):
    dp, fsdp = mesh.shape["dp"], mesh.shape["fsdp"]
    _, total, width = local.shape
    rows = total // (dp * fsdp)
    if fsdp != 2 or dp % 4:
        shard = lax.psum_scatter(
            local.reshape(BLOCKS, dp * fsdp, rows, width),
            ("dp", "fsdp"),
            scatter_dimension=1,
            tiled=False,
        )
        return shard.astype(jnp.float32), lax.psum(tiny, ("dp", "fsdp"))
    depth = dp // 4
    dma = pltpu.SemaphoreType.DMA
    bf16 = jnp.bfloat16
    return pl.pallas_call(
        functools.partial(scatter_kernel, depth),
        out_shape=(
            jax.ShapeDtypeStruct((BLOCKS, rows, width), jnp.float32),
            jax.ShapeDtypeStruct((8, 128), jnp.float32),
        ),
        in_specs=[pl.BlockSpec(memory_space=pl.ANY), pl.BlockSpec(memory_space=pltpu.VMEM)],
        out_specs=(
            pl.BlockSpec(memory_space=pltpu.VMEM),
            pl.BlockSpec(memory_space=pltpu.VMEM),
        ),
        scratch_shapes=[
            pltpu.VMEM((depth, BLOCKS, 2, 2, rows, width), bf16),
            pltpu.VMEM((depth, BLOCKS, 2, 2, rows, width), bf16),
            pltpu.VMEM((depth, HALF, 2, rows, width), bf16),
            pltpu.VMEM((depth, HALF, 2, rows, width), bf16),
            pltpu.VMEM((depth, HALF, rows, width), bf16),
            pltpu.VMEM((depth, HALF, rows, width), bf16),
            pltpu.VMEM((depth, BLOCKS, rows, width), bf16),
            pltpu.VMEM((depth, BLOCKS, rows, width), bf16),
            pltpu.VMEM((4, 8, 128), jnp.float32),
            pltpu.VMEM((3 + depth, 8, 128), jnp.float32),
            dma((depth,)),
            dma((depth,)),
            dma((depth,)),
            dma((4, depth)),
            dma((4, depth)),
            dma((depth,)),
            dma((2, depth)),
            dma((1 + 2 * depth,)),
            dma((3 + depth,)),
        ],
        compiler_params=pltpu.CompilerParams(
            collective_id=1, has_side_effects=True, vmem_limit_bytes=60 * 1024 * 1024
        ),
        name="scatter_all",
    )(local.reshape(BLOCKS, depth, 2, 2, 2, rows, width), tiny)


W = D // G
F32, BF16 = jnp.float32, jnp.bfloat16
PAD = 8


def nn(a, b):
    return lax.dot_general(a, b, (((1,), (0,)), ((), ())), preferred_element_type=F32)


def nt(a, b):
    return lax.dot_general(a, b, (((1,), (1,)), ((), ())), preferred_element_type=F32)


def tn(a, b):
    return lax.dot_general(a, b, (((0,), (0,)), ((), ())), preferred_element_type=F32)


def spread(rows):
    head = lax.broadcasted_iota(jnp.int32, (rows, W), 0) % 8
    channel = lax.broadcasted_iota(jnp.int32, (rows, W), 1) // HD
    return (head == channel).astype(F32).astype(BF16)


def forward_kernel(
    len_ref,
    hid_ref,
    win_ref,
    wpt_ref,
    depth_ref,
    kmt_ref,
    x_ref,
    proj_ref,
    dl_ref,
    kc_ref,
    wt_ref,
    lse_ref,
    ctx_ref,
    xs,
    sv,
    ot,
):
    length = len_ref[pl.program_id(0)]
    inside = lax.broadcasted_iota(jnp.int32, (SEQ, 1), 0) < length
    x = jnp.where(inside, hid_ref[0], jnp.zeros((), BF16))
    x_ref[0] = x
    xs[0:PAD] = jnp.zeros((PAD, D), F32)
    xs[PAD + SEQ :] = jnp.zeros((PAD, D), F32)
    xs[PAD : PAD + SEQ] = x.astype(F32)
    sv[0:PAD] = jnp.zeros((PAD, W), F32)
    sv[PAD + SEQ :] = jnp.zeros((PAD, W), F32)

    for b in range(4):
        part = nn(x_ref[0], win_ref[b]).astype(BF16)
        proj_ref[0, :, b * W : (b + 1) * W] = part
        if b == 3:
            sv[PAD : PAD + SEQ] = part.astype(F32)

    def column(c, carry):
        lane = pl.ds(pl.multiple_of(c * 128, 128), 128)
        for r in range(8):
            total = jnp.zeros((64, 128), F32)
            for k in range(K):
                start = PAD + r * 64 + k - K // 2
                total = total + xs[start : start + 64, lane] * depth_ref[k : k + 1, lane]
            dl_ref[0, r * 64 : (r + 1) * 64, lane] = total.astype(BF16)
        return carry

    lax.fori_loop(0, D // 128, column, 0)
    kc_ref[0] = nn(dl_ref[0], wpt_ref[0])
    mk = (kc_ref[0] * proj_ref[0, :, 0:W].astype(F32)).astype(BF16)
    logits = nt(kmt_ref[...], mk)
    top = logits[0:8]
    for k in range(1, K):
        top = jnp.maximum(top, logits[k * 8 : k * 8 + 8])
    parts = [jnp.exp(logits[k * 8 : k * 8 + 8] - top) for k in range(K)]
    inverse = 1.0 / sum(parts)
    both = []
    for k in range(K):
        weight = parts[k] * inverse
        wt_ref[0, k * 8 : k * 8 + 8] = weight
        high = weight.astype(BF16).astype(F32)
        both.append(jnp.concatenate([high, weight - high], axis=0).astype(BF16))
    e16 = spread(16)
    for r in range(4):
        total = jnp.zeros((128, W), F32)
        for k in range(K):
            start = PAD + r * 128 + k - K // 2
            total = total + tn(both[k][:, r * 128 : (r + 1) * 128], e16) * sv[start : start + 128]
        ctx_ref[0, r * 128 : (r + 1) * 128, W:] = total.astype(BF16)

    lane_head = lax.broadcasted_iota(jnp.int32, (1, 128), 1) // HD
    bias = jnp.where(inside, 0.0, -1e30).astype(F32)

    def pair(p, carry):
        def slab(part):
            return proj_ref[0, :, pl.ds(pl.multiple_of(part * W + p * 128, 128), 128)]

        q2, k2, v2 = slab(0), slab(1), slab(2)
        for h in range(2):
            scale = jnp.where(lane_head == h, 1.0 / math.sqrt(HD), 0.0).astype(BF16)
            scores = nt(k2, q2 * scale) + bias
            peak = jnp.max(scores, axis=0, keepdims=True)
            power = jnp.exp(scores - peak)
            total = jnp.sum(power, axis=0, keepdims=True)
            lse_ref[0, pl.ds(p * 2 + h, 1)] = peak + jnp.log(total)
            probs = (power * (1.0 / total)).astype(BF16)
            ot[h * HD : (h + 1) * HD] = tn(v2, probs)[h * HD : (h + 1) * HD]
        ctx_ref[0, :, pl.ds(pl.multiple_of(p * 128, 128), 128)] = ot[...].T.astype(BF16)
        return carry

    lax.fori_loop(0, HEADS // 2, pair, 0)


def forward(lengths, hidden, full, depth, kmt):
    rows = hidden.shape[0]

    def per_row(*shape):
        return pl.BlockSpec((1,) + shape, lambda r: (r, 0, 0))

    def out(dtype, *shape):
        return jax.ShapeDtypeStruct((rows,) + shape, dtype)

    return pl.pallas_call(
        forward_kernel,
        grid=(rows,),
        out_shape=(
            out(BF16, SEQ, D),
            out(BF16, SEQ, 4 * W),
            out(BF16, SEQ, D),
            out(F32, SEQ, W),
            out(F32, 8 * K, SEQ),
            out(F32, 8, SEQ),
            out(BF16, SEQ, D),
        ),
        in_specs=[
            pl.BlockSpec(memory_space=pltpu.SMEM),
            per_row(SEQ, D),
            pl.BlockSpec((4, D, W), lambda r: (0, 0, 0)),
            pl.BlockSpec((1, D, W), lambda r: (14, 0, 0)),
            pl.BlockSpec((16, D), lambda r: (0, 0)),
            pl.BlockSpec((8 * K, W), lambda r: (0, 0)),
        ],
        out_specs=(
            per_row(SEQ, D),
            per_row(SEQ, 4 * W),
            per_row(SEQ, D),
            per_row(SEQ, W),
            per_row(8 * K, SEQ),
            per_row(8, SEQ),
            per_row(SEQ, D),
        ),
        scratch_shapes=[
            pltpu.VMEM((SEQ + 2 * PAD, D), F32),
            pltpu.VMEM((SEQ + 2 * PAD, W), F32),
            pltpu.VMEM((128, SEQ), F32),
        ],
        compiler_params=pltpu.CompilerParams(vmem_limit_bytes=56 * 1024 * 1024),
        name="mixer_forward",
    )(lengths, hidden, full, full, depth, kmt)


TILE = 256
CHUNK = 16


def ffn_kernel(
    len_ref,
    ctx_ref,
    x_ref,
    og_ref,
    wout_ref,
    wdn_ref,
    wup_ref,
    gb_ref,
    y_ref,
    act_ref,
    gpre_ref,
    fb_ref,
    gffn_ref,
    gmix_ref,
    gr1_ref,
    gctx_ref,
    stat_ref,
    mix,
    first,
    n1,
    inv,
    ffn,
    pre,
    dg,
    gr2,
):
    step = pl.program_id(0)
    row = step // (SEQ // TILE)
    base = (step % (SEQ // TILE)) * TILE
    left = len_ref[row] - base

    @pl.when(step == 0)
    def _():
        stat_ref[...] = jnp.zeros_like(stat_ref)

    for b in range(2):
        mix[:, b * W : (b + 1) * W] = nn(ctx_ref[...], wout_ref[b])

    def mask_of(i):
        return (lax.broadcasted_iota(jnp.int32, (CHUNK, 1), 0) + i * CHUNK < left).astype(F32)

    def fold(values):
        return jnp.sum(values.reshape(CHUNK // 8, 8, D), axis=0)

    def tally(k, values):
        stat_ref[k] = stat_ref[k] + fold(values)

    def rows_of(i):
        return pl.ds(pl.multiple_of(i * CHUNK, CHUNK), CHUNK)

    def norm(values):
        average = jnp.mean(values, axis=-1, keepdims=True)
        centered = values - average
        inverse = lax.rsqrt(jnp.mean(centered * centered, axis=-1, keepdims=True) + EPSILON)
        return centered * inverse, inverse

    def norm_back(grad, normed, inverse, gain):
        scaled = grad * gain
        mean = jnp.mean(scaled, axis=-1, keepdims=True)
        other = jnp.mean(scaled * normed, axis=-1, keepdims=True)
        return inverse * (scaled - mean - normed * other)

    def norm_one(i, carry):
        rows = rows_of(i)
        xf, mixed = x_ref[rows].astype(F32), mix[rows]
        normed, inverse = norm(xf + mixed)
        result = normed * gb_ref[0:1] + gb_ref[2:3]
        n1[rows] = normed
        inv[rows] = jnp.broadcast_to(inverse, (CHUNK, 128))
        first[rows] = result
        fb_ref[rows] = result.astype(BF16)
        tally(0, xf * xf)
        tally(1, mixed * mixed * mask_of(i))
        return carry

    lax.fori_loop(0, TILE // CHUNK, norm_one, 0)

    for s in range(4):
        g = s // 2
        pre[...] = nt(fb_ref[:, g * W : (g + 1) * W], wup_ref[s])

        def gelu(i, carry):
            rows = rows_of(i)
            v = pre[rows]
            phi = 0.5 + 0.5 * lax.erf(v * math.sqrt(0.5))
            act_ref[rows, s * D : (s + 1) * D] = (v * phi).astype(BF16)
            dg[s, rows] = phi + v * jnp.exp(v * v * -0.5) * (1.0 / math.sqrt(2.0 * math.pi))
            return carry

        lax.fori_loop(0, TILE // CHUNK, gelu, 0)
        part = nn(act_ref[:, s * D : (s + 1) * D], wdn_ref[s])
        lanes = slice(g * W, (g + 1) * W)
        if s % 2 == 0:
            ffn[:, lanes] = part
        else:
            ffn[:, lanes] += part

    def norm_two(i, carry):
        rows = rows_of(i)
        mask = mask_of(i)
        out = ffn[rows]
        normed, inverse = norm(first[rows] + out)
        y = (normed * gb_ref[1:2] + gb_ref[3:4]) * mask
        y_ref[rows] = y.astype(BF16)
        grad = og_ref[rows].astype(F32) * mask
        back = norm_back(grad, normed, inverse, gb_ref[1:2])
        gr2[rows] = back
        gffn_ref[rows] = back.astype(BF16)
        tally(2, out * out * mask)
        tally(3, y * y)
        tally(5, grad * normed)
        tally(7, grad)
        return carry

    lax.fori_loop(0, TILE // CHUNK, norm_two, 0)

    for s in range(4):
        g = s // 2
        lanes = slice(g * W, (g + 1) * W)
        pre[...] = nt(gffn_ref[:, lanes], wdn_ref[s])

        def times(i, carry):
            rows = rows_of(i)
            gpre_ref[rows, s * D : (s + 1) * D] = (pre[rows] * dg[s, rows]).astype(BF16)
            return carry

        lax.fori_loop(0, TILE // CHUNK, times, 0)
        gr2[:, lanes] += nn(gpre_ref[:, s * D : (s + 1) * D], wup_ref[s])

    def norm_one_back(i, carry):
        rows = rows_of(i)
        grad, normed = gr2[rows], n1[rows]
        back = norm_back(grad, normed, inv[rows, 0:1], gb_ref[0:1])
        gr1_ref[rows] = back
        gmix_ref[rows] = back.astype(BF16)
        tally(4, grad * normed)
        tally(6, grad)
        return carry

    lax.fori_loop(0, TILE // CHUNK, norm_one_back, 0)
    gctx_ref[...] = (
        nt(gmix_ref[:, 0:W], wout_ref[0]) + nt(gmix_ref[:, W:], wout_ref[1])
    ).astype(BF16)


def feed_forward(lengths, ctx, x, out_grad, full, gb):
    tokens = x.shape[0]

    def per_tile(width):
        return pl.BlockSpec((TILE, width), lambda i: (i, 0))

    def out(dtype, width):
        return jax.ShapeDtypeStruct((tokens, width), dtype)

    return pl.pallas_call(
        ffn_kernel,
        grid=(tokens // TILE,),
        out_shape=(
            out(BF16, D),
            out(BF16, 4 * D),
            out(BF16, 4 * D),
            out(BF16, D),
            out(BF16, D),
            out(BF16, D),
            out(F32, D),
            out(BF16, D),
            jax.ShapeDtypeStruct((8, 8, D), F32),
        ),
        in_specs=[
            pl.BlockSpec(memory_space=pltpu.SMEM),
            per_tile(D),
            per_tile(D),
            per_tile(D),
            pl.BlockSpec((2, D, W), lambda i: (6, 0, 0)),
            pl.BlockSpec((4, D, W), lambda i: (1, 0, 0)),
            pl.BlockSpec((4, D, W), lambda i: (2, 0, 0)),
            pl.BlockSpec((8, D), lambda i: (0, 0)),
        ],
        out_specs=(
            per_tile(D),
            per_tile(4 * D),
            per_tile(4 * D),
            per_tile(D),
            per_tile(D),
            per_tile(D),
            per_tile(D),
            per_tile(D),
            pl.BlockSpec((8, 8, D), lambda i: (0, 0, 0)),
        ),
        scratch_shapes=[
            pltpu.VMEM((TILE, D), F32),
            pltpu.VMEM((TILE, D), F32),
            pltpu.VMEM((TILE, D), F32),
            pltpu.VMEM((TILE, 128), F32),
            pltpu.VMEM((TILE, D), F32),
            pltpu.VMEM((TILE, D), F32),
            pltpu.VMEM((4, TILE, D), F32),
            pltpu.VMEM((TILE, D), F32),
        ],
        compiler_params=pltpu.CompilerParams(vmem_limit_bytes=56 * 1024 * 1024),
        name="feed_forward",
    )(lengths, ctx, x, out_grad, full, full, full, gb)


def backward_kernel(
    len_ref,
    x_ref,
    proj_ref,
    dl_ref,
    kc_ref,
    wt_ref,
    lse_ref,
    gctx_ref,
    gr1_ref,
    win_ref,
    wpt_ref,
    depth_ref,
    kmt_ref,
    gproj_ref,
    gkc_ref,
    gin_ref,
    gkm_ref,
    gdk_ref,
    sv,
    gc,
    xs,
    gd,
    gs,
    gq,
    gt,
    dqt,
):
    row = pl.program_id(0)
    length = len_ref[row]
    inside = lax.broadcasted_iota(jnp.int32, (SEQ, 1), 0) < length

    @pl.when(row == 0)
    def _():
        gkm_ref[...] = jnp.zeros_like(gkm_ref)
        gdk_ref[...] = jnp.zeros_like(gdk_ref)

    for ref, width in ((sv, W), (gc, W), (xs, D), (gd, D)):
        ref[0:PAD] = jnp.zeros((PAD, width), F32)
        ref[PAD + SEQ :] = jnp.zeros((PAD, width), F32)
    sv[PAD : PAD + SEQ] = proj_ref[0, :, 3 * W :].astype(F32)
    gc[PAD : PAD + SEQ] = gctx_ref[0, :, W:].astype(F32)
    xs[PAD : PAD + SEQ] = x_ref[0].astype(F32)

    e16 = spread(16)
    place_row = lax.broadcasted_iota(jnp.int32, (W, 128), 0) // HD
    place_col = lax.broadcasted_iota(jnp.int32, (W, 128), 1)
    both = []
    for k in range(K):
        weight = pltpu.roll(wt_ref[0, k * 8 : k * 8 + 8], (k - K // 2) % SEQ, 1)
        high = weight.astype(BF16).astype(F32)
        both.append(jnp.concatenate([high, weight - high], axis=0).astype(BF16))
    for r in range(4):
        rows = slice(r * 128, (r + 1) * 128)
        spans = jnp.zeros((128, 128), F32)
        total = jnp.zeros((128, W), F32)
        for k in range(K):
            start = PAD + r * 128 + k - K // 2
            product_k = gc[PAD + r * 128 : PAD + (r + 1) * 128] * sv[start : start + 128]
            chosen = (place_col == place_row + 8 * k).astype(F32).astype(BF16)
            spans = spans + nn(product_k.astype(BF16), chosen)
            start = PAD + r * 128 - k + K // 2
            total = total + tn(both[k][:, rows], e16) * gc[start : start + 128]
        gt[:, rows] = spans.T
        gproj_ref[0, rows, 3 * W :] = total.astype(BF16)
    center = jnp.zeros((8, SEQ), F32)
    for k in range(K):
        center = center + wt_ref[0, k * 8 : k * 8 + 8] * gt[k * 8 : k * 8 + 8]
    glt = jnp.concatenate(
        [
            wt_ref[0, k * 8 : k * 8 + 8] * (gt[k * 8 : k * 8 + 8] - center)
            for k in range(K)
        ],
        axis=0,
    ).astype(BF16)
    query = proj_ref[0, :, 0:W].astype(F32)
    mk = (kc_ref[0] * query).astype(BF16)
    gkm_ref[...] += nn(glt, mk)
    mixed = tn(glt, kmt_ref[...])
    gkc_ref[0] = (mixed * query).astype(BF16)
    gq[...] = mixed * kc_ref[0]
    gd[PAD : PAD + SEQ] = nt(gkc_ref[0], wpt_ref[0])

    def column(c, carry):
        lane = pl.ds(pl.multiple_of(c * 128, 128), 128)
        sums = [jnp.zeros((8, 128), F32)] * K
        for r in range(8):
            total = jnp.zeros((64, 128), F32)
            center = PAD + r * 64
            grad = gd[center : center + 64, lane]
            for k in range(K):
                start = center + k - K // 2
                sums[k] = sums[k] + jnp.sum(
                    (xs[start : start + 64, lane] * grad).reshape(8, 8, 128), axis=0
                )
                start = center - k + K // 2
                total = total + gd[start : start + 64, lane] * depth_ref[k : k + 1, lane]
            gs[r * 64 : (r + 1) * 64, lane] = total
        for k in range(K):
            gdk_ref[k, :, lane] = gdk_ref[k, :, lane] + sums[k]
        return carry

    lax.fori_loop(0, D // 128, column, 0)

    lane_head = lax.broadcasted_iota(jnp.int32, (1, 128), 1) // HD
    bias = jnp.where(inside, 0.0, -1e30).astype(F32)

    def pair(p, carry):
        def lanes(part):
            return pl.ds(pl.multiple_of(part * W + p * 128, 128), 128)

        q2, k2, v2 = (proj_ref[0, :, lanes(part)] for part in range(3))
        g2 = gctx_ref[0, :, lanes(0)]
        results = []
        for h in range(2):
            mine = lane_head == h
            scale = jnp.where(mine, 1.0 / math.sqrt(HD), 0.0).astype(BF16)
            scores = nt(k2, q2 * scale) + bias
            probs = jnp.exp(scores - lse_ref[0, pl.ds(p * 2 + h, 1)])
            grads = nt(v2 * jnp.where(mine, 1.0, 0.0).astype(BF16), g2)
            correction = jnp.sum(probs * grads, axis=0, keepdims=True)
            grad_scores = (probs * (grads - correction)).astype(BF16)
            dqt[h * HD : (h + 1) * HD] = tn(k2, grad_scores)[h * HD : (h + 1) * HD]
            results.append((nn(grad_scores, q2), nn(probs.astype(BF16), g2)))
        low = lane_head == 0
        scale = 1.0 / math.sqrt(HD)
        gproj_ref[0, :, lanes(0)] = (dqt[...].T * scale + gq[:, lanes(0)]).astype(BF16)
        gproj_ref[0, :, lanes(1)] = (jnp.where(low, results[0][0], results[1][0]) * scale).astype(BF16)
        gproj_ref[0, :, lanes(2)] = jnp.where(low, results[0][1], results[1][1]).astype(BF16)
        return carry

    lax.fori_loop(0, HEADS // 2, pair, 0)

    for b in range(4):
        gs[...] += nt(gproj_ref[0, :, b * W : (b + 1) * W], win_ref[b])
    gin_ref[0] = jnp.where(inside, gr1_ref[0] + gs[...], 0.0).astype(BF16)


def backward(lengths, x, proj, dl, kc, wt, lse, gctx, gr1, full, depth, kmt):
    rows = x.shape[0]

    def per_row(*shape):
        return pl.BlockSpec((1,) + shape, lambda r: (r, 0, 0))

    def out(dtype, *shape):
        return jax.ShapeDtypeStruct((rows,) + shape, dtype)

    return pl.pallas_call(
        backward_kernel,
        grid=(rows,),
        out_shape=(
            out(BF16, SEQ, 4 * W),
            out(BF16, SEQ, W),
            out(BF16, SEQ, D),
            jax.ShapeDtypeStruct((8 * K, W), F32),
            jax.ShapeDtypeStruct((K, 8, D), F32),
        ),
        in_specs=[
            pl.BlockSpec(memory_space=pltpu.SMEM),
            per_row(SEQ, D),
            per_row(SEQ, 4 * W),
            per_row(SEQ, D),
            per_row(SEQ, W),
            per_row(8 * K, SEQ),
            per_row(8, SEQ),
            per_row(SEQ, D),
            per_row(SEQ, D),
            pl.BlockSpec((4, D, W), lambda r: (0, 0, 0)),
            pl.BlockSpec((1, D, W), lambda r: (14, 0, 0)),
            pl.BlockSpec((16, D), lambda r: (0, 0)),
            pl.BlockSpec((8 * K, W), lambda r: (0, 0)),
        ],
        out_specs=(
            per_row(SEQ, 4 * W),
            per_row(SEQ, W),
            per_row(SEQ, D),
            pl.BlockSpec((8 * K, W), lambda r: (0, 0)),
            pl.BlockSpec((K, 8, D), lambda r: (0, 0, 0)),
        ),
        scratch_shapes=[
            pltpu.VMEM((SEQ + 2 * PAD, W), F32),
            pltpu.VMEM((SEQ + 2 * PAD, W), F32),
            pltpu.VMEM((SEQ + 2 * PAD, D), F32),
            pltpu.VMEM((SEQ + 2 * PAD, D), F32),
            pltpu.VMEM((SEQ, D), F32),
            pltpu.VMEM((SEQ, W), F32),
            pltpu.VMEM((128, SEQ), F32),
            pltpu.VMEM((128, SEQ), F32),
        ],
        compiler_params=pltpu.CompilerParams(vmem_limit_bytes=56 * 1024 * 1024),
        name="mixer_backward",
    )(lengths, x, proj, dl, kc, wt, lse, gctx, gr1, full, full, depth, kmt)


def pack(in_weight, depth_kernel, point_weight, kernel_weight, out_weight, up_weight, down_weight, norm_gains, norm_biases):
    rows = in_weight.shape[0]

    def halves(grouped):
        return grouped.reshape(G * 2, rows, W)

    kernel = kernel_weight.reshape(K, rows, 3).transpose(1, 0, 2).reshape(rows, 3 * K)
    small = jnp.concatenate([depth_kernel.T, kernel, norm_gains.T, norm_biases.T], axis=1)
    small = jnp.pad(small, ((0, 0), (0, W - small.shape[1])))
    return jnp.concatenate(
        [
            in_weight.reshape(rows, 4, W).transpose(1, 0, 2),
            halves(down_weight),
            halves(up_weight.transpose(0, 2, 1)),
            out_weight.reshape(rows, 2, W).transpose(1, 0, 2),
            point_weight[None],
            small[None],
        ],
        axis=0,
    )


def unpack(shard):
    rows = shard.shape[1]
    small = shard[15]
    kernel = small[:, K : 4 * K].reshape(rows, K, 3).transpose(1, 0, 2).reshape(K, 3 * rows)
    return (
        shard[0:4].transpose(1, 0, 2).reshape(rows, 4 * W),
        small[:, :K].T,
        shard[14],
        kernel,
        shard[12:14].transpose(1, 0, 2).reshape(rows, 2 * W),
        shard[8:12].reshape(G, 2 * rows, W).transpose(0, 2, 1),
        shard[4:8].reshape(G, 2 * rows, W),
        small[:, 4 * K : 4 * K + 2].T,
        small[:, 4 * K + 2 : 4 * K + 4].T,
    )


def layer(hidden, lengths, full, out_grad):
    rows = hidden.shape[0]
    tokens = rows * SEQ
    small = full[15].astype(F32)
    depth = jnp.pad(small[:, :K].T, ((0, 16 - K), (0, 0)))
    kernel = small[:, K : 4 * K].reshape(D, K, 3).transpose(1, 0, 2).reshape(K, W, HEADS)
    kmt = jnp.pad(kernel.transpose(0, 2, 1), ((0, 0), (0, 8 - HEADS), (0, 0)))
    kmt = kmt.reshape(8 * K, W).astype(BF16)
    gb = jnp.pad(small[:, 4 * K : 4 * K + 4].T, ((0, 4), (0, 0)))

    x, proj, dl, kc, wt, lse, ctx = forward(lengths, hidden, full, depth, kmt)
    flat_x, flat_ctx = x.reshape(tokens, D), ctx.reshape(tokens, D)
    y, act, gpre, fb, gffn, gmix, gr1, gctx, stat = feed_forward(
        lengths, flat_ctx, flat_x, out_grad.reshape(tokens, D), full, gb
    )
    gproj, gkc, gin, gkm, gdk = backward(
        lengths,
        x,
        proj,
        dl,
        kc,
        wt,
        lse,
        gctx.reshape(rows, SEQ, D),
        gr1.reshape(rows, SEQ, D),
        full,
        depth,
        kmt,
    )
    stat = jnp.sum(stat, axis=1)
    grad_kernel = gkm.reshape(K, 8, W)[:, :HEADS].transpose(0, 2, 1).reshape(K, D, 3)
    grad_small = jnp.concatenate(
        [
            jnp.sum(gdk, axis=1).T,
            grad_kernel.transpose(1, 0, 2).reshape(D, 3 * K),
            stat[4:8].T,
        ],
        axis=1,
    )
    grad_small = jnp.pad(grad_small, ((0, 0), (0, W - grad_small.shape[1]))).astype(BF16)
    local = weight_grads(flat_x, dl, gproj, gkc, flat_ctx, gmix, act, gffn, gpre, fb, grad_small)
    sums = jnp.sum(stat[0:4], axis=1)
    count = jnp.sum(lengths).astype(F32)
    tiny = jnp.pad(jnp.concatenate([sums, count[None]]), (0, 123))
    tiny = jnp.broadcast_to(tiny[None], (8, 128))
    return y.reshape(rows, SEQ, D), gin, local, tiny


def weight_grads(x, dl, gproj, gkc, ctx, gmix, act, gffn, gpre, fb, grad_small):
    tokens = x.shape[0]
    gproj, gkc, dl = gproj.reshape(tokens, 4 * W), gkc.reshape(tokens, W), dl.reshape(tokens, D)

    def block(a, b):
        return tn(a, b).astype(BF16)

    def group(values, g):
        return values[:, g * W : (g + 1) * W]

    blocks = [block(x, group(gproj, b)) for b in range(4)]
    blocks += [block(act[:, s * D : (s + 1) * D], group(gffn, s // 2)) for s in range(4)]
    blocks += [block(gpre[:, s * D : (s + 1) * D], group(fb, s // 2)) for s in range(4)]
    blocks += [block(ctx, group(gmix, b)) for b in range(2)]
    blocks += [block(dl, gkc), grad_small]
    return jnp.stack(blocks)


def body(
    mesh,
    hidden,
    lengths,
    in_weight,
    depth_kernel,
    point_weight,
    kernel_weight,
    out_weight,
    up_weight,
    down_weight,
    norm_gains,
    norm_biases,
    out_grad,
):
    full = gather_all(
        pack(
            in_weight,
            depth_kernel,
            point_weight,
            kernel_weight,
            out_weight,
            up_weight,
            down_weight,
            norm_gains,
            norm_biases,
        ),
        mesh,
    )
    output, input_grad, local, tiny = layer(hidden, lengths, full, out_grad)
    shard, totals = scatter_all(local, tiny, mesh)
    rms = jnp.sqrt(totals[0, :4] / (totals[0, 4] * D))
    return (output, input_grad) + unpack(shard) + (rms,)


def solution(mesh):
    in_specs = (
        P(("dp", "fsdp"), None, None),
        P(("dp", "fsdp")),
        P(("dp", "fsdp"), None),
        P(None, ("dp", "fsdp")),
        P(("dp", "fsdp"), None),
        P(None, ("dp", "fsdp")),
        P(("dp", "fsdp"), None),
        P(None, None, ("dp", "fsdp")),
        P(None, ("dp", "fsdp"), None),
        P(None, ("dp", "fsdp")),
        P(None, ("dp", "fsdp")),
        P(("dp", "fsdp"), None, None),
    )
    out_specs = (
        P(("dp", "fsdp"), None, None),
        P(("dp", "fsdp"), None, None),
        P(("dp", "fsdp"), None),
        P(None, ("dp", "fsdp")),
        P(("dp", "fsdp"), None),
        P(None, ("dp", "fsdp")),
        P(("dp", "fsdp"), None),
        P(None, None, ("dp", "fsdp")),
        P(None, ("dp", "fsdp"), None),
        P(None, ("dp", "fsdp")),
        P(None, ("dp", "fsdp")),
        P(),
    )
    return jax.shard_map(functools.partial(body, mesh), mesh=mesh, in_specs=in_specs, out_specs=out_specs, check_vma=False)
```

```python
import functools
import math

import jax
import jax.numpy as jnp
from jax import lax
from jax.experimental import pallas as pl
from jax.experimental.pallas import tpu as pltpu
from jax.sharding import PartitionSpec as P

D = 768
HEADS = 6
HD = 64
G = 2
K = 9
SEQ = 512


EPSILON = 1e-06
MESH = pl.DeviceIdType.MESH
BLOCKS = 16
HALF = BLOCKS // 2


def place():
    dp, y = lax.axis_index("dp"), lax.axis_index("fsdp")
    return dp, dp // 4, (dp // 2) % 2, dp % 2, y


def partners(dp, x, core, y):
    return (dp + 1 - 2 * core, y), (dp + 2 - 4 * x, y), (dp, 1 - y)


def meet(peers, others):
    barrier = pltpu.get_barrier_semaphore()
    for peer in peers:
        pl.semaphore_signal(barrier, inc=1, device_id=peer, device_id_type=MESH)
    count = len(peers)
    for there, peer in others:

        @pl.when(there)
        def _():
            pl.semaphore_signal(barrier, inc=1, device_id=peer, device_id_type=MESH)

        count = count + there.astype(jnp.int32)
    pl.semaphore_wait(barrier, count)


def send(src, dst, send_sem, recv_sem, device):
    return pltpu.make_async_remote_copy(
        src_ref=src,
        dst_ref=dst,
        send_sem=send_sem,
        recv_sem=recv_sem,
        device_id=device,
        device_id_type=MESH,
    )


def gather_kernel(
    depth, p_ref, g_ref, own_sem, zs, zr, xs, xr, ys, yr, ds, dr, cs, cr
):
    dp, z, x, core, y = place()
    c_dev, x_dev, y_dev = partners(dp, x, core, y)
    up_dev, down_dev = (dp + 4, y), (dp - 4, y)
    own = pltpu.make_async_copy(p_ref, g_ref.at[:, z, x, core, y], own_sem)
    own.start()
    meet((c_dev, x_dev, y_dev), ((z + 1 < depth, up_dev), (z > 0, down_dev)))
    own.wait()
    steps = 2 * depth - 1

    def target(q):
        return z + ((q + 1) // 2) * (1 - 2 * (q % 2))

    def z_copy(j, way, device):
        slab = g_ref.at[:, j, x, core, y]
        return send(slab, slab, zs.at[way, j], zr.at[j], device)

    def x_copy(j):
        slab = g_ref.at[:, j, x, core, y]
        return send(slab, slab, xs.at[j], xr.at[j], x_dev)

    def y_copy(j):
        slab = g_ref.at[:, j, x, core, y]
        return send(slab, slab, ys.at[j], yr.at[j], y_dev)

    def d_copy(j, half):
        if half == 0:
            slab = g_ref.at[pl.ds(0, HALF), j, 1 - x, core, y]
            return send(slab, slab, ds.at[0, j], dr.at[0, j], y_dev)
        slab = g_ref.at[pl.ds(HALF, HALF), j, x, core, 1 - y]
        return send(slab, slab, ds.at[1, j], dr.at[1, j], x_dev)

    def c_copy(j, a, b):
        slab = g_ref.at[:, j, (x + a) % 2, core, (y + b) % 2]
        return send(slab, slab, cs.at[2 * a + b, j], cr.at[2 * a + b, j], c_dev)

    def c_arrival(j, a, b):
        slab = g_ref.at[:, j, (x + a) % 2, 1 - core, (y + b) % 2]
        return send(slab, slab, cs.at[2 * a + b, j], cr.at[2 * a + b, j], c_dev)

    def x_arrival(j):
        slab = g_ref.at[:, j, 1 - x, core, y]
        return send(slab, slab, xs.at[j], xr.at[j], x_dev)

    def y_arrival(j):
        slab = g_ref.at[:, j, x, core, 1 - y]
        return send(slab, slab, ys.at[j], yr.at[j], y_dev)

    def d_arrival(j, half):
        slab = g_ref.at[pl.ds(half * HALF, HALF), j, 1 - x, core, 1 - y]
        return send(slab, slab, ds.at[half, j], dr.at[half, j], y_dev if half == 0 else x_dev)

    def first(j):
        @pl.when(j != z)
        def _():
            z_copy(j, 0, up_dev).wait_recv()

        @pl.when((j <= z) & (z + 1 < depth))
        def _():
            z_copy(j, 0, up_dev).start()

        @pl.when((j >= z) & (z > 0))
        def _():
            z_copy(j, 1, down_dev).start()

        x_copy(j).start()
        y_copy(j).start()
        c_copy(j, 0, 0).start()

    def second(j):
        x_arrival(j).wait_recv()
        d_copy(j, 0).start()
        c_copy(j, 1, 0).start()
        y_arrival(j).wait_recv()
        d_copy(j, 1).start()
        c_copy(j, 0, 1).start()

    def third(j):
        d_arrival(j, 0).wait_recv()
        d_arrival(j, 1).wait_recv()
        c_copy(j, 1, 1).start()

    def stage(q, work):
        j = target(q)

        @pl.when((q >= 0) & (q < steps) & (j >= 0) & (j < depth))
        def _():
            work(j)

    def step(q, carry):
        stage(q, first)
        stage(q - 1, second)
        stage(q - 2, third)
        return carry

    lax.fori_loop(0, steps + 2, step, 0)

    def finish(j, carry):
        for a in range(2):
            for b in range(2):
                c_arrival(j, a, b).wait_recv()
                c_copy(j, a, b).wait_send()
        x_copy(j).wait_send()
        y_copy(j).wait_send()
        d_copy(j, 0).wait_send()
        d_copy(j, 1).wait_send()

        @pl.when((j <= z) & (z + 1 < depth))
        def _():
            z_copy(j, 0, up_dev).wait_send()

        @pl.when((j >= z) & (z > 0))
        def _():
            z_copy(j, 1, down_dev).wait_send()

        return carry

    lax.fori_loop(0, depth, finish, 0)


def gather_all(packed, mesh):
    dp, fsdp = mesh.shape["dp"], mesh.shape["fsdp"]
    _, rows, width = packed.shape
    if fsdp != 2 or dp % 4:
        full = lax.all_gather(packed, ("dp", "fsdp"), axis=1, tiled=False)
        return full.reshape(BLOCKS, dp * fsdp * rows, width)
    depth = dp // 4
    dma = pltpu.SemaphoreType.DMA
    full = pl.pallas_call(
        functools.partial(gather_kernel, depth),
        out_shape=jax.ShapeDtypeStruct((BLOCKS, depth, 2, 2, 2, rows, width), packed.dtype),
        in_specs=[pl.BlockSpec(memory_space=pltpu.VMEM)],
        out_specs=pl.BlockSpec(memory_space=pl.ANY),
        scratch_shapes=[
            dma(()),
            dma((2, depth)),
            dma((depth,)),
            dma((depth,)),
            dma((depth,)),
            dma((depth,)),
            dma((depth,)),
            dma((2, depth)),
            dma((2, depth)),
            dma((4, depth)),
            dma((4, depth)),
        ],
        compiler_params=pltpu.CompilerParams(collective_id=0, has_side_effects=True),
        name="gather_all",
    )(packed)
    return full.reshape(BLOCKS, dp * fsdp * rows, width)


W = D // G
F32, BF16 = jnp.float32, jnp.bfloat16
PAD = 8


def nn(a, b):
    return lax.dot_general(a, b, (((1,), (0,)), ((), ())), preferred_element_type=F32)


def nt(a, b):
    return lax.dot_general(a, b, (((1,), (1,)), ((), ())), preferred_element_type=F32)


def tn(a, b):
    return lax.dot_general(a, b, (((0,), (0,)), ((), ())), preferred_element_type=F32)


def spread(rows):
    head = lax.broadcasted_iota(jnp.int32, (rows, W), 0) % 8
    channel = lax.broadcasted_iota(jnp.int32, (rows, W), 1) // HD
    return (head == channel).astype(F32).astype(BF16)


def forward_kernel(
    len_ref,
    hid_ref,
    win_ref,
    wpt_ref,
    depth_ref,
    kmt_ref,
    x_ref,
    proj_ref,
    dl_ref,
    kc_ref,
    wt_ref,
    lse_ref,
    ctx_ref,
    xs,
    sv,
    ot,
):
    length = len_ref[pl.program_id(0)]
    inside = lax.broadcasted_iota(jnp.int32, (SEQ, 1), 0) < length
    x = jnp.where(inside, hid_ref[0], jnp.zeros((), BF16))
    x_ref[0] = x
    xs[0:PAD] = jnp.zeros((PAD, D), F32)
    xs[PAD + SEQ :] = jnp.zeros((PAD, D), F32)
    xs[PAD : PAD + SEQ] = x.astype(F32)
    sv[0:PAD] = jnp.zeros((PAD, W), F32)
    sv[PAD + SEQ :] = jnp.zeros((PAD, W), F32)

    for b in range(4):
        part = nn(x_ref[0], win_ref[b]).astype(BF16)
        proj_ref[0, :, b * W : (b + 1) * W] = part
        if b == 3:
            sv[PAD : PAD + SEQ] = part.astype(F32)

    def column(c, carry):
        lane = pl.ds(pl.multiple_of(c * 128, 128), 128)
        for r in range(8):
            total = jnp.zeros((64, 128), F32)
            for k in range(K):
                start = PAD + r * 64 + k - K // 2
                total = total + xs[start : start + 64, lane] * depth_ref[k : k + 1, lane]
            dl_ref[0, r * 64 : (r + 1) * 64, lane] = total.astype(BF16)
        return carry

    lax.fori_loop(0, D // 128, column, 0)
    kc_ref[0] = nn(dl_ref[0], wpt_ref[0])
    mk = (kc_ref[0] * proj_ref[0, :, 0:W].astype(F32)).astype(BF16)
    logits = nt(kmt_ref[...], mk)
    top = logits[0:8]
    for k in range(1, K):
        top = jnp.maximum(top, logits[k * 8 : k * 8 + 8])
    parts = [jnp.exp(logits[k * 8 : k * 8 + 8] - top) for k in range(K)]
    inverse = 1.0 / sum(parts)
    both = []
    for k in range(K):
        weight = parts[k] * inverse
        wt_ref[0, k * 8 : k * 8 + 8] = weight
        high = weight.astype(BF16).astype(F32)
        both.append(jnp.concatenate([high, weight - high], axis=0).astype(BF16))
    e16 = spread(16)
    for r in range(4):
        total = jnp.zeros((128, W), F32)
        for k in range(K):
            start = PAD + r * 128 + k - K // 2
            total = total + tn(both[k][:, r * 128 : (r + 1) * 128], e16) * sv[start : start + 128]
        ctx_ref[0, r * 128 : (r + 1) * 128, W:] = total.astype(BF16)

    lane_head = lax.broadcasted_iota(jnp.int32, (1, 128), 1) // HD
    bias = jnp.where(inside, 0.0, -1e30).astype(F32)

    def pair(p, carry):
        def slab(part):
            return proj_ref[0, :, pl.ds(pl.multiple_of(part * W + p * 128, 128), 128)]

        q2, k2, v2 = slab(0), slab(1), slab(2)
        for h in range(2):
            scale = jnp.where(lane_head == h, 1.0 / math.sqrt(HD), 0.0).astype(BF16)
            scores = nt(k2, q2 * scale) + bias
            peak = jnp.max(scores, axis=0, keepdims=True)
            power = jnp.exp(scores - peak)
            total = jnp.sum(power, axis=0, keepdims=True)
            lse_ref[0, pl.ds(p * 2 + h, 1)] = peak + jnp.log(total)
            probs = (power * (1.0 / total)).astype(BF16)
            ot[h * HD : (h + 1) * HD] = tn(v2, probs)[h * HD : (h + 1) * HD]
        ctx_ref[0, :, pl.ds(pl.multiple_of(p * 128, 128), 128)] = ot[...].T.astype(BF16)
        return carry

    lax.fori_loop(0, HEADS // 2, pair, 0)


def forward(lengths, hidden, full, depth, kmt):
    rows = hidden.shape[0]

    def per_row(*shape):
        return pl.BlockSpec((1,) + shape, lambda r: (r, 0, 0))

    def out(dtype, *shape):
        return jax.ShapeDtypeStruct((rows,) + shape, dtype)

    return pl.pallas_call(
        forward_kernel,
        grid=(rows,),
        out_shape=(
            out(BF16, SEQ, D),
            out(BF16, SEQ, 4 * W),
            out(BF16, SEQ, D),
            out(F32, SEQ, W),
            out(F32, 8 * K, SEQ),
            out(F32, 8, SEQ),
            out(BF16, SEQ, D),
        ),
        in_specs=[
            pl.BlockSpec(memory_space=pltpu.SMEM),
            per_row(SEQ, D),
            pl.BlockSpec((4, D, W), lambda r: (2, 0, 0)),
            pl.BlockSpec((1, D, W), lambda r: (14, 0, 0)),
            pl.BlockSpec((16, D), lambda r: (0, 0)),
            pl.BlockSpec((8 * K, W), lambda r: (0, 0)),
        ],
        out_specs=(
            per_row(SEQ, D),
            per_row(SEQ, 4 * W),
            per_row(SEQ, D),
            per_row(SEQ, W),
            per_row(8 * K, SEQ),
            per_row(8, SEQ),
            per_row(SEQ, D),
        ),
        scratch_shapes=[
            pltpu.VMEM((SEQ + 2 * PAD, D), F32),
            pltpu.VMEM((SEQ + 2 * PAD, W), F32),
            pltpu.VMEM((128, SEQ), F32),
        ],
        compiler_params=pltpu.CompilerParams(vmem_limit_bytes=56 * 1024 * 1024),
        name="mixer_forward",
    )(lengths, hidden, full, full, depth, kmt)


TILE = 256
CHUNK = 16


def ffn_kernel(
    len_ref,
    ctx_ref,
    x_ref,
    og_ref,
    wout_ref,
    wdn_ref,
    wup_ref,
    gb_ref,
    y_ref,
    act_ref,
    gpre_ref,
    fb_ref,
    gffn_ref,
    gmix_ref,
    gr1_ref,
    gctx_ref,
    stat_ref,
    mix,
    first,
    n1,
    inv,
    ffn,
    pre,
    dg,
    gr2,
):
    step = pl.program_id(0)
    row = step // (SEQ // TILE)
    base = (step % (SEQ // TILE)) * TILE
    left = len_ref[row] - base

    @pl.when(step == 0)
    def _():
        stat_ref[...] = jnp.zeros_like(stat_ref)

    for b in range(2):
        mix[:, b * W : (b + 1) * W] = nn(ctx_ref[...], wout_ref[b])

    def mask_of(i):
        return (lax.broadcasted_iota(jnp.int32, (CHUNK, 1), 0) + i * CHUNK < left).astype(F32)

    def fold(values):
        return jnp.sum(values.reshape(CHUNK // 8, 8, D), axis=0)

    def tally(k, values):
        stat_ref[k] = stat_ref[k] + fold(values)

    def rows_of(i):
        return pl.ds(pl.multiple_of(i * CHUNK, CHUNK), CHUNK)

    def norm(values):
        average = jnp.mean(values, axis=-1, keepdims=True)
        centered = values - average
        inverse = lax.rsqrt(jnp.mean(centered * centered, axis=-1, keepdims=True) + EPSILON)
        return centered * inverse, inverse

    def norm_back(grad, normed, inverse, gain):
        scaled = grad * gain
        mean = jnp.mean(scaled, axis=-1, keepdims=True)
        other = jnp.mean(scaled * normed, axis=-1, keepdims=True)
        return inverse * (scaled - mean - normed * other)

    def norm_one(i, carry):
        rows = rows_of(i)
        xf, mixed = x_ref[rows].astype(F32), mix[rows]
        normed, inverse = norm(xf + mixed)
        result = normed * gb_ref[0:1] + gb_ref[2:3]
        n1[rows] = normed
        inv[rows] = jnp.broadcast_to(inverse, (CHUNK, 128))
        first[rows] = result
        for g in range(G):
            fb_ref[g, rows] = result[:, g * W : (g + 1) * W].astype(BF16)
        tally(0, xf * xf)
        tally(1, mixed * mixed * mask_of(i))
        return carry

    lax.fori_loop(0, TILE // CHUNK, norm_one, 0)

    for s in range(4):
        g = s // 2
        pre[...] = nt(fb_ref[g], wup_ref[s])

        def gelu(i, carry):
            rows = rows_of(i)
            v = pre[rows]
            phi = 0.5 + 0.5 * lax.erf(v * math.sqrt(0.5))
            act_ref[s, rows] = (v * phi).astype(BF16)
            dg[s, rows] = phi + v * jnp.exp(v * v * -0.5) * (1.0 / math.sqrt(2.0 * math.pi))
            return carry

        lax.fori_loop(0, TILE // CHUNK, gelu, 0)
        part = nn(act_ref[s], wdn_ref[s])
        lanes = slice(g * W, (g + 1) * W)
        if s % 2 == 0:
            ffn[:, lanes] = part
        else:
            ffn[:, lanes] += part

    def norm_two(i, carry):
        rows = rows_of(i)
        mask = mask_of(i)
        out = ffn[rows]
        normed, inverse = norm(first[rows] + out)
        y = (normed * gb_ref[1:2] + gb_ref[3:4]) * mask
        y_ref[rows] = y.astype(BF16)
        grad = og_ref[rows].astype(F32) * mask
        back = norm_back(grad, normed, inverse, gb_ref[1:2])
        gr2[rows] = back
        for g in range(G):
            gffn_ref[g, rows] = back[:, g * W : (g + 1) * W].astype(BF16)
        tally(2, out * out * mask)
        tally(3, y * y)
        tally(5, grad * normed)
        tally(7, grad)
        return carry

    lax.fori_loop(0, TILE // CHUNK, norm_two, 0)

    for s in range(4):
        g = s // 2
        lanes = slice(g * W, (g + 1) * W)
        pre[...] = nt(gffn_ref[g], wdn_ref[s])

        def times(i, carry):
            rows = rows_of(i)
            gpre_ref[s, rows] = (pre[rows] * dg[s, rows]).astype(BF16)
            return carry

        lax.fori_loop(0, TILE // CHUNK, times, 0)
        gr2[:, lanes] += nn(gpre_ref[s], wup_ref[s])

    def norm_one_back(i, carry):
        rows = rows_of(i)
        grad, normed = gr2[rows], n1[rows]
        back = norm_back(grad, normed, inv[rows, 0:1], gb_ref[0:1])
        gr1_ref[rows] = back
        for g in range(2):
            gmix_ref[g, rows] = back[:, g * W : (g + 1) * W].astype(BF16)
        tally(4, grad * normed)
        tally(6, grad)
        return carry

    lax.fori_loop(0, TILE // CHUNK, norm_one_back, 0)
    gctx_ref[...] = (
        nt(gmix_ref[0], wout_ref[0]) + nt(gmix_ref[1], wout_ref[1])
    ).astype(BF16)


def feed_forward(lengths, ctx, x, out_grad, full, gb):
    tokens = x.shape[0]

    def per_tile(width):
        return pl.BlockSpec((TILE, width), lambda i: (i, 0))

    def out(dtype, width):
        return jax.ShapeDtypeStruct((tokens, width), dtype)

    def slabs(count, width):
        return pl.BlockSpec((count, TILE, width), lambda i: (0, i, 0))

    def slabs_out(count, width):
        return jax.ShapeDtypeStruct((count, tokens, width), BF16)

    return pl.pallas_call(
        ffn_kernel,
        grid=(tokens // TILE,),
        out_shape=(
            out(BF16, D),
            slabs_out(4, D),
            slabs_out(4, D),
            slabs_out(G, W),
            slabs_out(G, W),
            slabs_out(2, W),
            out(F32, D),
            out(BF16, D),
            jax.ShapeDtypeStruct((8, 8, D), F32),
        ),
        in_specs=[
            pl.BlockSpec(memory_space=pltpu.SMEM),
            per_tile(D),
            per_tile(D),
            per_tile(D),
            pl.BlockSpec((2, D, W), lambda i: (6, 0, 0)),
            pl.BlockSpec((4, D, W), lambda i: (0, 0, 0)),
            pl.BlockSpec((4, D, W), lambda i: (1, 0, 0)),
            pl.BlockSpec((8, D), lambda i: (0, 0)),
        ],
        out_specs=(
            per_tile(D),
            slabs(4, D),
            slabs(4, D),
            slabs(G, W),
            slabs(G, W),
            slabs(2, W),
            per_tile(D),
            per_tile(D),
            pl.BlockSpec((8, 8, D), lambda i: (0, 0, 0)),
        ),
        scratch_shapes=[
            pltpu.VMEM((TILE, D), F32),
            pltpu.VMEM((TILE, D), F32),
            pltpu.VMEM((TILE, D), F32),
            pltpu.VMEM((TILE, 128), F32),
            pltpu.VMEM((TILE, D), F32),
            pltpu.VMEM((TILE, D), F32),
            pltpu.VMEM((4, TILE, D), F32),
            pltpu.VMEM((TILE, D), F32),
        ],
        compiler_params=pltpu.CompilerParams(vmem_limit_bytes=56 * 1024 * 1024),
        name="feed_forward",
    )(lengths, ctx, x, out_grad, full, full, full, gb)


def backward_kernel(
    len_ref,
    x_ref,
    proj_ref,
    dl_ref,
    kc_ref,
    wt_ref,
    lse_ref,
    gctx_ref,
    gr1_ref,
    win_ref,
    wpt_ref,
    depth_ref,
    kmt_ref,
    gproj_ref,
    gkc_ref,
    gin_ref,
    gkm_ref,
    gdk_ref,
    sv,
    gc,
    xs,
    gd,
    gs,
    gq,
    gt,
    dqt,
):
    row = pl.program_id(0)
    length = len_ref[row]
    inside = lax.broadcasted_iota(jnp.int32, (SEQ, 1), 0) < length

    @pl.when(row == 0)
    def _():
        gkm_ref[...] = jnp.zeros_like(gkm_ref)
        gdk_ref[...] = jnp.zeros_like(gdk_ref)

    for ref, width in ((sv, W), (gc, W), (xs, D), (gd, D)):
        ref[0:PAD] = jnp.zeros((PAD, width), F32)
        ref[PAD + SEQ :] = jnp.zeros((PAD, width), F32)
    sv[PAD : PAD + SEQ] = proj_ref[0, :, 3 * W :].astype(F32)
    gc[PAD : PAD + SEQ] = gctx_ref[0, :, W:].astype(F32)
    xs[PAD : PAD + SEQ] = x_ref[0].astype(F32)

    e16 = spread(16)
    place_row = lax.broadcasted_iota(jnp.int32, (W, 128), 0) // HD
    place_col = lax.broadcasted_iota(jnp.int32, (W, 128), 1)
    both = []
    for k in range(K):
        weight = pltpu.roll(wt_ref[0, k * 8 : k * 8 + 8], (k - K // 2) % SEQ, 1)
        high = weight.astype(BF16).astype(F32)
        both.append(jnp.concatenate([high, weight - high], axis=0).astype(BF16))
    for r in range(4):
        rows = slice(r * 128, (r + 1) * 128)
        spans = jnp.zeros((128, 128), F32)
        total = jnp.zeros((128, W), F32)
        for k in range(K):
            start = PAD + r * 128 + k - K // 2
            product_k = gc[PAD + r * 128 : PAD + (r + 1) * 128] * sv[start : start + 128]
            chosen = (place_col == place_row + 8 * k).astype(F32).astype(BF16)
            spans = spans + nn(product_k.astype(BF16), chosen)
            start = PAD + r * 128 - k + K // 2
            total = total + tn(both[k][:, rows], e16) * gc[start : start + 128]
        gt[:, rows] = spans.T
        gproj_ref[3, rows] = total.astype(BF16)
    center = jnp.zeros((8, SEQ), F32)
    for k in range(K):
        center = center + wt_ref[0, k * 8 : k * 8 + 8] * gt[k * 8 : k * 8 + 8]
    glt = jnp.concatenate(
        [
            wt_ref[0, k * 8 : k * 8 + 8] * (gt[k * 8 : k * 8 + 8] - center)
            for k in range(K)
        ],
        axis=0,
    ).astype(BF16)
    query = proj_ref[0, :, 0:W].astype(F32)
    mk = (kc_ref[0] * query).astype(BF16)
    gkm_ref[...] += nn(glt, mk)
    mixed = tn(glt, kmt_ref[...])
    gkc_ref[0] = (mixed * query).astype(BF16)
    gq[...] = mixed * kc_ref[0]
    gd[PAD : PAD + SEQ] = nt(gkc_ref[0], wpt_ref[0])

    def column(c, carry):
        lane = pl.ds(pl.multiple_of(c * 128, 128), 128)
        sums = [jnp.zeros((8, 128), F32)] * K
        for r in range(8):
            total = jnp.zeros((64, 128), F32)
            center = PAD + r * 64
            grad = gd[center : center + 64, lane]
            for k in range(K):
                start = center + k - K // 2
                sums[k] = sums[k] + jnp.sum(
                    (xs[start : start + 64, lane] * grad).reshape(8, 8, 128), axis=0
                )
                start = center - k + K // 2
                total = total + gd[start : start + 64, lane] * depth_ref[k : k + 1, lane]
            gs[r * 64 : (r + 1) * 64, lane] = total
        for k in range(K):
            gdk_ref[k, :, lane] = gdk_ref[k, :, lane] + sums[k]
        return carry

    lax.fori_loop(0, D // 128, column, 0)

    lane_head = lax.broadcasted_iota(jnp.int32, (1, 128), 1) // HD
    bias = jnp.where(inside, 0.0, -1e30).astype(F32)

    def pair(p, carry):
        def lanes(part):
            return pl.ds(pl.multiple_of(part * W + p * 128, 128), 128)

        q2, k2, v2 = (proj_ref[0, :, lanes(part)] for part in range(3))
        g2 = gctx_ref[0, :, lanes(0)]
        results = []
        for h in range(2):
            mine = lane_head == h
            scale = jnp.where(mine, 1.0 / math.sqrt(HD), 0.0).astype(BF16)
            scores = nt(k2, q2 * scale) + bias
            probs = jnp.exp(scores - lse_ref[0, pl.ds(p * 2 + h, 1)])
            grads = nt(v2 * jnp.where(mine, 1.0, 0.0).astype(BF16), g2)
            correction = jnp.sum(probs * grads, axis=0, keepdims=True)
            grad_scores = (probs * (grads - correction)).astype(BF16)
            dqt[h * HD : (h + 1) * HD] = tn(k2, grad_scores)[h * HD : (h + 1) * HD]
            results.append((nn(grad_scores, q2), nn(probs.astype(BF16), g2)))
        low = lane_head == 0
        scale = 1.0 / math.sqrt(HD)
        gproj_ref[0, :, lanes(0)] = (dqt[...].T * scale + gq[:, lanes(0)]).astype(BF16)
        gproj_ref[1, :, lanes(0)] = (jnp.where(low, results[0][0], results[1][0]) * scale).astype(BF16)
        gproj_ref[2, :, lanes(0)] = jnp.where(low, results[0][1], results[1][1]).astype(BF16)
        return carry

    lax.fori_loop(0, HEADS // 2, pair, 0)

    for b in range(4):
        gs[...] += nt(gproj_ref[b], win_ref[b])
    gin_ref[0] = jnp.where(inside, gr1_ref[0] + gs[...], 0.0).astype(BF16)


def backward(lengths, x, proj, dl, kc, wt, lse, gctx, gr1, full, depth, kmt):
    rows = x.shape[0]

    def per_row(*shape):
        return pl.BlockSpec((1,) + shape, lambda r: (r, 0, 0))

    def out(dtype, *shape):
        return jax.ShapeDtypeStruct((rows,) + shape, dtype)

    return pl.pallas_call(
        backward_kernel,
        grid=(rows,),
        out_shape=(
            jax.ShapeDtypeStruct((4, rows * SEQ, W), BF16),
            out(BF16, SEQ, W),
            out(BF16, SEQ, D),
            jax.ShapeDtypeStruct((8 * K, W), F32),
            jax.ShapeDtypeStruct((K, 8, D), F32),
        ),
        in_specs=[
            pl.BlockSpec(memory_space=pltpu.SMEM),
            per_row(SEQ, D),
            per_row(SEQ, 4 * W),
            per_row(SEQ, D),
            per_row(SEQ, W),
            per_row(8 * K, SEQ),
            per_row(8, SEQ),
            per_row(SEQ, D),
            per_row(SEQ, D),
            pl.BlockSpec((4, D, W), lambda r: (2, 0, 0)),
            pl.BlockSpec((1, D, W), lambda r: (14, 0, 0)),
            pl.BlockSpec((16, D), lambda r: (0, 0)),
            pl.BlockSpec((8 * K, W), lambda r: (0, 0)),
        ],
        out_specs=(
            pl.BlockSpec((4, SEQ, W), lambda r: (0, r, 0)),
            per_row(SEQ, W),
            per_row(SEQ, D),
            pl.BlockSpec((8 * K, W), lambda r: (0, 0)),
            pl.BlockSpec((K, 8, D), lambda r: (0, 0, 0)),
        ),
        scratch_shapes=[
            pltpu.VMEM((SEQ + 2 * PAD, W), F32),
            pltpu.VMEM((SEQ + 2 * PAD, W), F32),
            pltpu.VMEM((SEQ + 2 * PAD, D), F32),
            pltpu.VMEM((SEQ + 2 * PAD, D), F32),
            pltpu.VMEM((SEQ, D), F32),
            pltpu.VMEM((SEQ, W), F32),
            pltpu.VMEM((128, SEQ), F32),
            pltpu.VMEM((128, SEQ), F32),
        ],
        compiler_params=pltpu.CompilerParams(vmem_limit_bytes=56 * 1024 * 1024),
        name="mixer_backward",
    )(lengths, x, proj, dl, kc, wt, lse, gctx, gr1, full, full, depth, kmt)


def pack(in_weight, depth_kernel, point_weight, kernel_weight, out_weight, up_weight, down_weight, norm_gains, norm_biases):
    rows = in_weight.shape[0]

    def halves(grouped):
        return grouped.reshape(G * 2, rows, W)

    kernel = kernel_weight.reshape(K, rows, 3).transpose(1, 0, 2).reshape(rows, 3 * K)
    small = jnp.concatenate([depth_kernel.T, kernel, norm_gains.T, norm_biases.T], axis=1)
    small = jnp.pad(small, ((0, 0), (0, W - small.shape[1])))
    return jnp.concatenate(
        [
            halves(down_weight),
            halves(up_weight.transpose(0, 2, 1)),
            in_weight.reshape(rows, 4, W).transpose(1, 0, 2),
            out_weight.reshape(rows, 2, W).transpose(1, 0, 2),
            point_weight[None],
            small[None],
        ],
        axis=0,
    )


def unpack(shard):
    rows = shard.shape[1]
    small = shard[15]
    kernel = small[:, K : 4 * K].reshape(rows, K, 3).transpose(1, 0, 2).reshape(K, 3 * rows)
    return (
        shard[8:12].transpose(1, 0, 2).reshape(rows, 4 * W),
        small[:, :K].T,
        shard[14],
        kernel,
        shard[12:14].transpose(1, 0, 2).reshape(rows, 2 * W),
        shard[4:8].reshape(G, 2 * rows, W).transpose(0, 2, 1),
        shard[0:4].reshape(G, 2 * rows, W),
        small[:, 4 * K : 4 * K + 2].T,
        small[:, 4 * K + 2 : 4 * K + 4].T,
    )


def layer(hidden, lengths, full, out_grad):
    rows = hidden.shape[0]
    tokens = rows * SEQ
    small = full[15].astype(F32)
    depth = jnp.pad(small[:, :K].T, ((0, 16 - K), (0, 0)))
    kernel = small[:, K : 4 * K].reshape(D, K, 3).transpose(1, 0, 2).reshape(K, W, HEADS)
    kmt = jnp.pad(kernel.transpose(0, 2, 1), ((0, 0), (0, 8 - HEADS), (0, 0)))
    kmt = kmt.reshape(8 * K, W).astype(BF16)
    gb = jnp.pad(small[:, 4 * K : 4 * K + 4].T, ((0, 4), (0, 0)))

    x, proj, dl, kc, wt, lse, ctx = forward(lengths, hidden, full, depth, kmt)
    flat_x, flat_ctx = x.reshape(tokens, D), ctx.reshape(tokens, D)
    y, act, gpre, fb, gffn, gmix, gr1, gctx, stat = feed_forward(
        lengths, flat_ctx, flat_x, out_grad.reshape(tokens, D), full, gb
    )
    gproj, gkc, gin, gkm, gdk = backward(
        lengths,
        x,
        proj,
        dl,
        kc,
        wt,
        lse,
        gctx.reshape(rows, SEQ, D),
        gr1.reshape(rows, SEQ, D),
        full,
        depth,
        kmt,
    )
    stat = jnp.sum(stat, axis=1)
    grad_kernel = gkm.reshape(K, 8, W)[:, :HEADS].transpose(0, 2, 1).reshape(K, D, 3)
    grad_small = jnp.concatenate(
        [
            jnp.sum(gdk, axis=1).T,
            grad_kernel.transpose(1, 0, 2).reshape(D, 3 * K),
            stat[4:8].T,
        ],
        axis=1,
    )
    grad_small = jnp.pad(grad_small, ((0, 0), (0, W - grad_small.shape[1]))).astype(BF16)
    factors = (
        flat_x,
        dl.reshape(tokens, D),
        gproj,
        gkc.reshape(tokens, W),
        flat_ctx,
        gmix,
        act,
        gffn,
        gpre,
        fb,
    )
    sums = jnp.sum(stat[0:4], axis=1)
    count = jnp.sum(lengths).astype(F32)
    tiny = jnp.pad(jnp.concatenate([sums, count[None]]), (0, 123))
    tiny = jnp.broadcast_to(tiny[None], (8, 128))
    return y.reshape(rows, SEQ, D), gin, factors, grad_small, tiny


def weight_grads(x, dl, gproj, gkc, ctx, gmix, act, gffn, gpre, fb, small):
    pairs = [(act[s], gffn[s // 2]) for s in range(4)]
    pairs += [(gpre[s], fb[s // 2]) for s in range(4)]
    pairs += [(x, gproj[b]) for b in range(4)]
    pairs += [(ctx, gmix[b]) for b in range(2)]
    pairs += [(dl, gkc)]
    return jnp.stack([tn(a, b).astype(BF16) for a, b in pairs] + [small])


def scatter_kernel(
    depth,
    x_ref,
    dl_ref,
    gproj_ref,
    gkc_ref,
    ctx_ref,
    gmix_ref,
    act_ref,
    gffn_ref,
    gpre_ref,
    fb_ref,
    small_ref,
    t_ref,
    o_ref,
    u_ref,
    left,
    right,
    part,
    rc,
    r1,
    r2,
    ru,
    rd,
    tiny,
    got,
    left_sem,
    right_sem,
    cs,
    cr,
    s1,
    q1,
    s2,
    q2,
    us,
    ur,
    ds,
    dr,
    ts,
    tr,
):
    dp, z, x, core, y = place()
    c_dev, x_dev, y_dev = partners(dp, x, core, y)
    up_dev, down_dev = (dp + 4, y), (dp - 4, y)
    last = BLOCKS - 1

    def fetch(t, act):
        def both(a, b):
            slot = t % 2
            for copy in (
                pltpu.make_async_copy(a, left.at[slot], left_sem.at[slot]),
                pltpu.make_async_copy(b, right.at[slot], right_sem.at[slot]),
            ):
                act(copy)

        @pl.when(t < 4)
        def _():
            both(act_ref.at[t], gffn_ref.at[t // 2])

        @pl.when((t >= 4) & (t < 8))
        def _():
            both(gpre_ref.at[t - 4], fb_ref.at[(t - 4) // 2])

        @pl.when((t >= 8) & (t < 12))
        def _():
            both(x_ref, gproj_ref.at[t - 8])

        @pl.when((t >= 12) & (t < 14))
        def _():
            both(ctx_ref, gmix_ref.at[t - 12])

        @pl.when(t == 14)
        def _():
            both(dl_ref, gkc_ref)

    def c_copy(t):
        return send(part.at[t, :, :, 1 - core], rc.at[t], cs.at[t], cr.at[t], c_dev)

    def first_copy(t, by_y):
        if by_y:
            return send(part.at[t, :, :, core, 1 - y], r1.at[t], s1.at[t], q1.at[t], y_dev)
        return send(part.at[t, :, 1 - x, core], r1.at[t], s1.at[t], q1.at[t], x_dev)

    def second_copy(t, by_y):
        if by_y:
            return send(part.at[t, :, 1 - x, core, y], r2.at[t], s2.at[t], q2.at[t], x_dev)
        return send(part.at[t, :, x, core, 1 - y], r2.at[t], s2.at[t], q2.at[t], y_dev)

    def up_copy(t, bottom):
        source = part.at[t, :, x, core, y] if bottom else ru.at[t]
        return send(source, ru.at[t], us.at[t], ur.at[t], up_dev)

    def down_copy(t, top):
        source = part.at[t, :, x, core, y] if top else rd.at[t]
        return send(source, rd.at[t], ds.at[t], dr.at[t], down_dev)

    def t_copy(k):
        return send(tiny.at[k], got.at[k], ts.at[k], tr.at[k], (c_dev, x_dev, y_dev)[k])

    def t_line(d, way):
        return send(
            tiny.at[3],
            got.at[3 + z],
            ts.at[2 + d if way > 0 else 1 + depth + d],
            tr.at[3 + z],
            (dp + 4 * d * way, y),
        )

    def t_arrival(level):
        return send(tiny.at[3], got.at[3 + level], ts.at[0], tr.at[3 + level], c_dev)

    def add(into, other):
        return (into.astype(F32) + other.astype(F32)).astype(BF16)

    def parity(t, work):
        @pl.when(t % 2 == 0)
        def _():
            work(True)

        @pl.when(t % 2 == 1)
        def _():
            work(False)

    fetch(0, lambda copy: copy.start())
    lines = tuple((z >= d, (dp - 4 * d, y)) for d in range(1, depth)) + tuple(
        (z + d < depth, (dp + 4 * d, y)) for d in range(1, depth)
    )
    meet((c_dev, x_dev, y_dev), lines)
    tiny[0] = t_ref[...]
    t_copy(0).start()

    def multiply(t):
        @pl.when(t + 1 < last)
        def _():
            fetch(t + 1, lambda copy: copy.start())

        @pl.when(t < last)
        def _():
            fetch(t, lambda copy: copy.wait())
            slot = t % 2
            for c in range(2):
                block = tn(left[slot, :, c * W : (c + 1) * W], right[slot])
                half = depth // 2
                part[t, c * half : (c + 1) * half] = block.reshape(
                    (half,) + part.shape[2:]
                ).astype(BF16)

        @pl.when(t == last)
        def _():
            part[t] = small_ref[...]

        c_copy(t).start()

    def stage_core(t):
        c_copy(t).wait_recv()

        def level(j, carry):
            part[t, j, :, core] = add(part[t, j, :, core], rc[t, j])
            return carry

        lax.fori_loop(0, depth, level, 0)
        parity(t, lambda by_y: first_copy(t, by_y).start())

    def stage_first(t):
        def work(by_y):
            first_copy(t, by_y).wait_recv()
            if by_y:
                part[t, :, :, core, y] = add(part[t, :, :, core, y], r1[t])
            else:
                part[t, :, x, core] = add(part[t, :, x, core], r1[t])
            second_copy(t, by_y).start()

        parity(t, work)

    def stage_second(t):
        parity(t, lambda by_y: second_copy(t, by_y).wait_recv())
        part[t, :, x, core, y] = add(part[t, :, x, core, y], r2[t])
        o_ref[t] = part[t, z, x, core, y].astype(F32)

    def stage_up(t):
        @pl.when(z == 0)
        def _():
            up_copy(t, True).start()

        @pl.when(z > 0)
        def _():
            up_copy(t, False).wait_recv()
            o_ref[t] = o_ref[t] + ru[t, z].astype(F32)

        @pl.when((z > 0) & (z + 1 < depth))
        def _():
            ru[t] = add(ru[t], part[t, :, x, core, y])
            up_copy(t, False).start()

    def stage_down(t):
        @pl.when(z + 1 == depth)
        def _():
            down_copy(t, True).start()

        @pl.when(z + 1 < depth)
        def _():
            down_copy(t, False).wait_recv()
            o_ref[t] = o_ref[t] + rd[t, z].astype(F32)

        @pl.when((z > 0) & (z + 1 < depth))
        def _():
            rd[t] = add(rd[t], part[t, :, x, core, y])
            down_copy(t, False).start()

    def stage(t, work):
        @pl.when((t >= 0) & (t < BLOCKS))
        def _():
            work(t)

    def tick(t, carry):
        stage(t, multiply)
        stage(t - 1, stage_core)
        stage(t - 3, stage_first)
        stage(t - 5, stage_second)
        stage(t - 5 - z, stage_up)
        stage(t - 5 - (depth - 1 - z), stage_down)
        return carry

    lax.fori_loop(0, BLOCKS + 5 + depth, tick, 0)

    for k in range(3):
        t_copy(k).wait_recv()
        tiny[k + 1] = tiny[k] + got[k]
        if k < 2:
            t_copy(k + 1).start()
    for d in range(1, depth):

        @pl.when(z + d < depth)
        def _():
            t_line(d, 1).start()

        @pl.when(z >= d)
        def _():
            t_line(d, -1).start()

    for level in range(depth):

        @pl.when(z == level)
        def _():
            got[3 + level] = tiny[3]

        @pl.when(z != level)
        def _():
            t_arrival(level).wait_recv()

    total = got[3]
    for level in range(1, depth):
        total = total + got[3 + level]
    u_ref[...] = total

    for d in range(1, depth):

        @pl.when(z + d < depth)
        def _():
            t_line(d, 1).wait_send()

        @pl.when(z >= d)
        def _():
            t_line(d, -1).wait_send()

    for k in range(3):
        t_copy(k).wait_send()

    def finish(t, carry):
        c_copy(t).wait_send()
        parity(t, lambda by_y: first_copy(t, by_y).wait_send())
        parity(t, lambda by_y: second_copy(t, by_y).wait_send())

        @pl.when(z + 1 < depth)
        def _():
            up_copy(t, False).wait_send()

        @pl.when(z > 0)
        def _():
            down_copy(t, False).wait_send()

        return carry

    lax.fori_loop(0, BLOCKS, finish, 0)


def scatter_all(factors, small, tiny, mesh):
    dp, fsdp = mesh.shape["dp"], mesh.shape["fsdp"]
    rows = D // (dp * fsdp)
    if fsdp != 2 or dp % 4:
        local = weight_grads(*factors, small)
        shard = lax.psum_scatter(
            local.reshape(BLOCKS, dp * fsdp, rows, W),
            ("dp", "fsdp"),
            scatter_dimension=1,
            tiled=False,
        )
        return shard.astype(F32), lax.psum(tiny, ("dp", "fsdp"))
    depth = dp // 4
    tokens = factors[0].shape[0]
    dma = pltpu.SemaphoreType.DMA
    anywhere = pl.BlockSpec(memory_space=pl.ANY)
    inside = pl.BlockSpec(memory_space=pltpu.VMEM)
    return pl.pallas_call(
        functools.partial(scatter_kernel, depth),
        out_shape=(
            jax.ShapeDtypeStruct((BLOCKS, rows, W), F32),
            jax.ShapeDtypeStruct((8, 128), F32),
        ),
        in_specs=[anywhere] * len(factors) + [inside, inside],
        out_specs=(inside, inside),
        scratch_shapes=[
            pltpu.VMEM((2, tokens, D), BF16),
            pltpu.VMEM((2, tokens, W), BF16),
            pltpu.VMEM((BLOCKS, depth, 2, 2, 2, rows, W), BF16),
            pltpu.VMEM((BLOCKS, depth, 2, 2, rows, W), BF16),
            pltpu.VMEM((BLOCKS, depth, 2, rows, W), BF16),
            pltpu.VMEM((BLOCKS, depth, rows, W), BF16),
            pltpu.VMEM((BLOCKS, depth, rows, W), BF16),
            pltpu.VMEM((BLOCKS, depth, rows, W), BF16),
            pltpu.VMEM((4, 8, 128), F32),
            pltpu.VMEM((3 + depth, 8, 128), F32),
            dma((2,)),
            dma((2,)),
        ]
        + [dma((BLOCKS,))] * 10
        + [dma((1 + 2 * depth,)), dma((3 + depth,))],
        compiler_params=pltpu.CompilerParams(
            collective_id=1, has_side_effects=True, vmem_limit_bytes=60 * 1024 * 1024
        ),
        name="scatter_all",
    )(*factors, small.reshape(depth, 2, 2, 2, rows, W), tiny)


def body(
    mesh,
    hidden,
    lengths,
    in_weight,
    depth_kernel,
    point_weight,
    kernel_weight,
    out_weight,
    up_weight,
    down_weight,
    norm_gains,
    norm_biases,
    out_grad,
):
    full = gather_all(
        pack(
            in_weight,
            depth_kernel,
            point_weight,
            kernel_weight,
            out_weight,
            up_weight,
            down_weight,
            norm_gains,
            norm_biases,
        ),
        mesh,
    )
    output, input_grad, factors, small, tiny = layer(hidden, lengths, full, out_grad)
    shard, totals = scatter_all(factors, small, tiny, mesh)
    rms = jnp.sqrt(totals[0, :4] / (totals[0, 4] * D))
    return (output, input_grad) + unpack(shard) + (rms,)


def solution(mesh):
    in_specs = (
        P(("dp", "fsdp"), None, None),
        P(("dp", "fsdp")),
        P(("dp", "fsdp"), None),
        P(None, ("dp", "fsdp")),
        P(("dp", "fsdp"), None),
        P(None, ("dp", "fsdp")),
        P(("dp", "fsdp"), None),
        P(None, None, ("dp", "fsdp")),
        P(None, ("dp", "fsdp"), None),
        P(None, ("dp", "fsdp")),
        P(None, ("dp", "fsdp")),
        P(("dp", "fsdp"), None, None),
    )
    out_specs = (
        P(("dp", "fsdp"), None, None),
        P(("dp", "fsdp"), None, None),
        P(("dp", "fsdp"), None),
        P(None, ("dp", "fsdp")),
        P(("dp", "fsdp"), None),
        P(None, ("dp", "fsdp")),
        P(("dp", "fsdp"), None),
        P(None, None, ("dp", "fsdp")),
        P(None, ("dp", "fsdp"), None),
        P(None, ("dp", "fsdp")),
        P(None, ("dp", "fsdp")),
        P(),
    )
    return jax.shard_map(functools.partial(body, mesh), mesh=mesh, in_specs=in_specs, out_specs=out_specs, check_vma=False)
```

```python
import functools
import math

import jax
import jax.numpy as jnp
from jax import lax
from jax.experimental import pallas as pl
from jax.experimental.pallas import tpu as pltpu
from jax.sharding import PartitionSpec as P

D = 768
HEADS = 6
HD = 64
G = 2
K = 9
SEQ = 512


EPSILON = 1e-06
MESH = pl.DeviceIdType.MESH
BLOCKS = 16
HALF = BLOCKS // 2


def place():
    dp, y = lax.axis_index("dp"), lax.axis_index("fsdp")
    return dp, dp // 4, (dp // 2) % 2, dp % 2, y


def partners(dp, x, core, y):
    return (dp + 1 - 2 * core, y), (dp + 2 - 4 * x, y), (dp, 1 - y)


def meet(peers, others):
    barrier = pltpu.get_barrier_semaphore()
    for peer in peers:
        pl.semaphore_signal(barrier, inc=1, device_id=peer, device_id_type=MESH)
    count = len(peers)
    for there, peer in others:

        @pl.when(there)
        def _():
            pl.semaphore_signal(barrier, inc=1, device_id=peer, device_id_type=MESH)

        count = count + there.astype(jnp.int32)
    pl.semaphore_wait(barrier, count)


def send(src, dst, send_sem, recv_sem, device):
    return pltpu.make_async_remote_copy(
        src_ref=src,
        dst_ref=dst,
        send_sem=send_sem,
        recv_sem=recv_sem,
        device_id=device,
        device_id_type=MESH,
    )


def gather_kernel(
    depth, p_ref, g_ref, own_sem, zs, zr, xs, xr, ys, yr, ds, dr, cs, cr
):
    dp, z, x, core, y = place()
    c_dev, x_dev, y_dev = partners(dp, x, core, y)
    up_dev, down_dev = (dp + 4, y), (dp - 4, y)
    own = pltpu.make_async_copy(p_ref, g_ref.at[:, z, x, core, y], own_sem)
    own.start()
    meet((c_dev, x_dev, y_dev), ((z + 1 < depth, up_dev), (z > 0, down_dev)))
    own.wait()
    steps = 2 * depth - 1

    def target(q):
        return z + ((q + 1) // 2) * (1 - 2 * (q % 2))

    def z_copy(j, way, device):
        slab = g_ref.at[:, j, x, core, y]
        return send(slab, slab, zs.at[way, j], zr.at[j], device)

    def x_copy(j):
        slab = g_ref.at[:, j, x, core, y]
        return send(slab, slab, xs.at[j], xr.at[j], x_dev)

    def y_copy(j):
        slab = g_ref.at[:, j, x, core, y]
        return send(slab, slab, ys.at[j], yr.at[j], y_dev)

    def d_copy(j, half):
        if half == 0:
            slab = g_ref.at[pl.ds(0, HALF), j, 1 - x, core, y]
            return send(slab, slab, ds.at[0, j], dr.at[0, j], y_dev)
        slab = g_ref.at[pl.ds(HALF, HALF), j, x, core, 1 - y]
        return send(slab, slab, ds.at[1, j], dr.at[1, j], x_dev)

    def c_copy(j, a, b):
        slab = g_ref.at[:, j, (x + a) % 2, core, (y + b) % 2]
        return send(slab, slab, cs.at[2 * a + b, j], cr.at[2 * a + b, j], c_dev)

    def c_arrival(j, a, b):
        slab = g_ref.at[:, j, (x + a) % 2, 1 - core, (y + b) % 2]
        return send(slab, slab, cs.at[2 * a + b, j], cr.at[2 * a + b, j], c_dev)

    def x_arrival(j):
        slab = g_ref.at[:, j, 1 - x, core, y]
        return send(slab, slab, xs.at[j], xr.at[j], x_dev)

    def y_arrival(j):
        slab = g_ref.at[:, j, x, core, 1 - y]
        return send(slab, slab, ys.at[j], yr.at[j], y_dev)

    def d_arrival(j, half):
        slab = g_ref.at[pl.ds(half * HALF, HALF), j, 1 - x, core, 1 - y]
        return send(slab, slab, ds.at[half, j], dr.at[half, j], y_dev if half == 0 else x_dev)

    def first(j):
        @pl.when(j != z)
        def _():
            z_copy(j, 0, up_dev).wait_recv()

        @pl.when((j <= z) & (z + 1 < depth))
        def _():
            z_copy(j, 0, up_dev).start()

        @pl.when((j >= z) & (z > 0))
        def _():
            z_copy(j, 1, down_dev).start()

        x_copy(j).start()
        y_copy(j).start()
        c_copy(j, 0, 0).start()

    def second(j):
        x_arrival(j).wait_recv()
        d_copy(j, 0).start()
        c_copy(j, 1, 0).start()
        y_arrival(j).wait_recv()
        d_copy(j, 1).start()
        c_copy(j, 0, 1).start()

    def third(j):
        d_arrival(j, 0).wait_recv()
        d_arrival(j, 1).wait_recv()
        c_copy(j, 1, 1).start()

    def stage(q, work):
        j = target(q)

        @pl.when((q >= 0) & (q < steps) & (j >= 0) & (j < depth))
        def _():
            work(j)

    def step(q, carry):
        stage(q, first)
        stage(q - 1, second)
        stage(q - 2, third)
        return carry

    lax.fori_loop(0, steps + 2, step, 0)

    def finish(j, carry):
        for a in range(2):
            for b in range(2):
                c_arrival(j, a, b).wait_recv()
                c_copy(j, a, b).wait_send()
        x_copy(j).wait_send()
        y_copy(j).wait_send()
        d_copy(j, 0).wait_send()
        d_copy(j, 1).wait_send()

        @pl.when((j <= z) & (z + 1 < depth))
        def _():
            z_copy(j, 0, up_dev).wait_send()

        @pl.when((j >= z) & (z > 0))
        def _():
            z_copy(j, 1, down_dev).wait_send()

        return carry

    lax.fori_loop(0, depth, finish, 0)


def gather_all(packed, mesh):
    dp, fsdp = mesh.shape["dp"], mesh.shape["fsdp"]
    _, rows, width = packed.shape
    if fsdp != 2 or dp % 4:
        full = lax.all_gather(packed, ("dp", "fsdp"), axis=1, tiled=False)
        return full.reshape(BLOCKS, dp * fsdp * rows, width)
    depth = dp // 4
    dma = pltpu.SemaphoreType.DMA
    full = pl.pallas_call(
        functools.partial(gather_kernel, depth),
        out_shape=jax.ShapeDtypeStruct((BLOCKS, depth, 2, 2, 2, rows, width), packed.dtype),
        in_specs=[pl.BlockSpec(memory_space=pltpu.VMEM)],
        out_specs=pl.BlockSpec(memory_space=pl.ANY),
        scratch_shapes=[
            dma(()),
            dma((2, depth)),
            dma((depth,)),
            dma((depth,)),
            dma((depth,)),
            dma((depth,)),
            dma((depth,)),
            dma((2, depth)),
            dma((2, depth)),
            dma((4, depth)),
            dma((4, depth)),
        ],
        compiler_params=pltpu.CompilerParams(collective_id=0, has_side_effects=True),
        name="gather_all",
    )(packed)
    return full.reshape(BLOCKS, dp * fsdp * rows, width)


W = D // G
F32, BF16 = jnp.float32, jnp.bfloat16
PAD = 8


def nn(a, b):
    return lax.dot_general(a, b, (((1,), (0,)), ((), ())), preferred_element_type=F32)


def nt(a, b):
    return lax.dot_general(a, b, (((1,), (1,)), ((), ())), preferred_element_type=F32)


def tn(a, b):
    return lax.dot_general(a, b, (((0,), (0,)), ((), ())), preferred_element_type=F32)


def spread(rows):
    head = lax.broadcasted_iota(jnp.int32, (rows, W), 0) % 8
    channel = lax.broadcasted_iota(jnp.int32, (rows, W), 1) // HD
    return (head == channel).astype(F32).astype(BF16)


def forward_kernel(
    len_ref,
    hid_ref,
    win_ref,
    wpt_ref,
    depth_ref,
    kmt_ref,
    x_ref,
    proj_ref,
    dl_ref,
    kc_ref,
    wt_ref,
    lse_ref,
    ctx_ref,
    xs,
    sv,
    ot,
):
    length = len_ref[pl.program_id(0)]
    inside = lax.broadcasted_iota(jnp.int32, (SEQ, 1), 0) < length
    x = jnp.where(inside, hid_ref[0], jnp.zeros((), BF16))
    x_ref[0] = x
    xs[0:PAD] = jnp.zeros((PAD, D), F32)
    xs[PAD + SEQ :] = jnp.zeros((PAD, D), F32)
    xs[PAD : PAD + SEQ] = x.astype(F32)
    sv[0:PAD] = jnp.zeros((PAD, W), F32)
    sv[PAD + SEQ :] = jnp.zeros((PAD, W), F32)

    for b in range(4):
        part = nn(x_ref[0], win_ref[b]).astype(BF16)
        proj_ref[0, :, b * W : (b + 1) * W] = part
        if b == 3:
            sv[PAD : PAD + SEQ] = part.astype(F32)

    def column(c, carry):
        lane = pl.ds(pl.multiple_of(c * 128, 128), 128)
        for r in range(8):
            total = jnp.zeros((64, 128), F32)
            for k in range(K):
                start = PAD + r * 64 + k - K // 2
                total = total + xs[start : start + 64, lane] * depth_ref[k : k + 1, lane]
            dl_ref[0, r * 64 : (r + 1) * 64, lane] = total.astype(BF16)
        return carry

    lax.fori_loop(0, D // 128, column, 0)
    kc_ref[0] = nn(dl_ref[0], wpt_ref[0])
    mk = (kc_ref[0] * proj_ref[0, :, 0:W].astype(F32)).astype(BF16)
    logits = nt(kmt_ref[...], mk)
    top = logits[0:8]
    for k in range(1, K):
        top = jnp.maximum(top, logits[k * 8 : k * 8 + 8])
    parts = [jnp.exp(logits[k * 8 : k * 8 + 8] - top) for k in range(K)]
    inverse = 1.0 / sum(parts)
    both = []
    for k in range(K):
        weight = parts[k] * inverse
        wt_ref[0, k * 8 : k * 8 + 8] = weight
        high = weight.astype(BF16).astype(F32)
        both.append(jnp.concatenate([high, weight - high], axis=0).astype(BF16))
    e16 = spread(16)
    for r in range(4):
        total = jnp.zeros((128, W), F32)
        for k in range(K):
            start = PAD + r * 128 + k - K // 2
            total = total + tn(both[k][:, r * 128 : (r + 1) * 128], e16) * sv[start : start + 128]
        ctx_ref[0, r * 128 : (r + 1) * 128, W:] = total.astype(BF16)

    lane_head = lax.broadcasted_iota(jnp.int32, (1, 128), 1) // HD
    bias = jnp.where(inside, 0.0, -1e30).astype(F32)

    def pair(p, carry):
        def slab(part):
            return proj_ref[0, :, pl.ds(pl.multiple_of(part * W + p * 128, 128), 128)]

        q2, k2, v2 = slab(0), slab(1), slab(2)
        for h in range(2):
            scale = jnp.where(lane_head == h, 1.0 / math.sqrt(HD), 0.0).astype(BF16)
            scores = nt(k2, q2 * scale) + bias
            peak = jnp.max(scores, axis=0, keepdims=True)
            power = jnp.exp(scores - peak)
            total = jnp.sum(power, axis=0, keepdims=True)
            lse_ref[0, pl.ds(p * 2 + h, 1)] = peak + jnp.log(total)
            probs = (power * (1.0 / total)).astype(BF16)
            ot[h * HD : (h + 1) * HD] = tn(v2, probs)[h * HD : (h + 1) * HD]
        ctx_ref[0, :, pl.ds(pl.multiple_of(p * 128, 128), 128)] = ot[...].T.astype(BF16)
        return carry

    lax.fori_loop(0, HEADS // 2, pair, 0)


def forward(lengths, hidden, full, depth, kmt):
    rows = hidden.shape[0]

    def per_row(*shape):
        return pl.BlockSpec((1,) + shape, lambda r: (r, 0, 0))

    def out(dtype, *shape):
        return jax.ShapeDtypeStruct((rows,) + shape, dtype)

    return pl.pallas_call(
        forward_kernel,
        grid=(rows,),
        out_shape=(
            out(BF16, SEQ, D),
            out(BF16, SEQ, 4 * W),
            out(BF16, SEQ, D),
            out(F32, SEQ, W),
            out(F32, 8 * K, SEQ),
            out(F32, 8, SEQ),
            out(BF16, SEQ, D),
        ),
        in_specs=[
            pl.BlockSpec(memory_space=pltpu.SMEM),
            per_row(SEQ, D),
            pl.BlockSpec((4, D, W), lambda r: (2, 0, 0)),
            pl.BlockSpec((1, D, W), lambda r: (14, 0, 0)),
            pl.BlockSpec((16, D), lambda r: (0, 0)),
            pl.BlockSpec((8 * K, W), lambda r: (0, 0)),
        ],
        out_specs=(
            per_row(SEQ, D),
            per_row(SEQ, 4 * W),
            per_row(SEQ, D),
            per_row(SEQ, W),
            per_row(8 * K, SEQ),
            per_row(8, SEQ),
            per_row(SEQ, D),
        ),
        scratch_shapes=[
            pltpu.VMEM((SEQ + 2 * PAD, D), F32),
            pltpu.VMEM((SEQ + 2 * PAD, W), F32),
            pltpu.VMEM((128, SEQ), F32),
        ],
        compiler_params=pltpu.CompilerParams(vmem_limit_bytes=56 * 1024 * 1024),
        name="mixer_forward",
    )(lengths, hidden, full, full, depth, kmt)


TILE = 256
CHUNK = 16
PART = 256


def ffn_kernel(
    len_ref,
    ctx_ref,
    x_ref,
    og_ref,
    wout_ref,
    wdn_ref,
    wup_ref,
    gb_ref,
    y_ref,
    act_ref,
    gpre_ref,
    fb_ref,
    gffn_ref,
    gmix_ref,
    gr1_ref,
    gctx_ref,
    stat_ref,
    mix,
    first,
    n1,
    inv,
    ffn,
    pre,
    dg,
    gr2,
):
    step = pl.program_id(0)
    row = step // (SEQ // TILE)
    base = (step % (SEQ // TILE)) * TILE
    left = len_ref[row] - base

    @pl.when(step == 0)
    def _():
        stat_ref[...] = jnp.zeros_like(stat_ref)

    for b in range(2):
        mix[:, b * W : (b + 1) * W] = nn(ctx_ref[...], wout_ref[b])

    def mask_of(i):
        return (lax.broadcasted_iota(jnp.int32, (CHUNK, 1), 0) + i * CHUNK < left).astype(F32)

    def fold(values):
        return jnp.sum(values.reshape(CHUNK // 8, 8, D), axis=0)

    def tally(k, values):
        stat_ref[k] = stat_ref[k] + fold(values)

    def rows_of(i):
        return pl.ds(pl.multiple_of(i * CHUNK, CHUNK), CHUNK)

    def norm(values):
        average = jnp.mean(values, axis=-1, keepdims=True)
        centered = values - average
        inverse = lax.rsqrt(jnp.mean(centered * centered, axis=-1, keepdims=True) + EPSILON)
        return centered * inverse, inverse

    def norm_back(grad, normed, inverse, gain):
        scaled = grad * gain
        mean = jnp.mean(scaled, axis=-1, keepdims=True)
        other = jnp.mean(scaled * normed, axis=-1, keepdims=True)
        return inverse * (scaled - mean - normed * other)

    def norm_one(i, carry):
        rows = rows_of(i)
        xf, mixed = x_ref[rows].astype(F32), mix[rows]
        normed, inverse = norm(xf + mixed)
        result = normed * gb_ref[0:1] + gb_ref[2:3]
        n1[rows] = normed
        inv[rows] = jnp.broadcast_to(inverse, (CHUNK, 128))
        first[rows] = result
        for g in range(G):
            fb_ref[g, rows] = result[:, g * W : (g + 1) * W].astype(BF16)
        tally(0, xf * xf)
        tally(1, mixed * mixed * mask_of(i))
        return carry

    lax.fori_loop(0, TILE // CHUNK, norm_one, 0)

    def part_of(c):
        return c // 3, pl.ds(c % 3 * PART, PART)

    def expand(c):
        s, units = part_of(c)
        pre[c % 2] = nt(fb_ref[s // 2], wup_ref[s, units])

    def gelu(c):
        s, units = part_of(c)
        for r in range(TILE // 32):
            rows = slice(r * 32, (r + 1) * 32)
            v = pre[c % 2, rows]
            phi = 0.5 + 0.5 * lax.erf(v * math.sqrt(0.5))
            act_ref[s, rows, units] = (v * phi).astype(BF16)
            dg[s, rows, units] = phi + v * jnp.exp(v * v * -0.5) * (1.0 / math.sqrt(2.0 * math.pi))

    def contract(s):
        g = s // 2
        part = nn(act_ref[s], wdn_ref[s])
        lanes = slice(g * W, (g + 1) * W)
        if s % 2 == 0:
            ffn[:, lanes] = part
        else:
            ffn[:, lanes] += part

    parts = 4 * D // PART
    expand(0)
    for c in range(parts):
        if c + 1 < parts:
            expand(c + 1)
        if c % 3 == 0 and c > 0:
            contract(c // 3 - 1)
        gelu(c)
    contract(3)

    def norm_two(i, carry):
        rows = rows_of(i)
        mask = mask_of(i)
        out = ffn[rows]
        normed, inverse = norm(first[rows] + out)
        y = (normed * gb_ref[1:2] + gb_ref[3:4]) * mask
        y_ref[rows] = y.astype(BF16)
        grad = og_ref[rows].astype(F32) * mask
        back = norm_back(grad, normed, inverse, gb_ref[1:2])
        gr2[rows] = back
        for g in range(G):
            gffn_ref[g, rows] = back[:, g * W : (g + 1) * W].astype(BF16)
        tally(2, out * out * mask)
        tally(3, y * y)
        tally(5, grad * normed)
        tally(7, grad)
        return carry

    lax.fori_loop(0, TILE // CHUNK, norm_two, 0)

    for c in range(parts):
        s, units = part_of(c)
        gpre_ref[s, :, units] = (nt(gffn_ref[s // 2], wdn_ref[s, units]) * dg[s, :, units]).astype(BF16)
        if c % 3 == 2:
            lanes = slice(s // 2 * W, (s // 2 + 1) * W)
            gr2[:, lanes] += nn(gpre_ref[s], wup_ref[s])

    def norm_one_back(i, carry):
        rows = rows_of(i)
        grad, normed = gr2[rows], n1[rows]
        back = norm_back(grad, normed, inv[rows, 0:1], gb_ref[0:1])
        gr1_ref[rows] = back
        for g in range(2):
            gmix_ref[g, rows] = back[:, g * W : (g + 1) * W].astype(BF16)
        tally(4, grad * normed)
        tally(6, grad)
        return carry

    lax.fori_loop(0, TILE // CHUNK, norm_one_back, 0)
    gctx_ref[...] = (
        nt(gmix_ref[0], wout_ref[0]) + nt(gmix_ref[1], wout_ref[1])
    ).astype(BF16)


def feed_forward(lengths, ctx, x, out_grad, full, gb):
    tokens = x.shape[0]

    def per_tile(width):
        return pl.BlockSpec((TILE, width), lambda i: (i, 0))

    def out(dtype, width):
        return jax.ShapeDtypeStruct((tokens, width), dtype)

    def slabs(count, width):
        return pl.BlockSpec((count, TILE, width), lambda i: (0, i, 0))

    def slabs_out(count, width):
        return jax.ShapeDtypeStruct((count, tokens, width), BF16)

    return pl.pallas_call(
        ffn_kernel,
        grid=(tokens // TILE,),
        out_shape=(
            out(BF16, D),
            slabs_out(4, D),
            slabs_out(4, D),
            slabs_out(G, W),
            slabs_out(G, W),
            slabs_out(2, W),
            out(F32, D),
            out(BF16, D),
            jax.ShapeDtypeStruct((8, 8, D), F32),
        ),
        in_specs=[
            pl.BlockSpec(memory_space=pltpu.SMEM),
            per_tile(D),
            per_tile(D),
            per_tile(D),
            pl.BlockSpec((2, D, W), lambda i: (6, 0, 0)),
            pl.BlockSpec((4, D, W), lambda i: (0, 0, 0)),
            pl.BlockSpec((4, D, W), lambda i: (1, 0, 0)),
            pl.BlockSpec((8, D), lambda i: (0, 0)),
        ],
        out_specs=(
            per_tile(D),
            slabs(4, D),
            slabs(4, D),
            slabs(G, W),
            slabs(G, W),
            slabs(2, W),
            per_tile(D),
            per_tile(D),
            pl.BlockSpec((8, 8, D), lambda i: (0, 0, 0)),
        ),
        scratch_shapes=[
            pltpu.VMEM((TILE, D), F32),
            pltpu.VMEM((TILE, D), F32),
            pltpu.VMEM((TILE, D), F32),
            pltpu.VMEM((TILE, 128), F32),
            pltpu.VMEM((TILE, D), F32),
            pltpu.VMEM((2, TILE, PART), F32),
            pltpu.VMEM((4, TILE, D), F32),
            pltpu.VMEM((TILE, D), F32),
        ],
        compiler_params=pltpu.CompilerParams(vmem_limit_bytes=56 * 1024 * 1024),
        name="feed_forward",
    )(lengths, ctx, x, out_grad, full, full, full, gb)


def backward_kernel(
    len_ref,
    x_ref,
    proj_ref,
    dl_ref,
    kc_ref,
    wt_ref,
    lse_ref,
    gctx_ref,
    gr1_ref,
    win_ref,
    wpt_ref,
    depth_ref,
    kmt_ref,
    gproj_ref,
    gkc_ref,
    gin_ref,
    gkm_ref,
    gdk_ref,
    sv,
    gc,
    xs,
    gd,
    gs,
    gq,
    gt,
    dqt,
):
    row = pl.program_id(0)
    length = len_ref[row]
    inside = lax.broadcasted_iota(jnp.int32, (SEQ, 1), 0) < length

    @pl.when(row == 0)
    def _():
        gkm_ref[...] = jnp.zeros_like(gkm_ref)
        gdk_ref[...] = jnp.zeros_like(gdk_ref)

    for ref, width in ((sv, W), (gc, W), (xs, D), (gd, D)):
        ref[0:PAD] = jnp.zeros((PAD, width), F32)
        ref[PAD + SEQ :] = jnp.zeros((PAD, width), F32)
    sv[PAD : PAD + SEQ] = proj_ref[0, :, 3 * W :].astype(F32)
    gc[PAD : PAD + SEQ] = gctx_ref[0, :, W:].astype(F32)
    xs[PAD : PAD + SEQ] = x_ref[0].astype(F32)

    e16 = spread(16)
    place_row = lax.broadcasted_iota(jnp.int32, (W, 128), 0) // HD
    place_col = lax.broadcasted_iota(jnp.int32, (W, 128), 1)
    both = []
    for k in range(K):
        weight = pltpu.roll(wt_ref[0, k * 8 : k * 8 + 8], (k - K // 2) % SEQ, 1)
        high = weight.astype(BF16).astype(F32)
        both.append(jnp.concatenate([high, weight - high], axis=0).astype(BF16))
    for r in range(4):
        rows = slice(r * 128, (r + 1) * 128)
        spans = jnp.zeros((128, 128), F32)
        total = jnp.zeros((128, W), F32)
        for k in range(K):
            start = PAD + r * 128 + k - K // 2
            product_k = gc[PAD + r * 128 : PAD + (r + 1) * 128] * sv[start : start + 128]
            chosen = (place_col == place_row + 8 * k).astype(F32).astype(BF16)
            spans = spans + nn(product_k.astype(BF16), chosen)
            start = PAD + r * 128 - k + K // 2
            total = total + tn(both[k][:, rows], e16) * gc[start : start + 128]
        gt[:, rows] = spans.T
        gproj_ref[3, rows] = total.astype(BF16)
    center = jnp.zeros((8, SEQ), F32)
    for k in range(K):
        center = center + wt_ref[0, k * 8 : k * 8 + 8] * gt[k * 8 : k * 8 + 8]
    glt = jnp.concatenate(
        [
            wt_ref[0, k * 8 : k * 8 + 8] * (gt[k * 8 : k * 8 + 8] - center)
            for k in range(K)
        ],
        axis=0,
    ).astype(BF16)
    query = proj_ref[0, :, 0:W].astype(F32)
    mk = (kc_ref[0] * query).astype(BF16)
    gkm_ref[...] += nn(glt, mk)
    mixed = tn(glt, kmt_ref[...])
    gkc_ref[0] = (mixed * query).astype(BF16)
    gq[...] = mixed * kc_ref[0]
    gd[PAD : PAD + SEQ] = nt(gkc_ref[0], wpt_ref[0])

    def column(c, carry):
        lane = pl.ds(pl.multiple_of(c * 128, 128), 128)
        sums = [jnp.zeros((8, 128), F32)] * K
        for r in range(8):
            total = jnp.zeros((64, 128), F32)
            center = PAD + r * 64
            grad = gd[center : center + 64, lane]
            for k in range(K):
                start = center + k - K // 2
                sums[k] = sums[k] + jnp.sum(
                    (xs[start : start + 64, lane] * grad).reshape(8, 8, 128), axis=0
                )
                start = center - k + K // 2
                total = total + gd[start : start + 64, lane] * depth_ref[k : k + 1, lane]
            gs[r * 64 : (r + 1) * 64, lane] = total
        for k in range(K):
            gdk_ref[k, :, lane] = gdk_ref[k, :, lane] + sums[k]
        return carry

    lax.fori_loop(0, D // 128, column, 0)

    lane_head = lax.broadcasted_iota(jnp.int32, (1, 128), 1) // HD
    bias = jnp.where(inside, 0.0, -1e30).astype(F32)

    def pair(p, carry):
        def lanes(part):
            return pl.ds(pl.multiple_of(part * W + p * 128, 128), 128)

        q2, k2, v2 = (proj_ref[0, :, lanes(part)] for part in range(3))
        g2 = gctx_ref[0, :, lanes(0)]
        results = []
        for h in range(2):
            mine = lane_head == h
            scale = jnp.where(mine, 1.0 / math.sqrt(HD), 0.0).astype(BF16)
            scores = nt(k2, q2 * scale) + bias
            probs = jnp.exp(scores - lse_ref[0, pl.ds(p * 2 + h, 1)])
            grads = nt(v2 * jnp.where(mine, 1.0, 0.0).astype(BF16), g2)
            correction = jnp.sum(probs * grads, axis=0, keepdims=True)
            grad_scores = (probs * (grads - correction)).astype(BF16)
            dqt[h * HD : (h + 1) * HD] = tn(k2, grad_scores)[h * HD : (h + 1) * HD]
            results.append((nn(grad_scores, q2), nn(probs.astype(BF16), g2)))
        low = lane_head == 0
        scale = 1.0 / math.sqrt(HD)
        gproj_ref[0, :, lanes(0)] = (dqt[...].T * scale + gq[:, lanes(0)]).astype(BF16)
        gproj_ref[1, :, lanes(0)] = (jnp.where(low, results[0][0], results[1][0]) * scale).astype(BF16)
        gproj_ref[2, :, lanes(0)] = jnp.where(low, results[0][1], results[1][1]).astype(BF16)
        return carry

    lax.fori_loop(0, HEADS // 2, pair, 0)

    for b in range(4):
        gs[...] += nt(gproj_ref[b], win_ref[b])
    gin_ref[0] = jnp.where(inside, gr1_ref[0] + gs[...], 0.0).astype(BF16)


def backward(lengths, x, proj, dl, kc, wt, lse, gctx, gr1, full, depth, kmt):
    rows = x.shape[0]

    def per_row(*shape):
        return pl.BlockSpec((1,) + shape, lambda r: (r, 0, 0))

    def out(dtype, *shape):
        return jax.ShapeDtypeStruct((rows,) + shape, dtype)

    return pl.pallas_call(
        backward_kernel,
        grid=(rows,),
        out_shape=(
            jax.ShapeDtypeStruct((4, rows * SEQ, W), BF16),
            out(BF16, SEQ, W),
            out(BF16, SEQ, D),
            jax.ShapeDtypeStruct((8 * K, W), F32),
            jax.ShapeDtypeStruct((K, 8, D), F32),
        ),
        in_specs=[
            pl.BlockSpec(memory_space=pltpu.SMEM),
            per_row(SEQ, D),
            per_row(SEQ, 4 * W),
            per_row(SEQ, D),
            per_row(SEQ, W),
            per_row(8 * K, SEQ),
            per_row(8, SEQ),
            per_row(SEQ, D),
            per_row(SEQ, D),
            pl.BlockSpec((4, D, W), lambda r: (2, 0, 0)),
            pl.BlockSpec((1, D, W), lambda r: (14, 0, 0)),
            pl.BlockSpec((16, D), lambda r: (0, 0)),
            pl.BlockSpec((8 * K, W), lambda r: (0, 0)),
        ],
        out_specs=(
            pl.BlockSpec((4, SEQ, W), lambda r: (0, r, 0)),
            per_row(SEQ, W),
            per_row(SEQ, D),
            pl.BlockSpec((8 * K, W), lambda r: (0, 0)),
            pl.BlockSpec((K, 8, D), lambda r: (0, 0, 0)),
        ),
        scratch_shapes=[
            pltpu.VMEM((SEQ + 2 * PAD, W), F32),
            pltpu.VMEM((SEQ + 2 * PAD, W), F32),
            pltpu.VMEM((SEQ + 2 * PAD, D), F32),
            pltpu.VMEM((SEQ + 2 * PAD, D), F32),
            pltpu.VMEM((SEQ, D), F32),
            pltpu.VMEM((SEQ, W), F32),
            pltpu.VMEM((128, SEQ), F32),
            pltpu.VMEM((128, SEQ), F32),
        ],
        compiler_params=pltpu.CompilerParams(vmem_limit_bytes=56 * 1024 * 1024),
        name="mixer_backward",
    )(lengths, x, proj, dl, kc, wt, lse, gctx, gr1, full, full, depth, kmt)


def pack(in_weight, depth_kernel, point_weight, kernel_weight, out_weight, up_weight, down_weight, norm_gains, norm_biases):
    rows = in_weight.shape[0]

    def halves(grouped):
        return grouped.reshape(G * 2, rows, W)

    kernel = kernel_weight.reshape(K, rows, 3).transpose(1, 0, 2).reshape(rows, 3 * K)
    small = jnp.concatenate([depth_kernel.T, kernel, norm_gains.T, norm_biases.T], axis=1)
    small = jnp.pad(small, ((0, 0), (0, W - small.shape[1])))
    return jnp.concatenate(
        [
            halves(down_weight),
            halves(up_weight.transpose(0, 2, 1)),
            in_weight.reshape(rows, 4, W).transpose(1, 0, 2),
            out_weight.reshape(rows, 2, W).transpose(1, 0, 2),
            point_weight[None],
            small[None],
        ],
        axis=0,
    )


def unpack(shard):
    rows = shard.shape[1]
    small = shard[15]
    kernel = small[:, K : 4 * K].reshape(rows, K, 3).transpose(1, 0, 2).reshape(K, 3 * rows)
    return (
        shard[8:12].transpose(1, 0, 2).reshape(rows, 4 * W),
        small[:, :K].T,
        shard[14],
        kernel,
        shard[12:14].transpose(1, 0, 2).reshape(rows, 2 * W),
        shard[4:8].reshape(G, 2 * rows, W).transpose(0, 2, 1),
        shard[0:4].reshape(G, 2 * rows, W),
        small[:, 4 * K : 4 * K + 2].T,
        small[:, 4 * K + 2 : 4 * K + 4].T,
    )


def layer(hidden, lengths, full, out_grad):
    rows = hidden.shape[0]
    tokens = rows * SEQ
    small = full[15].astype(F32)
    depth = jnp.pad(small[:, :K].T, ((0, 16 - K), (0, 0)))
    kernel = small[:, K : 4 * K].reshape(D, K, 3).transpose(1, 0, 2).reshape(K, W, HEADS)
    kmt = jnp.pad(kernel.transpose(0, 2, 1), ((0, 0), (0, 8 - HEADS), (0, 0)))
    kmt = kmt.reshape(8 * K, W).astype(BF16)
    gb = jnp.pad(small[:, 4 * K : 4 * K + 4].T, ((0, 4), (0, 0)))

    x, proj, dl, kc, wt, lse, ctx = forward(lengths, hidden, full, depth, kmt)
    flat_x, flat_ctx = x.reshape(tokens, D), ctx.reshape(tokens, D)
    y, act, gpre, fb, gffn, gmix, gr1, gctx, stat = feed_forward(
        lengths, flat_ctx, flat_x, out_grad.reshape(tokens, D), full, gb
    )
    gproj, gkc, gin, gkm, gdk = backward(
        lengths,
        x,
        proj,
        dl,
        kc,
        wt,
        lse,
        gctx.reshape(rows, SEQ, D),
        gr1.reshape(rows, SEQ, D),
        full,
        depth,
        kmt,
    )
    stat = jnp.sum(stat, axis=1)
    grad_kernel = gkm.reshape(K, 8, W)[:, :HEADS].transpose(0, 2, 1).reshape(K, D, 3)
    grad_small = jnp.concatenate(
        [
            jnp.sum(gdk, axis=1).T,
            grad_kernel.transpose(1, 0, 2).reshape(D, 3 * K),
            stat[4:8].T,
        ],
        axis=1,
    )
    grad_small = jnp.pad(grad_small, ((0, 0), (0, W - grad_small.shape[1]))).astype(BF16)
    factors = (
        flat_x,
        dl.reshape(tokens, D),
        gproj,
        gkc.reshape(tokens, W),
        flat_ctx,
        gmix,
        act,
        gffn,
        gpre,
        fb,
    )
    sums = jnp.sum(stat[0:4], axis=1)
    count = jnp.sum(lengths).astype(F32)
    tiny = jnp.pad(jnp.concatenate([sums, count[None]]), (0, 123))
    tiny = jnp.broadcast_to(tiny[None], (8, 128))
    return y.reshape(rows, SEQ, D), gin, factors, grad_small, tiny


def weight_grads(x, dl, gproj, gkc, ctx, gmix, act, gffn, gpre, fb, small):
    pairs = [(act[s], gffn[s // 2]) for s in range(4)]
    pairs += [(gpre[s], fb[s // 2]) for s in range(4)]
    pairs += [(x, gproj[b]) for b in range(4)]
    pairs += [(ctx, gmix[b]) for b in range(2)]
    pairs += [(dl, gkc)]
    return jnp.stack([tn(a, b).astype(BF16) for a, b in pairs] + [small])


def scatter_kernel(
    depth,
    x_ref,
    dl_ref,
    gproj_ref,
    gkc_ref,
    ctx_ref,
    gmix_ref,
    act_ref,
    gffn_ref,
    gpre_ref,
    fb_ref,
    small_ref,
    t_ref,
    o_ref,
    u_ref,
    left,
    right,
    part,
    rc,
    r1,
    r2,
    ru,
    rd,
    tiny,
    got,
    left_sem,
    right_sem,
    cs,
    cr,
    s1,
    q1,
    s2,
    q2,
    us,
    ur,
    ds,
    dr,
    ts,
    tr,
):
    dp, z, x, core, y = place()
    c_dev, x_dev, y_dev = partners(dp, x, core, y)
    up_dev, down_dev = (dp + 4, y), (dp - 4, y)
    last = BLOCKS - 1

    def fetch(t, act):
        def both(a, b):
            slot = t % 2
            for copy in (
                pltpu.make_async_copy(a, left.at[slot], left_sem.at[slot]),
                pltpu.make_async_copy(b, right.at[slot], right_sem.at[slot]),
            ):
                act(copy)

        @pl.when(t < 4)
        def _():
            both(act_ref.at[t], gffn_ref.at[t // 2])

        @pl.when((t >= 4) & (t < 8))
        def _():
            both(gpre_ref.at[t - 4], fb_ref.at[(t - 4) // 2])

        @pl.when((t >= 8) & (t < 12))
        def _():
            both(x_ref, gproj_ref.at[t - 8])

        @pl.when((t >= 12) & (t < 14))
        def _():
            both(ctx_ref, gmix_ref.at[t - 12])

        @pl.when(t == 14)
        def _():
            both(dl_ref, gkc_ref)

    def c_copy(t):
        return send(part.at[t, :, :, 1 - core], rc.at[t], cs.at[t], cr.at[t], c_dev)

    def first_copy(t, by_y):
        if by_y:
            return send(part.at[t, :, :, core, 1 - y], r1.at[t], s1.at[t], q1.at[t], y_dev)
        return send(part.at[t, :, 1 - x, core], r1.at[t], s1.at[t], q1.at[t], x_dev)

    def second_copy(t, by_y):
        if by_y:
            return send(part.at[t, :, 1 - x, core, y], r2.at[t], s2.at[t], q2.at[t], x_dev)
        return send(part.at[t, :, x, core, 1 - y], r2.at[t], s2.at[t], q2.at[t], y_dev)

    def up_copy(t, bottom):
        source = part.at[t, :, x, core, y] if bottom else ru.at[t]
        return send(source, ru.at[t], us.at[t], ur.at[t], up_dev)

    def down_copy(t, top):
        source = part.at[t, :, x, core, y] if top else rd.at[t]
        return send(source, rd.at[t], ds.at[t], dr.at[t], down_dev)

    def t_copy(k):
        return send(tiny.at[k], got.at[k], ts.at[k], tr.at[k], (c_dev, x_dev, y_dev)[k])

    def t_line(d, way):
        return send(
            tiny.at[3],
            got.at[3 + z],
            ts.at[2 + d if way > 0 else 1 + depth + d],
            tr.at[3 + z],
            (dp + 4 * d * way, y),
        )

    def t_arrival(level):
        return send(tiny.at[3], got.at[3 + level], ts.at[0], tr.at[3 + level], c_dev)

    def add(into, other):
        return (into.astype(F32) + other.astype(F32)).astype(BF16)

    def parity(t, work):
        @pl.when(t % 2 == 0)
        def _():
            work(True)

        @pl.when(t % 2 == 1)
        def _():
            work(False)

    fetch(0, lambda copy: copy.start())
    lines = tuple((z >= d, (dp - 4 * d, y)) for d in range(1, depth)) + tuple(
        (z + d < depth, (dp + 4 * d, y)) for d in range(1, depth)
    )
    meet((c_dev, x_dev, y_dev), lines)
    tiny[0] = t_ref[...]
    t_copy(0).start()

    def multiply(t):
        @pl.when(t + 1 < last)
        def _():
            fetch(t + 1, lambda copy: copy.start())

        @pl.when(t < last)
        def _():
            fetch(t, lambda copy: copy.wait())
            slot = t % 2
            for c in range(2):
                block = tn(left[slot, :, c * W : (c + 1) * W], right[slot])
                half = depth // 2
                part[t, c * half : (c + 1) * half] = block.reshape(
                    (half,) + part.shape[2:]
                ).astype(BF16)

        @pl.when(t == last)
        def _():
            part[t] = small_ref[...]

        c_copy(t).start()

    def stage_core(t):
        c_copy(t).wait_recv()

        def level(j, carry):
            part[t, j, :, core] = add(part[t, j, :, core], rc[t, j])
            return carry

        lax.fori_loop(0, depth, level, 0)
        parity(t, lambda by_y: first_copy(t, by_y).start())

    def stage_first(t):
        def work(by_y):
            first_copy(t, by_y).wait_recv()
            if by_y:
                part[t, :, :, core, y] = add(part[t, :, :, core, y], r1[t])
            else:
                part[t, :, x, core] = add(part[t, :, x, core], r1[t])
            second_copy(t, by_y).start()

        parity(t, work)

    def stage_second(t):
        parity(t, lambda by_y: second_copy(t, by_y).wait_recv())
        part[t, :, x, core, y] = add(part[t, :, x, core, y], r2[t])
        o_ref[t] = part[t, z, x, core, y].astype(F32)

    def stage_up(t):
        @pl.when(z == 0)
        def _():
            up_copy(t, True).start()

        @pl.when(z > 0)
        def _():
            up_copy(t, False).wait_recv()
            o_ref[t] = o_ref[t] + ru[t, z].astype(F32)

        @pl.when((z > 0) & (z + 1 < depth))
        def _():
            ru[t] = add(ru[t], part[t, :, x, core, y])
            up_copy(t, False).start()

    def stage_down(t):
        @pl.when(z + 1 == depth)
        def _():
            down_copy(t, True).start()

        @pl.when(z + 1 < depth)
        def _():
            down_copy(t, False).wait_recv()
            o_ref[t] = o_ref[t] + rd[t, z].astype(F32)

        @pl.when((z > 0) & (z + 1 < depth))
        def _():
            rd[t] = add(rd[t], part[t, :, x, core, y])
            down_copy(t, False).start()

    def stage(t, work):
        @pl.when((t >= 0) & (t < BLOCKS))
        def _():
            work(t)

    def sums(t):
        for k in range(3):

            @pl.when(t == 3 * k + 3)
            def _():
                t_copy(k).wait_recv()
                tiny[k + 1] = tiny[k] + got[k]
                if k < 2:
                    t_copy(k + 1).start()

        @pl.when(t == 10)
        def _():
            for d in range(1, depth):

                @pl.when(z + d < depth)
                def _():
                    t_line(d, 1).start()

                @pl.when(z >= d)
                def _():
                    t_line(d, -1).start()

    def tick(t, carry):
        stage(t, multiply)
        stage(t - 1, stage_core)
        stage(t - 3, stage_first)
        stage(t - 5, stage_second)
        stage(t - 5 - z, stage_up)
        stage(t - 5 - (depth - 1 - z), stage_down)
        sums(t)
        return carry

    lax.fori_loop(0, BLOCKS + 5 + depth, tick, 0)

    for level in range(depth):

        @pl.when(z == level)
        def _():
            got[3 + level] = tiny[3]

        @pl.when(z != level)
        def _():
            t_arrival(level).wait_recv()

    total = got[3]
    for level in range(1, depth):
        total = total + got[3 + level]
    u_ref[...] = total

    for d in range(1, depth):

        @pl.when(z + d < depth)
        def _():
            t_line(d, 1).wait_send()

        @pl.when(z >= d)
        def _():
            t_line(d, -1).wait_send()

    for k in range(3):
        t_copy(k).wait_send()

    def finish(t, carry):
        c_copy(t).wait_send()
        parity(t, lambda by_y: first_copy(t, by_y).wait_send())
        parity(t, lambda by_y: second_copy(t, by_y).wait_send())

        @pl.when(z + 1 < depth)
        def _():
            up_copy(t, False).wait_send()

        @pl.when(z > 0)
        def _():
            down_copy(t, False).wait_send()

        return carry

    lax.fori_loop(0, BLOCKS, finish, 0)


def scatter_all(factors, small, tiny, mesh):
    dp, fsdp = mesh.shape["dp"], mesh.shape["fsdp"]
    rows = D // (dp * fsdp)
    if fsdp != 2 or dp % 4:
        local = weight_grads(*factors, small)
        shard = lax.psum_scatter(
            local.reshape(BLOCKS, dp * fsdp, rows, W),
            ("dp", "fsdp"),
            scatter_dimension=1,
            tiled=False,
        )
        return shard.astype(F32), lax.psum(tiny, ("dp", "fsdp"))
    depth = dp // 4
    tokens = factors[0].shape[0]
    dma = pltpu.SemaphoreType.DMA
    anywhere = pl.BlockSpec(memory_space=pl.ANY)
    inside = pl.BlockSpec(memory_space=pltpu.VMEM)
    return pl.pallas_call(
        functools.partial(scatter_kernel, depth),
        out_shape=(
            jax.ShapeDtypeStruct((BLOCKS, rows, W), F32),
            jax.ShapeDtypeStruct((8, 128), F32),
        ),
        in_specs=[anywhere] * len(factors) + [inside, inside],
        out_specs=(inside, inside),
        scratch_shapes=[
            pltpu.VMEM((2, tokens, D), BF16),
            pltpu.VMEM((2, tokens, W), BF16),
            pltpu.VMEM((BLOCKS, depth, 2, 2, 2, rows, W), BF16),
            pltpu.VMEM((BLOCKS, depth, 2, 2, rows, W), BF16),
            pltpu.VMEM((BLOCKS, depth, 2, rows, W), BF16),
            pltpu.VMEM((BLOCKS, depth, rows, W), BF16),
            pltpu.VMEM((BLOCKS, depth, rows, W), BF16),
            pltpu.VMEM((BLOCKS, depth, rows, W), BF16),
            pltpu.VMEM((4, 8, 128), F32),
            pltpu.VMEM((3 + depth, 8, 128), F32),
            dma((2,)),
            dma((2,)),
        ]
        + [dma((BLOCKS,))] * 10
        + [dma((1 + 2 * depth,)), dma((3 + depth,))],
        compiler_params=pltpu.CompilerParams(
            collective_id=1, has_side_effects=True, vmem_limit_bytes=60 * 1024 * 1024
        ),
        name="scatter_all",
    )(*factors, small.reshape(depth, 2, 2, 2, rows, W), tiny)


def body(
    mesh,
    hidden,
    lengths,
    in_weight,
    depth_kernel,
    point_weight,
    kernel_weight,
    out_weight,
    up_weight,
    down_weight,
    norm_gains,
    norm_biases,
    out_grad,
):
    full = gather_all(
        pack(
            in_weight,
            depth_kernel,
            point_weight,
            kernel_weight,
            out_weight,
            up_weight,
            down_weight,
            norm_gains,
            norm_biases,
        ),
        mesh,
    )
    output, input_grad, factors, small, tiny = layer(hidden, lengths, full, out_grad)
    shard, totals = scatter_all(factors, small, tiny, mesh)
    rms = jnp.sqrt(totals[0, :4] / (totals[0, 4] * D))
    return (output, input_grad) + unpack(shard) + (rms,)


def solution(mesh):
    in_specs = (
        P(("dp", "fsdp"), None, None),
        P(("dp", "fsdp")),
        P(("dp", "fsdp"), None),
        P(None, ("dp", "fsdp")),
        P(("dp", "fsdp"), None),
        P(None, ("dp", "fsdp")),
        P(("dp", "fsdp"), None),
        P(None, None, ("dp", "fsdp")),
        P(None, ("dp", "fsdp"), None),
        P(None, ("dp", "fsdp")),
        P(None, ("dp", "fsdp")),
        P(("dp", "fsdp"), None, None),
    )
    out_specs = (
        P(("dp", "fsdp"), None, None),
        P(("dp", "fsdp"), None, None),
        P(("dp", "fsdp"), None),
        P(None, ("dp", "fsdp")),
        P(("dp", "fsdp"), None),
        P(None, ("dp", "fsdp")),
        P(("dp", "fsdp"), None),
        P(None, None, ("dp", "fsdp")),
        P(None, ("dp", "fsdp"), None),
        P(None, ("dp", "fsdp")),
        P(None, ("dp", "fsdp")),
        P(),
    )
    return jax.shard_map(functools.partial(body, mesh), mesh=mesh, in_specs=in_specs, out_specs=out_specs, check_vma=False)
```

```python
import functools
import math

import jax
import jax.numpy as jnp
from jax import lax
from jax.experimental import pallas as pl
from jax.experimental.pallas import tpu as pltpu
from jax.sharding import PartitionSpec as P

D = 768
HEADS = 6
HD = 64
G = 2
K = 9
SEQ = 512


EPSILON = 1e-06
MESH = pl.DeviceIdType.MESH
BLOCKS = 16
HALF = BLOCKS // 2


def place():
    dp, y = lax.axis_index("dp"), lax.axis_index("fsdp")
    return dp, dp // 4, (dp // 2) % 2, dp % 2, y


def partners(dp, x, core, y):
    return (dp + 1 - 2 * core, y), (dp + 2 - 4 * x, y), (dp, 1 - y)


def meet(peers, others):
    barrier = pltpu.get_barrier_semaphore()
    for peer in peers:
        pl.semaphore_signal(barrier, inc=1, device_id=peer, device_id_type=MESH)
    count = len(peers)
    for there, peer in others:

        @pl.when(there)
        def _():
            pl.semaphore_signal(barrier, inc=1, device_id=peer, device_id_type=MESH)

        count = count + there.astype(jnp.int32)
    pl.semaphore_wait(barrier, count)


def send(src, dst, send_sem, recv_sem, device):
    return pltpu.make_async_remote_copy(
        src_ref=src,
        dst_ref=dst,
        send_sem=send_sem,
        recv_sem=recv_sem,
        device_id=device,
        device_id_type=MESH,
    )


def gather_kernel(
    depth, p_ref, g_ref, own_sem, zs, zr, xs, xr, ys, yr, ds, dr, cs, cr
):
    dp, z, x, core, y = place()
    c_dev, x_dev, y_dev = partners(dp, x, core, y)
    up_dev, down_dev = (dp + 4, y), (dp - 4, y)
    own = pltpu.make_async_copy(p_ref, g_ref.at[:, z, x, core, y], own_sem)
    own.start()
    meet((c_dev, x_dev, y_dev), ((z + 1 < depth, up_dev), (z > 0, down_dev)))
    own.wait()
    steps = 2 * depth - 1

    def target(q):
        return z + ((q + 1) // 2) * (1 - 2 * (q % 2))

    def z_copy(j, way, device):
        slab = g_ref.at[:, j, x, core, y]
        return send(slab, slab, zs.at[way, j], zr.at[j], device)

    def x_copy(j):
        slab = g_ref.at[:, j, x, core, y]
        return send(slab, slab, xs.at[j], xr.at[j], x_dev)

    def y_copy(j):
        slab = g_ref.at[:, j, x, core, y]
        return send(slab, slab, ys.at[j], yr.at[j], y_dev)

    def d_copy(j, half):
        if half == 0:
            slab = g_ref.at[pl.ds(0, HALF), j, 1 - x, core, y]
            return send(slab, slab, ds.at[0, j], dr.at[0, j], y_dev)
        slab = g_ref.at[pl.ds(HALF, HALF), j, x, core, 1 - y]
        return send(slab, slab, ds.at[1, j], dr.at[1, j], x_dev)

    def c_copy(j, a, b):
        slab = g_ref.at[:, j, (x + a) % 2, core, (y + b) % 2]
        return send(slab, slab, cs.at[2 * a + b, j], cr.at[2 * a + b, j], c_dev)

    def c_arrival(j, a, b):
        slab = g_ref.at[:, j, (x + a) % 2, 1 - core, (y + b) % 2]
        return send(slab, slab, cs.at[2 * a + b, j], cr.at[2 * a + b, j], c_dev)

    def x_arrival(j):
        slab = g_ref.at[:, j, 1 - x, core, y]
        return send(slab, slab, xs.at[j], xr.at[j], x_dev)

    def y_arrival(j):
        slab = g_ref.at[:, j, x, core, 1 - y]
        return send(slab, slab, ys.at[j], yr.at[j], y_dev)

    def d_arrival(j, half):
        slab = g_ref.at[pl.ds(half * HALF, HALF), j, 1 - x, core, 1 - y]
        return send(slab, slab, ds.at[half, j], dr.at[half, j], y_dev if half == 0 else x_dev)

    def first(j):
        @pl.when(j != z)
        def _():
            z_copy(j, 0, up_dev).wait_recv()

        @pl.when((j <= z) & (z + 1 < depth))
        def _():
            z_copy(j, 0, up_dev).start()

        @pl.when((j >= z) & (z > 0))
        def _():
            z_copy(j, 1, down_dev).start()

        x_copy(j).start()
        y_copy(j).start()
        c_copy(j, 0, 0).start()

    def second(j):
        x_arrival(j).wait_recv()
        d_copy(j, 0).start()
        c_copy(j, 1, 0).start()
        y_arrival(j).wait_recv()
        d_copy(j, 1).start()
        c_copy(j, 0, 1).start()

    def third(j):
        d_arrival(j, 0).wait_recv()
        d_arrival(j, 1).wait_recv()
        c_copy(j, 1, 1).start()

    def stage(q, work):
        j = target(q)

        @pl.when((q >= 0) & (q < steps) & (j >= 0) & (j < depth))
        def _():
            work(j)

    def step(q, carry):
        stage(q, first)
        stage(q - 1, second)
        stage(q - 2, third)
        return carry

    lax.fori_loop(0, steps + 2, step, 0)

    def finish(j, carry):
        for a in range(2):
            for b in range(2):
                c_arrival(j, a, b).wait_recv()
                c_copy(j, a, b).wait_send()
        x_copy(j).wait_send()
        y_copy(j).wait_send()
        d_copy(j, 0).wait_send()
        d_copy(j, 1).wait_send()

        @pl.when((j <= z) & (z + 1 < depth))
        def _():
            z_copy(j, 0, up_dev).wait_send()

        @pl.when((j >= z) & (z > 0))
        def _():
            z_copy(j, 1, down_dev).wait_send()

        return carry

    lax.fori_loop(0, depth, finish, 0)


def gather_all(packed, mesh):
    dp, fsdp = mesh.shape["dp"], mesh.shape["fsdp"]
    _, rows, width = packed.shape
    if fsdp != 2 or dp % 4:
        full = lax.all_gather(packed, ("dp", "fsdp"), axis=1, tiled=False)
        return full.reshape(BLOCKS, dp * fsdp * rows, width)
    depth = dp // 4
    dma = pltpu.SemaphoreType.DMA
    full = pl.pallas_call(
        functools.partial(gather_kernel, depth),
        out_shape=jax.ShapeDtypeStruct((BLOCKS, depth, 2, 2, 2, rows, width), packed.dtype),
        in_specs=[pl.BlockSpec(memory_space=pltpu.VMEM)],
        out_specs=pl.BlockSpec(memory_space=pl.ANY),
        scratch_shapes=[
            dma(()),
            dma((2, depth)),
            dma((depth,)),
            dma((depth,)),
            dma((depth,)),
            dma((depth,)),
            dma((depth,)),
            dma((2, depth)),
            dma((2, depth)),
            dma((4, depth)),
            dma((4, depth)),
        ],
        compiler_params=pltpu.CompilerParams(collective_id=0, has_side_effects=True),
        name="gather_all",
    )(packed)
    return full.reshape(BLOCKS, dp * fsdp * rows, width)


W = D // G
F32, BF16 = jnp.float32, jnp.bfloat16
PAD = 8


def nn(a, b):
    return lax.dot_general(a, b, (((1,), (0,)), ((), ())), preferred_element_type=F32)


def nt(a, b):
    return lax.dot_general(a, b, (((1,), (1,)), ((), ())), preferred_element_type=F32)


def tn(a, b):
    return lax.dot_general(a, b, (((0,), (0,)), ((), ())), preferred_element_type=F32)


def spread(rows):
    head = lax.broadcasted_iota(jnp.int32, (rows, W), 0) % 8
    channel = lax.broadcasted_iota(jnp.int32, (rows, W), 1) // HD
    return (head == channel).astype(F32).astype(BF16)


def forward_kernel(
    len_ref,
    hid_ref,
    wa_ref,
    wb_ref,
    wpt_ref,
    depth_ref,
    kmt_ref,
    x_ref,
    proj_ref,
    dl_ref,
    kc_ref,
    wt_ref,
    lse_ref,
    ctx_ref,
    xs,
    sv,
    ot,
):
    length = len_ref[pl.program_id(0)]
    inside = lax.broadcasted_iota(jnp.int32, (SEQ, 1), 0) < length
    x = jnp.where(inside, hid_ref[0], jnp.zeros((), BF16))
    x_ref[0] = x
    xs[0:PAD] = jnp.zeros((PAD, D), F32)
    xs[PAD + SEQ :] = jnp.zeros((PAD, D), F32)
    xs[PAD : PAD + SEQ] = x.astype(F32)
    sv[0:PAD] = jnp.zeros((PAD, W), F32)
    sv[PAD + SEQ :] = jnp.zeros((PAD, W), F32)

    for b in range(4):
        part = nn(x_ref[0], (wa_ref, wb_ref)[b // 2][b % 2]).astype(BF16)
        proj_ref[0, :, b * W : (b + 1) * W] = part
        if b == 3:
            sv[PAD : PAD + SEQ] = part.astype(F32)

    def column(c, carry):
        lane = pl.ds(pl.multiple_of(c * 128, 128), 128)
        for r in range(8):
            total = jnp.zeros((64, 128), F32)
            for k in range(K):
                start = PAD + r * 64 + k - K // 2
                total = total + xs[start : start + 64, lane] * depth_ref[k : k + 1, lane]
            dl_ref[0, r * 64 : (r + 1) * 64, lane] = total.astype(BF16)
        return carry

    lax.fori_loop(0, D // 128, column, 0)
    kc_ref[0] = nn(dl_ref[0], wpt_ref[0])
    mk = (kc_ref[0] * proj_ref[0, :, 0:W].astype(F32)).astype(BF16)
    logits = nt(kmt_ref[...], mk)
    top = logits[0:8]
    for k in range(1, K):
        top = jnp.maximum(top, logits[k * 8 : k * 8 + 8])
    parts = [jnp.exp(logits[k * 8 : k * 8 + 8] - top) for k in range(K)]
    inverse = 1.0 / sum(parts)
    both = []
    for k in range(K):
        weight = parts[k] * inverse
        wt_ref[0, k * 8 : k * 8 + 8] = weight
        high = weight.astype(BF16).astype(F32)
        both.append(jnp.concatenate([high, weight - high], axis=0).astype(BF16))
    e16 = spread(16)
    for r in range(4):
        total = jnp.zeros((128, W), F32)
        for k in range(K):
            start = PAD + r * 128 + k - K // 2
            total = total + tn(both[k][:, r * 128 : (r + 1) * 128], e16) * sv[start : start + 128]
        ctx_ref[0, r * 128 : (r + 1) * 128, W:] = total.astype(BF16)

    lane_head = lax.broadcasted_iota(jnp.int32, (1, 128), 1) // HD
    bias = jnp.where(inside, 0.0, -1e30).astype(F32)

    def pair(p, carry):
        def slab(part):
            return proj_ref[0, :, pl.ds(pl.multiple_of(part * W + p * 128, 128), 128)]

        q2, k2, v2 = slab(0), slab(1), slab(2)
        for h in range(2):
            scale = jnp.where(lane_head == h, 1.0 / math.sqrt(HD), 0.0).astype(BF16)
            scores = nt(k2, q2 * scale) + bias
            peak = jnp.max(scores, axis=0, keepdims=True)
            power = jnp.exp(scores - peak)
            total = jnp.sum(power, axis=0, keepdims=True)
            lse_ref[0, pl.ds(p * 2 + h, 1)] = peak + jnp.log(total)
            probs = (power * (1.0 / total)).astype(BF16)
            ot[h * HD : (h + 1) * HD] = tn(v2, probs)[h * HD : (h + 1) * HD]
        ctx_ref[0, :, pl.ds(pl.multiple_of(p * 128, 128), 128)] = ot[...].T.astype(BF16)
        return carry

    lax.fori_loop(0, HEADS // 2, pair, 0)


def forward(lengths, hidden, full, depth, kmt):
    rows = hidden.shape[0]

    def per_row(*shape):
        return pl.BlockSpec((1,) + shape, lambda r: (r, 0, 0))

    def out(dtype, *shape):
        return jax.ShapeDtypeStruct((rows,) + shape, dtype)

    return pl.pallas_call(
        forward_kernel,
        grid=(rows,),
        out_shape=(
            out(BF16, SEQ, D),
            out(BF16, SEQ, 4 * W),
            out(BF16, SEQ, D),
            out(F32, SEQ, W),
            out(F32, 8 * K, SEQ),
            out(F32, 8, SEQ),
            out(BF16, SEQ, D),
        ),
        in_specs=[
            pl.BlockSpec(memory_space=pltpu.SMEM),
            per_row(SEQ, D),
            pl.BlockSpec((2, D, W), lambda r: (5, 0, 0)),
            pl.BlockSpec((2, D, W), lambda r: (6, 0, 0)),
            pl.BlockSpec((1, D, W), lambda r: (14, 0, 0)),
            pl.BlockSpec((16, D), lambda r: (0, 0)),
            pl.BlockSpec((8 * K, W), lambda r: (0, 0)),
        ],
        out_specs=(
            per_row(SEQ, D),
            per_row(SEQ, 4 * W),
            per_row(SEQ, D),
            per_row(SEQ, W),
            per_row(8 * K, SEQ),
            per_row(8, SEQ),
            per_row(SEQ, D),
        ),
        scratch_shapes=[
            pltpu.VMEM((SEQ + 2 * PAD, D), F32),
            pltpu.VMEM((SEQ + 2 * PAD, W), F32),
            pltpu.VMEM((128, SEQ), F32),
        ],
        compiler_params=pltpu.CompilerParams(vmem_limit_bytes=56 * 1024 * 1024),
        name="mixer_forward",
    )(lengths, hidden, full, full, full, depth, kmt)


TILE = 256
CHUNK = 16
PART = 256


def ffn_kernel(
    len_ref,
    ctx_ref,
    x_ref,
    og_ref,
    wout_ref,
    wdn_ref,
    wup_ref,
    gb_ref,
    y_ref,
    act_ref,
    gpre_ref,
    fb_ref,
    gffn_ref,
    gmix_ref,
    gr1_ref,
    gctx_ref,
    stat_ref,
    mix,
    first,
    n1,
    inv,
    ffn,
    pre,
    dg,
    gr2,
):
    step = pl.program_id(0)
    row = step // (SEQ // TILE)
    base = (step % (SEQ // TILE)) * TILE
    left = len_ref[row] - base

    @pl.when(step == 0)
    def _():
        stat_ref[...] = jnp.zeros_like(stat_ref)

    for b in range(2):
        mix[:, b * W : (b + 1) * W] = nn(ctx_ref[...], wout_ref[b])

    def mask_of(i):
        return (lax.broadcasted_iota(jnp.int32, (CHUNK, 1), 0) + i * CHUNK < left).astype(F32)

    def fold(values):
        return jnp.sum(values.reshape(CHUNK // 8, 8, D), axis=0)

    def tally(k, values):
        stat_ref[k] = stat_ref[k] + fold(values)

    def rows_of(i):
        return pl.ds(pl.multiple_of(i * CHUNK, CHUNK), CHUNK)

    def norm(values):
        average = jnp.mean(values, axis=-1, keepdims=True)
        centered = values - average
        inverse = lax.rsqrt(jnp.mean(centered * centered, axis=-1, keepdims=True) + EPSILON)
        return centered * inverse, inverse

    def norm_back(grad, normed, inverse, gain):
        scaled = grad * gain
        mean = jnp.mean(scaled, axis=-1, keepdims=True)
        other = jnp.mean(scaled * normed, axis=-1, keepdims=True)
        return inverse * (scaled - mean - normed * other)

    def norm_one(i, carry):
        rows = rows_of(i)
        xf, mixed = x_ref[rows].astype(F32), mix[rows]
        normed, inverse = norm(xf + mixed)
        result = normed * gb_ref[0:1] + gb_ref[2:3]
        n1[rows] = normed
        inv[rows] = jnp.broadcast_to(inverse, (CHUNK, 128))
        first[rows] = result
        for g in range(G):
            fb_ref[g, rows] = result[:, g * W : (g + 1) * W].astype(BF16)
        tally(0, xf * xf)
        tally(1, mixed * mixed * mask_of(i))
        return carry

    lax.fori_loop(0, TILE // CHUNK, norm_one, 0)

    def part_of(c):
        return c // 3, pl.ds(c % 3 * PART, PART)

    def expand(c):
        s, units = part_of(c)
        pre[c % 2] = nt(fb_ref[s // 2], wup_ref[s, units])

    def gelu(c):
        s, units = part_of(c)
        for r in range(TILE // 32):
            rows = slice(r * 32, (r + 1) * 32)
            v = pre[c % 2, rows]
            phi = 0.5 + 0.5 * lax.erf(v * math.sqrt(0.5))
            act_ref[s, rows, units] = (v * phi).astype(BF16)
            dg[s, rows, units] = phi + v * jnp.exp(v * v * -0.5) * (1.0 / math.sqrt(2.0 * math.pi))

    def contract(s):
        g = s // 2
        part = nn(act_ref[s], wdn_ref[s])
        lanes = slice(g * W, (g + 1) * W)
        if s % 2 == 0:
            ffn[:, lanes] = part
        else:
            ffn[:, lanes] += part

    parts = 4 * D // PART
    expand(0)
    for c in range(parts):
        if c + 1 < parts:
            expand(c + 1)
        if c % 3 == 0 and c > 0:
            contract(c // 3 - 1)
        gelu(c)
    contract(3)

    def norm_two(i, carry):
        rows = rows_of(i)
        mask = mask_of(i)
        out = ffn[rows]
        normed, inverse = norm(first[rows] + out)
        y = (normed * gb_ref[1:2] + gb_ref[3:4]) * mask
        y_ref[rows] = y.astype(BF16)
        grad = og_ref[rows].astype(F32) * mask
        back = norm_back(grad, normed, inverse, gb_ref[1:2])
        gr2[rows] = back
        for g in range(G):
            gffn_ref[g, rows] = back[:, g * W : (g + 1) * W].astype(BF16)
        tally(2, out * out * mask)
        tally(3, y * y)
        tally(5, grad * normed)
        tally(7, grad)
        return carry

    lax.fori_loop(0, TILE // CHUNK, norm_two, 0)

    for c in range(parts):
        s, units = part_of(c)
        gpre_ref[s, :, units] = (nt(gffn_ref[s // 2], wdn_ref[s, units]) * dg[s, :, units]).astype(BF16)
        if c % 3 == 2:
            lanes = slice(s // 2 * W, (s // 2 + 1) * W)
            gr2[:, lanes] += nn(gpre_ref[s], wup_ref[s])

    def norm_one_back(i, carry):
        rows = rows_of(i)
        grad, normed = gr2[rows], n1[rows]
        back = norm_back(grad, normed, inv[rows, 0:1], gb_ref[0:1])
        gr1_ref[rows] = back
        for g in range(2):
            gmix_ref[g, rows] = back[:, g * W : (g + 1) * W].astype(BF16)
        tally(4, grad * normed)
        tally(6, grad)
        return carry

    lax.fori_loop(0, TILE // CHUNK, norm_one_back, 0)
    gctx_ref[...] = (
        nt(gmix_ref[0], wout_ref[0]) + nt(gmix_ref[1], wout_ref[1])
    ).astype(BF16)


def feed_forward(lengths, ctx, x, out_grad, full, gb):
    tokens = x.shape[0]

    def per_tile(width):
        return pl.BlockSpec((TILE, width), lambda i: (i, 0))

    def out(dtype, width):
        return jax.ShapeDtypeStruct((tokens, width), dtype)

    def slabs(count, width):
        return pl.BlockSpec((count, TILE, width), lambda i: (0, i, 0))

    def slabs_out(count, width):
        return jax.ShapeDtypeStruct((count, tokens, width), BF16)

    return pl.pallas_call(
        ffn_kernel,
        grid=(tokens // TILE,),
        out_shape=(
            out(BF16, D),
            slabs_out(4, D),
            slabs_out(4, D),
            slabs_out(G, W),
            slabs_out(G, W),
            slabs_out(2, W),
            out(F32, D),
            out(BF16, D),
            jax.ShapeDtypeStruct((8, 8, D), F32),
        ),
        in_specs=[
            pl.BlockSpec(memory_space=pltpu.SMEM),
            per_tile(D),
            per_tile(D),
            per_tile(D),
            pl.BlockSpec((2, D, W), lambda i: (4, 0, 0)),
            pl.BlockSpec((4, D, W), lambda i: (0, 0, 0)),
            pl.BlockSpec((4, D, W), lambda i: (1, 0, 0)),
            pl.BlockSpec((8, D), lambda i: (0, 0)),
        ],
        out_specs=(
            per_tile(D),
            slabs(4, D),
            slabs(4, D),
            slabs(G, W),
            slabs(G, W),
            slabs(2, W),
            per_tile(D),
            per_tile(D),
            pl.BlockSpec((8, 8, D), lambda i: (0, 0, 0)),
        ),
        scratch_shapes=[
            pltpu.VMEM((TILE, D), F32),
            pltpu.VMEM((TILE, D), F32),
            pltpu.VMEM((TILE, D), F32),
            pltpu.VMEM((TILE, 128), F32),
            pltpu.VMEM((TILE, D), F32),
            pltpu.VMEM((2, TILE, PART), F32),
            pltpu.VMEM((4, TILE, D), F32),
            pltpu.VMEM((TILE, D), F32),
        ],
        compiler_params=pltpu.CompilerParams(vmem_limit_bytes=56 * 1024 * 1024),
        name="feed_forward",
    )(lengths, ctx, x, out_grad, full, full, full, gb)


def backward_kernel(
    len_ref,
    x_ref,
    proj_ref,
    dl_ref,
    kc_ref,
    wt_ref,
    lse_ref,
    gctx_ref,
    gr1_ref,
    wa_ref,
    wb_ref,
    wpt_ref,
    depth_ref,
    kmt_ref,
    gproj_ref,
    gkc_ref,
    gin_ref,
    gkm_ref,
    gdk_ref,
    sv,
    gc,
    xs,
    gd,
    gs,
    gq,
    gt,
    dqt,
):
    row = pl.program_id(0)
    length = len_ref[row]
    inside = lax.broadcasted_iota(jnp.int32, (SEQ, 1), 0) < length

    @pl.when(row == 0)
    def _():
        gkm_ref[...] = jnp.zeros_like(gkm_ref)
        gdk_ref[...] = jnp.zeros_like(gdk_ref)

    for ref, width in ((sv, W), (gc, W), (xs, D), (gd, D)):
        ref[0:PAD] = jnp.zeros((PAD, width), F32)
        ref[PAD + SEQ :] = jnp.zeros((PAD, width), F32)
    sv[PAD : PAD + SEQ] = proj_ref[0, :, 3 * W :].astype(F32)
    gc[PAD : PAD + SEQ] = gctx_ref[0, :, W:].astype(F32)
    xs[PAD : PAD + SEQ] = x_ref[0].astype(F32)

    e16 = spread(16)
    place_row = lax.broadcasted_iota(jnp.int32, (W, 128), 0) // HD
    place_col = lax.broadcasted_iota(jnp.int32, (W, 128), 1)
    both = []
    for k in range(K):
        weight = pltpu.roll(wt_ref[0, k * 8 : k * 8 + 8], (k - K // 2) % SEQ, 1)
        high = weight.astype(BF16).astype(F32)
        both.append(jnp.concatenate([high, weight - high], axis=0).astype(BF16))
    for r in range(4):
        rows = slice(r * 128, (r + 1) * 128)
        spans = jnp.zeros((128, 128), F32)
        total = jnp.zeros((128, W), F32)
        for k in range(K):
            start = PAD + r * 128 + k - K // 2
            product_k = gc[PAD + r * 128 : PAD + (r + 1) * 128] * sv[start : start + 128]
            chosen = (place_col == place_row + 8 * k).astype(F32).astype(BF16)
            spans = spans + nn(product_k.astype(BF16), chosen)
            start = PAD + r * 128 - k + K // 2
            total = total + tn(both[k][:, rows], e16) * gc[start : start + 128]
        gt[:, rows] = spans.T
        gproj_ref[3, rows] = total.astype(BF16)
    center = jnp.zeros((8, SEQ), F32)
    for k in range(K):
        center = center + wt_ref[0, k * 8 : k * 8 + 8] * gt[k * 8 : k * 8 + 8]
    glt = jnp.concatenate(
        [
            wt_ref[0, k * 8 : k * 8 + 8] * (gt[k * 8 : k * 8 + 8] - center)
            for k in range(K)
        ],
        axis=0,
    ).astype(BF16)
    query = proj_ref[0, :, 0:W].astype(F32)
    mk = (kc_ref[0] * query).astype(BF16)
    gkm_ref[...] += nn(glt, mk)
    mixed = tn(glt, kmt_ref[...])
    gkc_ref[0] = (mixed * query).astype(BF16)
    gq[...] = mixed * kc_ref[0]
    gd[PAD : PAD + SEQ] = nt(gkc_ref[0], wpt_ref[0])

    def column(c, carry):
        lane = pl.ds(pl.multiple_of(c * 128, 128), 128)
        sums = [jnp.zeros((8, 128), F32)] * K
        for r in range(8):
            total = jnp.zeros((64, 128), F32)
            center = PAD + r * 64
            grad = gd[center : center + 64, lane]
            for k in range(K):
                start = center + k - K // 2
                sums[k] = sums[k] + jnp.sum(
                    (xs[start : start + 64, lane] * grad).reshape(8, 8, 128), axis=0
                )
                start = center - k + K // 2
                total = total + gd[start : start + 64, lane] * depth_ref[k : k + 1, lane]
            gs[r * 64 : (r + 1) * 64, lane] = total
        for k in range(K):
            gdk_ref[k, :, lane] = gdk_ref[k, :, lane] + sums[k]
        return carry

    lax.fori_loop(0, D // 128, column, 0)

    lane_head = lax.broadcasted_iota(jnp.int32, (1, 128), 1) // HD
    bias = jnp.where(inside, 0.0, -1e30).astype(F32)

    def pair(p, carry):
        def lanes(part):
            return pl.ds(pl.multiple_of(part * W + p * 128, 128), 128)

        q2, k2, v2 = (proj_ref[0, :, lanes(part)] for part in range(3))
        g2 = gctx_ref[0, :, lanes(0)]
        results = []
        for h in range(2):
            mine = lane_head == h
            scale = jnp.where(mine, 1.0 / math.sqrt(HD), 0.0).astype(BF16)
            scores = nt(k2, q2 * scale) + bias
            probs = jnp.exp(scores - lse_ref[0, pl.ds(p * 2 + h, 1)])
            grads = nt(v2 * jnp.where(mine, 1.0, 0.0).astype(BF16), g2)
            correction = jnp.sum(probs * grads, axis=0, keepdims=True)
            grad_scores = (probs * (grads - correction)).astype(BF16)
            dqt[h * HD : (h + 1) * HD] = tn(k2, grad_scores)[h * HD : (h + 1) * HD]
            results.append((nn(grad_scores, q2), nn(probs.astype(BF16), g2)))
        low = lane_head == 0
        scale = 1.0 / math.sqrt(HD)
        gproj_ref[0, :, lanes(0)] = (dqt[...].T * scale + gq[:, lanes(0)]).astype(BF16)
        gproj_ref[1, :, lanes(0)] = (jnp.where(low, results[0][0], results[1][0]) * scale).astype(BF16)
        gproj_ref[2, :, lanes(0)] = jnp.where(low, results[0][1], results[1][1]).astype(BF16)
        return carry

    lax.fori_loop(0, HEADS // 2, pair, 0)

    for b in range(4):
        gs[...] += nt(gproj_ref[b], (wa_ref, wb_ref)[b // 2][b % 2])
    gin_ref[0] = jnp.where(inside, gr1_ref[0] + gs[...], 0.0).astype(BF16)


def backward(lengths, x, proj, dl, kc, wt, lse, gctx, gr1, full, depth, kmt):
    rows = x.shape[0]

    def per_row(*shape):
        return pl.BlockSpec((1,) + shape, lambda r: (r, 0, 0))

    def out(dtype, *shape):
        return jax.ShapeDtypeStruct((rows,) + shape, dtype)

    return pl.pallas_call(
        backward_kernel,
        grid=(rows,),
        out_shape=(
            jax.ShapeDtypeStruct((4, rows * SEQ, W), BF16),
            out(BF16, SEQ, W),
            out(BF16, SEQ, D),
            jax.ShapeDtypeStruct((8 * K, W), F32),
            jax.ShapeDtypeStruct((K, 8, D), F32),
        ),
        in_specs=[
            pl.BlockSpec(memory_space=pltpu.SMEM),
            per_row(SEQ, D),
            per_row(SEQ, 4 * W),
            per_row(SEQ, D),
            per_row(SEQ, W),
            per_row(8 * K, SEQ),
            per_row(8, SEQ),
            per_row(SEQ, D),
            per_row(SEQ, D),
            pl.BlockSpec((2, D, W), lambda r: (5, 0, 0)),
            pl.BlockSpec((2, D, W), lambda r: (6, 0, 0)),
            pl.BlockSpec((1, D, W), lambda r: (14, 0, 0)),
            pl.BlockSpec((16, D), lambda r: (0, 0)),
            pl.BlockSpec((8 * K, W), lambda r: (0, 0)),
        ],
        out_specs=(
            pl.BlockSpec((4, SEQ, W), lambda r: (0, r, 0)),
            per_row(SEQ, W),
            per_row(SEQ, D),
            pl.BlockSpec((8 * K, W), lambda r: (0, 0)),
            pl.BlockSpec((K, 8, D), lambda r: (0, 0, 0)),
        ),
        scratch_shapes=[
            pltpu.VMEM((SEQ + 2 * PAD, W), F32),
            pltpu.VMEM((SEQ + 2 * PAD, W), F32),
            pltpu.VMEM((SEQ + 2 * PAD, D), F32),
            pltpu.VMEM((SEQ + 2 * PAD, D), F32),
            pltpu.VMEM((SEQ, D), F32),
            pltpu.VMEM((SEQ, W), F32),
            pltpu.VMEM((128, SEQ), F32),
            pltpu.VMEM((128, SEQ), F32),
        ],
        compiler_params=pltpu.CompilerParams(vmem_limit_bytes=56 * 1024 * 1024),
        name="mixer_backward",
    )(lengths, x, proj, dl, kc, wt, lse, gctx, gr1, full, full, full, depth, kmt)


def pack(in_weight, depth_kernel, point_weight, kernel_weight, out_weight, up_weight, down_weight, norm_gains, norm_biases):
    rows = in_weight.shape[0]

    def halves(grouped):
        return grouped.reshape(G * 2, rows, W)

    kernel = kernel_weight.reshape(K, rows, 3).transpose(1, 0, 2).reshape(rows, 3 * K)
    small = jnp.concatenate([depth_kernel.T, kernel, norm_gains.T, norm_biases.T], axis=1)
    small = jnp.pad(small, ((0, 0), (0, W - small.shape[1])))
    return jnp.concatenate(
        [
            halves(down_weight),
            halves(up_weight.transpose(0, 2, 1)),
            out_weight.reshape(rows, 2, W).transpose(1, 0, 2),
            in_weight.reshape(rows, 4, W).transpose(1, 0, 2),
            point_weight[None],
            small[None],
        ],
        axis=0,
    )


def unpack(shard):
    rows = shard.shape[1]
    small = shard[15]
    kernel = small[:, K : 4 * K].reshape(rows, K, 3).transpose(1, 0, 2).reshape(K, 3 * rows)
    return (
        shard[10:14].transpose(1, 0, 2).reshape(rows, 4 * W),
        small[:, :K].T,
        shard[14],
        kernel,
        shard[8:10].transpose(1, 0, 2).reshape(rows, 2 * W),
        shard[4:8].reshape(G, 2 * rows, W).transpose(0, 2, 1),
        shard[0:4].reshape(G, 2 * rows, W),
        small[:, 4 * K : 4 * K + 2].T,
        small[:, 4 * K + 2 : 4 * K + 4].T,
    )


def constants(full):
    small = full[15].astype(F32)
    depth = jnp.pad(small[:, :K].T, ((0, 16 - K), (0, 0)))
    kernel = small[:, K : 4 * K].reshape(D, K, 3).transpose(1, 0, 2).reshape(K, W, HEADS)
    kmt = jnp.pad(kernel.transpose(0, 2, 1), ((0, 0), (0, 8 - HEADS), (0, 0)))
    kmt = kmt.reshape(8 * K, W).astype(BF16)
    gb = jnp.pad(small[:, 4 * K : 4 * K + 4].T, ((0, 4), (0, 0)))
    return depth, kmt, gb


def layer(mesh, hidden, lengths, full, out_grad):
    rows = hidden.shape[0]
    tokens = rows * SEQ
    depth, kmt, gb = constants(full)
    x, proj, dl, kc, wt, lse, ctx = forward(lengths, hidden, full, depth, kmt)
    flat_x, flat_ctx = x.reshape(tokens, D), ctx.reshape(tokens, D)
    y, act, gpre, fb, gffn, gmix, gr1, gctx, stat = feed_forward(
        lengths, flat_ctx, flat_x, out_grad.reshape(tokens, D), full, gb
    )
    gctx, gr1 = gctx.reshape(rows, SEQ, D), gr1.reshape(rows, SEQ, D)
    if fused(mesh, rows):
        gin, shard, totals = backward_scatter(
            mesh, lengths, x, proj, dl, kc, wt, lse, gctx, gr1, full, depth, kmt, ctx, gmix, act, gffn, gpre, fb, stat
        )
        return y.reshape(rows, SEQ, D), gin, shard, totals
    gproj, gkc, gin, gkm, gdk = backward(
        lengths, x, proj, dl, kc, wt, lse, gctx, gr1, full, depth, kmt
    )
    stat = jnp.sum(stat, axis=1)
    grad_kernel = gkm.reshape(K, 8, W)[:, :HEADS].transpose(0, 2, 1).reshape(K, D, 3)
    small = jnp.concatenate(
        [
            jnp.sum(gdk, axis=1).T,
            grad_kernel.transpose(1, 0, 2).reshape(D, 3 * K),
            stat[4:8].T,
        ],
        axis=1,
    )
    small = jnp.pad(small, ((0, 0), (0, W - small.shape[1]))).astype(BF16)
    local = weight_grads(
        flat_x, dl.reshape(tokens, D), gproj, gkc.reshape(tokens, W), flat_ctx, gmix, act, gffn, gpre, fb, small
    )
    sums = jnp.concatenate([jnp.sum(stat[0:4], axis=1), jnp.sum(lengths).astype(F32)[None]])
    if mesh is None:
        return y.reshape(rows, SEQ, D), gin, local.astype(F32), sums[None]
    devices = mesh.shape["dp"] * mesh.shape["fsdp"]
    shard = lax.psum_scatter(
        local.reshape(BLOCKS, devices, D // devices, W),
        ("dp", "fsdp"),
        scatter_dimension=1,
        tiled=False,
    )
    return (
        y.reshape(rows, SEQ, D),
        gin,
        shard.astype(F32),
        lax.psum(sums, ("dp", "fsdp"))[None],
    )


def fused(mesh, rows):
    return mesh is not None and mesh.shape["fsdp"] == 2 and mesh.shape["dp"] % 4 == 0 and rows == 2


def weight_grads(x, dl, gproj, gkc, ctx, gmix, act, gffn, gpre, fb, small):
    pairs = [(act[s], gffn[s // 2]) for s in range(4)]
    pairs += [(gpre[s], fb[s // 2]) for s in range(4)]
    pairs += [(ctx, gmix[b]) for b in range(2)]
    pairs += [(x, gproj[b]) for b in range(4)]
    pairs += [(dl, gkc)]
    return jnp.stack([tn(a, b).astype(BF16) for a, b in pairs] + [small])


def backward_scatter_kernel(
    depth,
    len_ref,
    x_hbm,
    proj_hbm,
    dl_hbm,
    kc_hbm,
    wt_hbm,
    lse_hbm,
    gctx_hbm,
    gr1_hbm,
    full_hbm,
    depth_ref,
    kmt_ref,
    ctx_hbm,
    gmix_hbm,
    act_hbm,
    gffn_hbm,
    gpre_hbm,
    fb_hbm,
    stat_ref,
    gin_ref,
    o_ref,
    u_ref,
    x_ref,
    proj_ref,
    dl_ref,
    kc_ref,
    wt_ref,
    lse_ref,
    gctx_ref,
    gr1_ref,
    win_ref,
    wpt_ref,
    gproj_ref,
    gkc_ref,
    gkm,
    gdk,
    small,
    sv,
    gc,
    xs,
    gd,
    gs,
    gq,
    gt,
    dqt,
    left,
    right,
    part,
    rc,
    r1,
    r2,
    ru,
    rd,
    tiny,
    got,
    in_sem,
    left_sem,
    right_sem,
    cs,
    cr,
    s1,
    q1,
    s2,
    q2,
    us,
    ur,
    ds,
    dr,
    ts,
    tr,
):
    dp, z, x, core, y = place()
    c_dev, x_dev, y_dev = partners(dp, x, core, y)
    up_dev, down_dev = (dp + 4, y), (dp - 4, y)
    last = BLOCKS - 1
    rows = x_ref.shape[0]
    early = 5 * rows

    def fetch(t, act):
        def both(a, b):
            slot = t % 2
            for copy in (
                pltpu.make_async_copy(a, left.at[slot], left_sem.at[slot]),
                pltpu.make_async_copy(b, right.at[slot], right_sem.at[slot]),
            ):
                act(copy)

        @pl.when(t < 4)
        def _():
            both(act_hbm.at[t], gffn_hbm.at[t // 2])

        @pl.when((t >= 4) & (t < 8))
        def _():
            both(gpre_hbm.at[t - 4], fb_hbm.at[(t - 4) // 2])

        @pl.when((t >= 8) & (t < 10))
        def _():
            both(ctx_hbm, gmix_hbm.at[t - 8])

        @pl.when((t >= 10) & (t < 14))
        def _():
            both(x_hbm, gproj_ref.at[:, t - 10])

        @pl.when(t == 14)
        def _():
            both(dl_hbm, gkc_ref)

    def c_copy(t):
        return send(part.at[t, :, :, 1 - core], rc.at[t], cs.at[t], cr.at[t], c_dev)

    def first_copy(t, by_y):
        if by_y:
            return send(part.at[t, :, :, core, 1 - y], r1.at[t], s1.at[t], q1.at[t], y_dev)
        return send(part.at[t, :, 1 - x, core], r1.at[t], s1.at[t], q1.at[t], x_dev)

    def second_copy(t, by_y):
        if by_y:
            return send(part.at[t, :, 1 - x, core, y], r2.at[t], s2.at[t], q2.at[t], x_dev)
        return send(part.at[t, :, x, core, 1 - y], r2.at[t], s2.at[t], q2.at[t], y_dev)

    def up_copy(t, bottom):
        source = part.at[t, :, x, core, y] if bottom else ru.at[t]
        return send(source, ru.at[t], us.at[t], ur.at[t], up_dev)

    def down_copy(t, top):
        source = part.at[t, :, x, core, y] if top else rd.at[t]
        return send(source, rd.at[t], ds.at[t], dr.at[t], down_dev)

    def t_copy(k):
        return send(tiny.at[k], got.at[k], ts.at[k], tr.at[k], (c_dev, x_dev, y_dev)[k])

    def t_line(d, way):
        return send(
            tiny.at[3],
            got.at[3 + z],
            ts.at[2 + d if way > 0 else 1 + depth + d],
            tr.at[3 + z],
            (dp + 4 * d * way, y),
        )

    def t_arrival(level):
        return send(tiny.at[3], got.at[3 + level], ts.at[0], tr.at[3 + level], c_dev)

    def add(into, other):
        return (into.astype(F32) + other.astype(F32)).astype(BF16)

    def parity(t, work):
        @pl.when(t % 2 == 0)
        def _():
            work(True)

        @pl.when(t % 2 == 1)
        def _():
            work(False)


    def inside_of(r):
        return lax.broadcasted_iota(jnp.int32, (SEQ, 1), 0) < len_ref[r]

    def piece_span(r):
        sv[PAD : PAD + SEQ] = proj_ref[r, :, 3 * W :].astype(F32)
        gc[PAD : PAD + SEQ] = gctx_ref[r, :, W:].astype(F32)
        xs[PAD : PAD + SEQ] = x_ref[r].astype(F32)

        e16 = spread(16)
        place_row = lax.broadcasted_iota(jnp.int32, (W, 128), 0) // HD
        place_col = lax.broadcasted_iota(jnp.int32, (W, 128), 1)
        both = []
        for k in range(K):
            weight = pltpu.roll(wt_ref[r, k * 8 : k * 8 + 8], (k - K // 2) % SEQ, 1)
            high = weight.astype(BF16).astype(F32)
            both.append(jnp.concatenate([high, weight - high], axis=0).astype(BF16))
        for n in range(4):
            rows = slice(n * 128, (n + 1) * 128)
            spans = jnp.zeros((128, 128), F32)
            total = jnp.zeros((128, W), F32)
            for k in range(K):
                start = PAD + n * 128 + k - K // 2
                product_k = gc[PAD + n * 128 : PAD + (n + 1) * 128] * sv[start : start + 128]
                chosen = (place_col == place_row + 8 * k).astype(F32).astype(BF16)
                spans = spans + nn(product_k.astype(BF16), chosen)
                start = PAD + n * 128 - k + K // 2
                total = total + tn(both[k][:, rows], e16) * gc[start : start + 128]
            gt[:, rows] = spans.T
            gproj_ref[r, 3, rows] = total.astype(BF16)

    def piece_logits(r):
        center = jnp.zeros((8, SEQ), F32)
        for k in range(K):
            center = center + wt_ref[r, k * 8 : k * 8 + 8] * gt[k * 8 : k * 8 + 8]
        glt = jnp.concatenate(
            [
                wt_ref[r, k * 8 : k * 8 + 8] * (gt[k * 8 : k * 8 + 8] - center)
                for k in range(K)
            ],
            axis=0,
        ).astype(BF16)
        query = proj_ref[r, :, 0:W].astype(F32)
        mk = (kc_ref[r] * query).astype(BF16)
        gkm[...] += nn(glt, mk)
        mixed = tn(glt, kmt_ref[...])
        gkc_ref[r] = (mixed * query).astype(BF16)
        gq[...] = mixed * kc_ref[r]
        gd[PAD : PAD + SEQ] = nt(gkc_ref[r], wpt_ref[0])


    def piece_columns(r):
        def column(c, carry):
            lane = pl.ds(pl.multiple_of(c * 128, 128), 128)
            sums = [jnp.zeros((8, 128), F32)] * K
            for n in range(8):
                total = jnp.zeros((64, 128), F32)
                center = PAD + n * 64
                grad = gd[center : center + 64, lane]
                for k in range(K):
                    start = center + k - K // 2
                    sums[k] = sums[k] + jnp.sum(
                        (xs[start : start + 64, lane] * grad).reshape(8, 8, 128), axis=0
                    )
                    start = center - k + K // 2
                    total = total + gd[start : start + 64, lane] * depth_ref[k : k + 1, lane]
                gs[n * 64 : (n + 1) * 64, lane] = total
            for k in range(K):
                gdk[k, :, lane] = gdk[k, :, lane] + sums[k]
            return carry

        lax.fori_loop(0, D // 128, column, 0)


    def piece_pairs(r, first, stop):
        inside = inside_of(r)
        lane_head = lax.broadcasted_iota(jnp.int32, (1, 128), 1) // HD
        bias = jnp.where(inside, 0.0, -1e30).astype(F32)

        def pair(p, carry):
            def lanes(part):
                return pl.ds(pl.multiple_of(part * W + p * 128, 128), 128)

            q2, k2, v2 = (proj_ref[r, :, lanes(part)] for part in range(3))
            g2 = gctx_ref[r, :, lanes(0)]
            results = []
            for h in range(2):
                mine = lane_head == h
                scale = jnp.where(mine, 1.0 / math.sqrt(HD), 0.0).astype(BF16)
                scores = nt(k2, q2 * scale) + bias
                probs = jnp.exp(scores - lse_ref[r, pl.ds(p * 2 + h, 1)])
                grads = nt(v2 * jnp.where(mine, 1.0, 0.0).astype(BF16), g2)
                correction = jnp.sum(probs * grads, axis=0, keepdims=True)
                grad_scores = (probs * (grads - correction)).astype(BF16)
                dqt[h * HD : (h + 1) * HD] = tn(k2, grad_scores)[h * HD : (h + 1) * HD]
                results.append((nn(grad_scores, q2), nn(probs.astype(BF16), g2)))
            low = lane_head == 0
            scale = 1.0 / math.sqrt(HD)
            gproj_ref[r, 0, :, lanes(0)] = (dqt[...].T * scale + gq[:, lanes(0)]).astype(BF16)
            gproj_ref[r, 1, :, lanes(0)] = (jnp.where(low, results[0][0], results[1][0]) * scale).astype(BF16)
            gproj_ref[r, 2, :, lanes(0)] = jnp.where(low, results[0][1], results[1][1]).astype(BF16)
            return carry

        lax.fori_loop(first, stop, pair, 0)


    def piece_inputs(r):
        inside = inside_of(r)
        for b in range(4):
            gs[...] += nt(gproj_ref[r, b], win_ref[b])
        gin_ref[r] = jnp.where(inside, gr1_ref[r] + gs[...], 0.0).astype(BF16)


    def chosen(height, rule):
        row = lax.broadcasted_iota(jnp.int32, (height, 128), 0)
        lane = lax.broadcasted_iota(jnp.int32, (height, 128), 1)
        return rule(row, lane).astype(F32).astype(BF16)

    def gather_small():
        taps = jnp.concatenate(
            [jnp.sum(gdk[...], axis=1), jnp.zeros((16 - K, D), F32), jnp.sum(stat_ref[...], axis=1)]
        ).astype(BF16)
        pick = chosen(
            24,
            lambda row, lane: ((row < K) & (lane == row)) | ((row >= 20) & (lane == row - 20 + 4 * K)),
        )
        both = tn(taps, pick)
        low = gkm[...].astype(BF16)
        small[...] = both
        for odd in range(2):
            pick = chosen(
                8 * K,
                lambda row, lane: (row % 8 >= 3 * odd)
                & (row % 8 < 3 * odd + 3)
                & (lane == K + row // 8 * 3 + row % 8 - 3 * odd),
            )
            half = pl.ds(odd, W, stride=2)
            small[half] = small[half] + tn(low, pick)

    loads = (
        (x_hbm, x_ref),
        (proj_hbm, proj_ref),
        (dl_hbm, dl_ref),
        (kc_hbm, kc_ref),
        (wt_hbm, wt_ref),
        (lse_hbm, lse_ref),
        (gctx_hbm, gctx_ref),
        (gr1_hbm, gr1_ref),
        (full_hbm.at[pl.ds(10, 4)], win_ref),
        (full_hbm.at[pl.ds(14, 1)], wpt_ref),
    )
    inputs = [
        pltpu.make_async_copy(source, target, in_sem.at[i])
        for i, (source, target) in enumerate(loads)
    ]
    fetch(0, lambda copy: copy.start())
    for copy in inputs:
        copy.start()
    gkm[...] = jnp.zeros_like(gkm)
    gdk[...] = jnp.zeros_like(gdk)
    for ref, width in ((sv, W), (gc, W), (xs, D), (gd, D)):
        ref[0:PAD] = jnp.zeros((PAD, width), F32)
        ref[PAD + SEQ :] = jnp.zeros((PAD, width), F32)
    lines = tuple((z >= d, (dp - 4 * d, y)) for d in range(1, depth)) + tuple(
        (z + d < depth, (dp + 4 * d, y)) for d in range(1, depth)
    )
    meet((c_dev, x_dev, y_dev), lines)
    lane = lax.broadcasted_iota(jnp.int32, (8, 128), 1)
    mine = jnp.zeros((8, 128), F32)
    for k in range(4):
        mine = jnp.where(lane == k, jnp.sum(stat_ref[k]), mine)
    count = len_ref[0]
    for r in range(1, rows):
        count = count + len_ref[r]
    tiny[0] = jnp.where(lane == 4, count.astype(F32), mine)
    t_copy(0).start()

    def multiply(t):
        @pl.when(t == early)
        def _():
            fetch(t, lambda copy: copy.start())

        @pl.when((t + 1 < last) & (t + 1 != early))
        def _():
            fetch(t + 1, lambda copy: copy.start())

        @pl.when(t < last)
        def _():
            fetch(t, lambda copy: copy.wait())
            slot = t % 2
            for c in range(2):
                a = left[slot, :, :, c * W : (c + 1) * W].reshape(rows * SEQ, W)
                block = tn(a, right[slot].reshape(rows * SEQ, W))
                half = depth // 2
                part[t, c * half : (c + 1) * half] = block.reshape(
                    (half,) + part.shape[2:]
                ).astype(BF16)

        @pl.when(t == last)
        def _():
            gather_small()
            filled = jnp.concatenate([small[...], jnp.zeros((D, W - 128), F32)], axis=1)
            part[t] = filled.reshape(part.shape[1:]).astype(BF16)

        c_copy(t).start()

    def stage_core(t):
        c_copy(t).wait_recv()

        def level(j, carry):
            part[t, j, :, core] = add(part[t, j, :, core], rc[t, j])
            return carry

        lax.fori_loop(0, depth, level, 0)
        parity(t, lambda by_y: first_copy(t, by_y).start())

    def stage_first(t):
        def work(by_y):
            first_copy(t, by_y).wait_recv()
            if by_y:
                part[t, :, :, core, y] = add(part[t, :, :, core, y], r1[t])
            else:
                part[t, :, x, core] = add(part[t, :, x, core], r1[t])
            second_copy(t, by_y).start()

        parity(t, work)

    def stage_second(t):
        parity(t, lambda by_y: second_copy(t, by_y).wait_recv())
        part[t, :, x, core, y] = add(part[t, :, x, core, y], r2[t])
        o_ref[t] = part[t, z, x, core, y].astype(F32)

    def stage_up(t):
        @pl.when(z == 0)
        def _():
            up_copy(t, True).start()

        @pl.when(z > 0)
        def _():
            up_copy(t, False).wait_recv()
            o_ref[t] = o_ref[t] + ru[t, z].astype(F32)

        @pl.when((z > 0) & (z + 1 < depth))
        def _():
            ru[t] = add(ru[t], part[t, :, x, core, y])
            up_copy(t, False).start()

    def stage_down(t):
        @pl.when(z + 1 == depth)
        def _():
            down_copy(t, True).start()

        @pl.when(z + 1 < depth)
        def _():
            down_copy(t, False).wait_recv()
            o_ref[t] = o_ref[t] + rd[t, z].astype(F32)

        @pl.when((z > 0) & (z + 1 < depth))
        def _():
            rd[t] = add(rd[t], part[t, :, x, core, y])
            down_copy(t, False).start()

    def stage(t, work):
        @pl.when((t >= 0) & (t < BLOCKS))
        def _():
            work(t)

    def sums(t):
        for k in range(3):

            @pl.when(t == 3 * k + 3)
            def _():
                t_copy(k).wait_recv()
                tiny[k + 1] = tiny[k] + got[k]
                if k < 2:
                    t_copy(k + 1).start()

        @pl.when(t == 10)
        def _():
            for d in range(1, depth):

                @pl.when(z + d < depth)
                def _():
                    t_line(d, 1).start()

                @pl.when(z >= d)
                def _():
                    t_line(d, -1).start()

    def tick(t, carry):
        stage(t, multiply)
        stage(t - 1, stage_core)
        stage(t - 3, stage_first)
        stage(t - 5, stage_second)
        stage(t - 5 - z, stage_up)
        stage(t - 5 - (depth - 1 - z), stage_down)
        sums(t)
        row = t // 5

        def when(i, work):
            @pl.when((t < early) & (t % 5 == i))
            def _():
                work()

        @pl.when(t == 0)
        def _():
            for copy in inputs:
                copy.wait()

        when(0, lambda: piece_span(row))
        when(1, lambda: piece_logits(row))
        when(2, lambda: piece_columns(row))
        when(3, lambda: piece_pairs(row, 0, 2))

        def close():
            piece_pairs(row, 2, 3)
            piece_inputs(row)

        when(4, close)
        return carry

    lax.fori_loop(0, BLOCKS + 5 + depth, tick, 0)

    for level in range(depth):

        @pl.when(z == level)
        def _():
            got[3 + level] = tiny[3]

        @pl.when(z != level)
        def _():
            t_arrival(level).wait_recv()

    total = got[3]
    for level in range(1, depth):
        total = total + got[3 + level]
    u_ref[...] = total

    for d in range(1, depth):

        @pl.when(z + d < depth)
        def _():
            t_line(d, 1).wait_send()

        @pl.when(z >= d)
        def _():
            t_line(d, -1).wait_send()

    for k in range(3):
        t_copy(k).wait_send()

    def finish(t, carry):
        c_copy(t).wait_send()
        parity(t, lambda by_y: first_copy(t, by_y).wait_send())
        parity(t, lambda by_y: second_copy(t, by_y).wait_send())

        @pl.when(z + 1 < depth)
        def _():
            up_copy(t, False).wait_send()

        @pl.when(z > 0)
        def _():
            down_copy(t, False).wait_send()

        return carry

    lax.fori_loop(0, BLOCKS, finish, 0)


def backward_scatter(mesh, lengths, x, proj, dl, kc, wt, lse, gctx, gr1, full, depth_kernel, kmt, ctx, gmix, act, gffn, gpre, fb, stat):
    dp, fsdp = mesh.shape["dp"], mesh.shape["fsdp"]
    share = D // (dp * fsdp)
    depth = dp // 4
    rows = x.shape[0]
    dma = pltpu.SemaphoreType.DMA
    anywhere = pl.BlockSpec(memory_space=pl.ANY)
    inside = pl.BlockSpec(memory_space=pltpu.VMEM)

    def by_row(values):
        return values.reshape(values.shape[:-2] + (rows, SEQ, values.shape[-1]))

    return pl.pallas_call(
        functools.partial(backward_scatter_kernel, depth),
        out_shape=(
            jax.ShapeDtypeStruct((rows, SEQ, D), BF16),
            jax.ShapeDtypeStruct((BLOCKS, share, W), F32),
            jax.ShapeDtypeStruct((8, 128), F32),
        ),
        in_specs=[pl.BlockSpec(memory_space=pltpu.SMEM)]
        + [anywhere] * 9
        + [inside] * 2
        + [anywhere] * 6
        + [inside],
        out_specs=(inside, inside, inside),
        scratch_shapes=[
            pltpu.VMEM((rows, SEQ, D), BF16),
            pltpu.VMEM((rows, SEQ, 4 * W), BF16),
            pltpu.VMEM((rows, SEQ, D), BF16),
            pltpu.VMEM((rows, SEQ, W), F32),
            pltpu.VMEM((rows, 8 * K, SEQ), F32),
            pltpu.VMEM((rows, 8, SEQ), F32),
            pltpu.VMEM((rows, SEQ, D), BF16),
            pltpu.VMEM((rows, SEQ, D), F32),
            pltpu.VMEM((4, D, W), BF16),
            pltpu.VMEM((1, D, W), BF16),
            pltpu.VMEM((rows, 4, SEQ, W), BF16),
            pltpu.VMEM((rows, SEQ, W), BF16),
            pltpu.VMEM((8 * K, W), F32),
            pltpu.VMEM((K, 8, D), F32),
            pltpu.VMEM((D, 128), F32),
            pltpu.VMEM((SEQ + 2 * PAD, W), F32),
            pltpu.VMEM((SEQ + 2 * PAD, W), F32),
            pltpu.VMEM((SEQ + 2 * PAD, D), F32),
            pltpu.VMEM((SEQ + 2 * PAD, D), F32),
            pltpu.VMEM((SEQ, D), F32),
            pltpu.VMEM((SEQ, W), F32),
            pltpu.VMEM((128, SEQ), F32),
            pltpu.VMEM((128, SEQ), F32),
            pltpu.VMEM((2, rows, SEQ, D), BF16),
            pltpu.VMEM((2, rows, SEQ, W), BF16),
            pltpu.VMEM((BLOCKS, depth, 2, 2, 2, share, W), BF16),
            pltpu.VMEM((BLOCKS, depth, 2, 2, share, W), BF16),
            pltpu.VMEM((BLOCKS, depth, 2, share, W), BF16),
            pltpu.VMEM((BLOCKS, depth, share, W), BF16),
            pltpu.VMEM((BLOCKS, depth, share, W), BF16),
            pltpu.VMEM((BLOCKS, depth, share, W), BF16),
            pltpu.VMEM((4, 8, 128), F32),
            pltpu.VMEM((3 + depth, 8, 128), F32),
            dma((10,)),
            dma((2,)),
            dma((2,)),
        ]
        + [dma((BLOCKS,))] * 10
        + [dma((1 + 2 * depth,)), dma((3 + depth,))],
        compiler_params=pltpu.CompilerParams(
            collective_id=1, has_side_effects=True, vmem_limit_bytes=67_000_000
        ),
        name="backward_scatter",
    )(
        lengths,
        x,
        proj,
        dl,
        kc,
        wt,
        lse,
        gctx,
        gr1,
        full,
        depth_kernel,
        kmt,
        ctx,
        by_row(gmix),
        by_row(act),
        by_row(gffn),
        by_row(gpre),
        by_row(fb),
        stat,
    )


def body(
    mesh,
    hidden,
    lengths,
    in_weight,
    depth_kernel,
    point_weight,
    kernel_weight,
    out_weight,
    up_weight,
    down_weight,
    norm_gains,
    norm_biases,
    out_grad,
):
    full = gather_all(
        pack(
            in_weight,
            depth_kernel,
            point_weight,
            kernel_weight,
            out_weight,
            up_weight,
            down_weight,
            norm_gains,
            norm_biases,
        ),
        mesh,
    )
    output, input_grad, shard, totals = layer(mesh, hidden, lengths, full, out_grad)
    rms = jnp.sqrt(totals[0, :4] / (totals[0, 4] * D))
    return (output, input_grad) + unpack(shard) + (rms,)


def solution(mesh):
    in_specs = (
        P(("dp", "fsdp"), None, None),
        P(("dp", "fsdp")),
        P(("dp", "fsdp"), None),
        P(None, ("dp", "fsdp")),
        P(("dp", "fsdp"), None),
        P(None, ("dp", "fsdp")),
        P(("dp", "fsdp"), None),
        P(None, None, ("dp", "fsdp")),
        P(None, ("dp", "fsdp"), None),
        P(None, ("dp", "fsdp")),
        P(None, ("dp", "fsdp")),
        P(("dp", "fsdp"), None, None),
    )
    out_specs = (
        P(("dp", "fsdp"), None, None),
        P(("dp", "fsdp"), None, None),
        P(("dp", "fsdp"), None),
        P(None, ("dp", "fsdp")),
        P(("dp", "fsdp"), None),
        P(None, ("dp", "fsdp")),
        P(("dp", "fsdp"), None),
        P(None, None, ("dp", "fsdp")),
        P(None, ("dp", "fsdp"), None),
        P(None, ("dp", "fsdp")),
        P(None, ("dp", "fsdp")),
        P(),
    )
    return jax.shard_map(functools.partial(body, mesh), mesh=mesh, in_specs=in_specs, out_specs=out_specs, check_vma=False)
```

```python
import functools
import math

import jax
import jax.numpy as jnp
from jax import lax
from jax.experimental import pallas as pl
from jax.experimental.pallas import tpu as pltpu
from jax.sharding import PartitionSpec as P

D = 768
HEADS = 6
HD = 64
G = 2
K = 9
SEQ = 512


EPSILON = 1e-06
MESH = pl.DeviceIdType.MESH
BLOCKS = 16
HALF = BLOCKS // 2


def place():
    dp, y = lax.axis_index("dp"), lax.axis_index("fsdp")
    return dp, dp // 4, (dp // 2) % 2, dp % 2, y


def partners(dp, x, core, y):
    return (dp + 1 - 2 * core, y), (dp + 2 - 4 * x, y), (dp, 1 - y)


def meet(peers, others):
    barrier = pltpu.get_barrier_semaphore()
    for peer in peers:
        pl.semaphore_signal(barrier, inc=1, device_id=peer, device_id_type=MESH)
    count = len(peers)
    for there, peer in others:

        @pl.when(there)
        def _():
            pl.semaphore_signal(barrier, inc=1, device_id=peer, device_id_type=MESH)

        count = count + there.astype(jnp.int32)
    pl.semaphore_wait(barrier, count)


def send(src, dst, send_sem, recv_sem, device):
    return pltpu.make_async_remote_copy(
        src_ref=src,
        dst_ref=dst,
        send_sem=send_sem,
        recv_sem=recv_sem,
        device_id=device,
        device_id_type=MESH,
    )


def gather_all(packed, mesh):
    if mesh is None:
        return packed
    full = lax.all_gather(packed, ("dp", "fsdp"), axis=1, tiled=False)
    return full.reshape(BLOCKS, D, packed.shape[2])


W = D // G
F32, BF16 = jnp.float32, jnp.bfloat16
PAD = 8


def nn(a, b):
    return lax.dot_general(a, b, (((1,), (0,)), ((), ())), preferred_element_type=F32)


def nt(a, b):
    return lax.dot_general(a, b, (((1,), (1,)), ((), ())), preferred_element_type=F32)


def tn(a, b):
    return lax.dot_general(a, b, (((0,), (0,)), ((), ())), preferred_element_type=F32)


def spread(rows):
    head = lax.broadcasted_iota(jnp.int32, (rows, W), 0) % 8
    channel = lax.broadcasted_iota(jnp.int32, (rows, W), 1) // HD
    return (head == channel).astype(F32).astype(BF16)


def forward_kernel(
    len_ref,
    hid_ref,
    wa_ref,
    wb_ref,
    wpt_ref,
    depth_ref,
    kmt_ref,
    x_ref,
    proj_ref,
    dl_ref,
    kc_ref,
    wt_ref,
    lse_ref,
    ctx_ref,
    xs,
    sv,
    ot,
):
    length = len_ref[pl.program_id(0)]
    inside = lax.broadcasted_iota(jnp.int32, (SEQ, 1), 0) < length
    x = jnp.where(inside, hid_ref[0], jnp.zeros((), BF16))
    x_ref[0] = x
    xs[0:PAD] = jnp.zeros((PAD, D), F32)
    xs[PAD + SEQ :] = jnp.zeros((PAD, D), F32)
    xs[PAD : PAD + SEQ] = x.astype(F32)
    sv[0:PAD] = jnp.zeros((PAD, W), F32)
    sv[PAD + SEQ :] = jnp.zeros((PAD, W), F32)

    for b in range(4):
        part = nn(x_ref[0], (wa_ref, wb_ref)[b // 2][b % 2]).astype(BF16)
        proj_ref[0, :, b * W : (b + 1) * W] = part
        if b == 3:
            sv[PAD : PAD + SEQ] = part.astype(F32)

    def column(c, carry):
        lane = pl.ds(pl.multiple_of(c * 128, 128), 128)
        for r in range(8):
            total = jnp.zeros((64, 128), F32)
            for k in range(K):
                start = PAD + r * 64 + k - K // 2
                total = total + xs[start : start + 64, lane] * depth_ref[k : k + 1, lane]
            dl_ref[0, r * 64 : (r + 1) * 64, lane] = total.astype(BF16)
        return carry

    lax.fori_loop(0, D // 128, column, 0)
    kc_ref[0] = nn(dl_ref[0], wpt_ref[0])
    mk = (kc_ref[0] * proj_ref[0, :, 0:W].astype(F32)).astype(BF16)
    logits = nt(kmt_ref[...], mk)
    top = logits[0:8]
    for k in range(1, K):
        top = jnp.maximum(top, logits[k * 8 : k * 8 + 8])
    parts = [jnp.exp(logits[k * 8 : k * 8 + 8] - top) for k in range(K)]
    inverse = 1.0 / sum(parts)
    both = []
    for k in range(K):
        weight = parts[k] * inverse
        wt_ref[0, k * 8 : k * 8 + 8] = weight
        high = weight.astype(BF16).astype(F32)
        both.append(jnp.concatenate([high, weight - high], axis=0).astype(BF16))
    e16 = spread(16)
    for r in range(4):
        total = jnp.zeros((128, W), F32)
        for k in range(K):
            start = PAD + r * 128 + k - K // 2
            total = total + tn(both[k][:, r * 128 : (r + 1) * 128], e16) * sv[start : start + 128]
        ctx_ref[0, r * 128 : (r + 1) * 128, W:] = total.astype(BF16)

    lane_head = lax.broadcasted_iota(jnp.int32, (1, 128), 1) // HD
    bias = jnp.where(inside, 0.0, -1e30).astype(F32)

    def pair(p, carry):
        def slab(part):
            return proj_ref[0, :, pl.ds(pl.multiple_of(part * W + p * 128, 128), 128)]

        q2, k2, v2 = slab(0), slab(1), slab(2)
        for h in range(2):
            scale = jnp.where(lane_head == h, 1.0 / math.sqrt(HD), 0.0).astype(BF16)
            scores = nt(k2, q2 * scale) + bias
            peak = jnp.max(scores, axis=0, keepdims=True)
            power = jnp.exp(scores - peak)
            total = jnp.sum(power, axis=0, keepdims=True)
            lse_ref[0, pl.ds(p * 2 + h, 1)] = peak + jnp.log(total)
            probs = (power * (1.0 / total)).astype(BF16)
            ot[h * HD : (h + 1) * HD] = tn(v2, probs)[h * HD : (h + 1) * HD]
        ctx_ref[0, :, pl.ds(pl.multiple_of(p * 128, 128), 128)] = ot[...].T.astype(BF16)
        return carry

    lax.fori_loop(0, HEADS // 2, pair, 0)


def forward(lengths, hidden, full, depth, kmt):
    rows = hidden.shape[0]

    def per_row(*shape):
        return pl.BlockSpec((1,) + shape, lambda r: (r, 0, 0))

    def out(dtype, *shape):
        return jax.ShapeDtypeStruct((rows,) + shape, dtype)

    return pl.pallas_call(
        forward_kernel,
        grid=(rows,),
        out_shape=(
            out(BF16, SEQ, D),
            out(BF16, SEQ, 4 * W),
            out(BF16, SEQ, D),
            out(F32, SEQ, W),
            out(F32, 8 * K, SEQ),
            out(F32, 8, SEQ),
            out(BF16, SEQ, D),
        ),
        in_specs=[
            pl.BlockSpec(memory_space=pltpu.SMEM),
            per_row(SEQ, D),
            pl.BlockSpec((2, D, W), lambda r: (5, 0, 0)),
            pl.BlockSpec((2, D, W), lambda r: (6, 0, 0)),
            pl.BlockSpec((1, D, W), lambda r: (14, 0, 0)),
            pl.BlockSpec((16, D), lambda r: (0, 0)),
            pl.BlockSpec((8 * K, W), lambda r: (0, 0)),
        ],
        out_specs=(
            per_row(SEQ, D),
            per_row(SEQ, 4 * W),
            per_row(SEQ, D),
            per_row(SEQ, W),
            per_row(8 * K, SEQ),
            per_row(8, SEQ),
            per_row(SEQ, D),
        ),
        scratch_shapes=[
            pltpu.VMEM((SEQ + 2 * PAD, D), F32),
            pltpu.VMEM((SEQ + 2 * PAD, W), F32),
            pltpu.VMEM((128, SEQ), F32),
        ],
        compiler_params=pltpu.CompilerParams(vmem_limit_bytes=56 * 1024 * 1024),
        name="mixer_forward",
    )(lengths, hidden, full, full, full, depth, kmt)


TILE = 256
CHUNK = 16
PART = 256


def ffn_kernel(
    len_ref,
    ctx_ref,
    x_ref,
    og_ref,
    wout_ref,
    wdn_ref,
    wup_ref,
    gb_ref,
    y_ref,
    act_ref,
    gpre_ref,
    fb_ref,
    gffn_ref,
    gmix_ref,
    gr1_ref,
    gctx_ref,
    stat_ref,
    mix,
    first,
    n1,
    inv,
    ffn,
    pre,
    dg,
    gr2,
):
    step = pl.program_id(0)
    row = step // (SEQ // TILE)
    base = (step % (SEQ // TILE)) * TILE
    left = len_ref[row] - base

    @pl.when(step == 0)
    def _():
        stat_ref[...] = jnp.zeros_like(stat_ref)

    for b in range(2):
        mix[:, b * W : (b + 1) * W] = nn(ctx_ref[...], wout_ref[b])

    def mask_of(i):
        return (lax.broadcasted_iota(jnp.int32, (CHUNK, 1), 0) + i * CHUNK < left).astype(F32)

    def fold(values):
        return jnp.sum(values.reshape(CHUNK // 8, 8, D), axis=0)

    def tally(k, values):
        stat_ref[k] = stat_ref[k] + fold(values)

    def rows_of(i):
        return pl.ds(pl.multiple_of(i * CHUNK, CHUNK), CHUNK)

    def norm(values):
        average = jnp.mean(values, axis=-1, keepdims=True)
        centered = values - average
        inverse = lax.rsqrt(jnp.mean(centered * centered, axis=-1, keepdims=True) + EPSILON)
        return centered * inverse, inverse

    def norm_back(grad, normed, inverse, gain):
        scaled = grad * gain
        mean = jnp.mean(scaled, axis=-1, keepdims=True)
        other = jnp.mean(scaled * normed, axis=-1, keepdims=True)
        return inverse * (scaled - mean - normed * other)

    def norm_one(i, carry):
        rows = rows_of(i)
        xf, mixed = x_ref[rows].astype(F32), mix[rows]
        normed, inverse = norm(xf + mixed)
        result = normed * gb_ref[0:1] + gb_ref[2:3]
        n1[rows] = normed
        inv[rows] = jnp.broadcast_to(inverse, (CHUNK, 128))
        first[rows] = result
        for g in range(G):
            fb_ref[g, rows] = result[:, g * W : (g + 1) * W].astype(BF16)
        tally(0, xf * xf)
        tally(1, mixed * mixed * mask_of(i))
        return carry

    lax.fori_loop(0, TILE // CHUNK, norm_one, 0)

    def part_of(c):
        return c // 3, pl.ds(c % 3 * PART, PART)

    def expand(c):
        s, units = part_of(c)
        pre[c % 2] = nt(fb_ref[s // 2], wup_ref[s, units])

    def gelu(c):
        s, units = part_of(c)
        for r in range(TILE // 32):
            rows = slice(r * 32, (r + 1) * 32)
            v = pre[c % 2, rows]
            phi = 0.5 + 0.5 * lax.erf(v * math.sqrt(0.5))
            act_ref[s, rows, units] = (v * phi).astype(BF16)
            dg[s, rows, units] = phi + v * jnp.exp(v * v * -0.5) * (1.0 / math.sqrt(2.0 * math.pi))

    def contract(s):
        g = s // 2
        part = nn(act_ref[s], wdn_ref[s])
        lanes = slice(g * W, (g + 1) * W)
        if s % 2 == 0:
            ffn[:, lanes] = part
        else:
            ffn[:, lanes] += part

    parts = 4 * D // PART
    expand(0)
    for c in range(parts):
        if c + 1 < parts:
            expand(c + 1)
        if c % 3 == 0 and c > 0:
            contract(c // 3 - 1)
        gelu(c)
    contract(3)

    def norm_two(i, carry):
        rows = rows_of(i)
        mask = mask_of(i)
        out = ffn[rows]
        normed, inverse = norm(first[rows] + out)
        y = (normed * gb_ref[1:2] + gb_ref[3:4]) * mask
        y_ref[rows] = y.astype(BF16)
        grad = og_ref[rows].astype(F32) * mask
        back = norm_back(grad, normed, inverse, gb_ref[1:2])
        gr2[rows] = back
        for g in range(G):
            gffn_ref[g, rows] = back[:, g * W : (g + 1) * W].astype(BF16)
        tally(2, out * out * mask)
        tally(3, y * y)
        tally(5, grad * normed)
        tally(7, grad)
        return carry

    lax.fori_loop(0, TILE // CHUNK, norm_two, 0)

    for c in range(parts):
        s, units = part_of(c)
        gpre_ref[s, :, units] = (nt(gffn_ref[s // 2], wdn_ref[s, units]) * dg[s, :, units]).astype(BF16)
        if c % 3 == 2:
            lanes = slice(s // 2 * W, (s // 2 + 1) * W)
            gr2[:, lanes] += nn(gpre_ref[s], wup_ref[s])

    def norm_one_back(i, carry):
        rows = rows_of(i)
        grad, normed = gr2[rows], n1[rows]
        back = norm_back(grad, normed, inv[rows, 0:1], gb_ref[0:1])
        gr1_ref[rows] = back
        for g in range(2):
            gmix_ref[g, rows] = back[:, g * W : (g + 1) * W].astype(BF16)
        tally(4, grad * normed)
        tally(6, grad)
        return carry

    lax.fori_loop(0, TILE // CHUNK, norm_one_back, 0)
    gctx_ref[...] = (
        nt(gmix_ref[0], wout_ref[0]) + nt(gmix_ref[1], wout_ref[1])
    ).astype(BF16)


def feed_forward(lengths, ctx, x, out_grad, full, gb):
    tokens = x.shape[0]

    def per_tile(width):
        return pl.BlockSpec((TILE, width), lambda i: (i, 0))

    def out(dtype, width):
        return jax.ShapeDtypeStruct((tokens, width), dtype)

    def slabs(count, width):
        return pl.BlockSpec((count, TILE, width), lambda i: (0, i, 0))

    def slabs_out(count, width):
        return jax.ShapeDtypeStruct((count, tokens, width), BF16)

    return pl.pallas_call(
        ffn_kernel,
        grid=(tokens // TILE,),
        out_shape=(
            out(BF16, D),
            slabs_out(4, D),
            slabs_out(4, D),
            slabs_out(G, W),
            slabs_out(G, W),
            slabs_out(2, W),
            out(F32, D),
            out(BF16, D),
            jax.ShapeDtypeStruct((8, 8, D), F32),
        ),
        in_specs=[
            pl.BlockSpec(memory_space=pltpu.SMEM),
            per_tile(D),
            per_tile(D),
            per_tile(D),
            pl.BlockSpec((2, D, W), lambda i: (4, 0, 0)),
            pl.BlockSpec((4, D, W), lambda i: (0, 0, 0)),
            pl.BlockSpec((4, D, W), lambda i: (1, 0, 0)),
            pl.BlockSpec((8, D), lambda i: (0, 0)),
        ],
        out_specs=(
            per_tile(D),
            slabs(4, D),
            slabs(4, D),
            slabs(G, W),
            slabs(G, W),
            slabs(2, W),
            per_tile(D),
            per_tile(D),
            pl.BlockSpec((8, 8, D), lambda i: (0, 0, 0)),
        ),
        scratch_shapes=[
            pltpu.VMEM((TILE, D), F32),
            pltpu.VMEM((TILE, D), F32),
            pltpu.VMEM((TILE, D), F32),
            pltpu.VMEM((TILE, 128), F32),
            pltpu.VMEM((TILE, D), F32),
            pltpu.VMEM((2, TILE, PART), F32),
            pltpu.VMEM((4, TILE, D), F32),
            pltpu.VMEM((TILE, D), F32),
        ],
        compiler_params=pltpu.CompilerParams(vmem_limit_bytes=56 * 1024 * 1024),
        name="feed_forward",
    )(lengths, ctx, x, out_grad, full, full, full, gb)


def backward_kernel(
    len_ref,
    x_ref,
    proj_ref,
    dl_ref,
    kc_ref,
    wt_ref,
    lse_ref,
    gctx_ref,
    gr1_ref,
    wa_ref,
    wb_ref,
    wpt_ref,
    depth_ref,
    kmt_ref,
    gproj_ref,
    gkc_ref,
    gin_ref,
    gkm_ref,
    gdk_ref,
    sv,
    gc,
    xs,
    gd,
    gs,
    gq,
    gt,
    dqt,
):
    row = pl.program_id(0)
    length = len_ref[row]
    inside = lax.broadcasted_iota(jnp.int32, (SEQ, 1), 0) < length

    @pl.when(row == 0)
    def _():
        gkm_ref[...] = jnp.zeros_like(gkm_ref)
        gdk_ref[...] = jnp.zeros_like(gdk_ref)

    for ref, width in ((sv, W), (gc, W), (xs, D), (gd, D)):
        ref[0:PAD] = jnp.zeros((PAD, width), F32)
        ref[PAD + SEQ :] = jnp.zeros((PAD, width), F32)
    sv[PAD : PAD + SEQ] = proj_ref[0, :, 3 * W :].astype(F32)
    gc[PAD : PAD + SEQ] = gctx_ref[0, :, W:].astype(F32)
    xs[PAD : PAD + SEQ] = x_ref[0].astype(F32)

    e16 = spread(16)
    place_row = lax.broadcasted_iota(jnp.int32, (W, 128), 0) // HD
    place_col = lax.broadcasted_iota(jnp.int32, (W, 128), 1)
    both = []
    for k in range(K):
        weight = pltpu.roll(wt_ref[0, k * 8 : k * 8 + 8], (k - K // 2) % SEQ, 1)
        high = weight.astype(BF16).astype(F32)
        both.append(jnp.concatenate([high, weight - high], axis=0).astype(BF16))
    for r in range(4):
        rows = slice(r * 128, (r + 1) * 128)
        spans = jnp.zeros((128, 128), F32)
        total = jnp.zeros((128, W), F32)
        for k in range(K):
            start = PAD + r * 128 + k - K // 2
            product_k = gc[PAD + r * 128 : PAD + (r + 1) * 128] * sv[start : start + 128]
            chosen = (place_col == place_row + 8 * k).astype(F32).astype(BF16)
            spans = spans + nn(product_k.astype(BF16), chosen)
            start = PAD + r * 128 - k + K // 2
            total = total + tn(both[k][:, rows], e16) * gc[start : start + 128]
        gt[:, rows] = spans.T
        gproj_ref[3, rows] = total.astype(BF16)
    center = jnp.zeros((8, SEQ), F32)
    for k in range(K):
        center = center + wt_ref[0, k * 8 : k * 8 + 8] * gt[k * 8 : k * 8 + 8]
    glt = jnp.concatenate(
        [
            wt_ref[0, k * 8 : k * 8 + 8] * (gt[k * 8 : k * 8 + 8] - center)
            for k in range(K)
        ],
        axis=0,
    ).astype(BF16)
    query = proj_ref[0, :, 0:W].astype(F32)
    mk = (kc_ref[0] * query).astype(BF16)
    gkm_ref[...] += nn(glt, mk)
    mixed = tn(glt, kmt_ref[...])
    gkc_ref[0] = (mixed * query).astype(BF16)
    gq[...] = mixed * kc_ref[0]
    gd[PAD : PAD + SEQ] = nt(gkc_ref[0], wpt_ref[0])

    def column(c, carry):
        lane = pl.ds(pl.multiple_of(c * 128, 128), 128)
        sums = [jnp.zeros((8, 128), F32)] * K
        for r in range(8):
            total = jnp.zeros((64, 128), F32)
            center = PAD + r * 64
            grad = gd[center : center + 64, lane]
            for k in range(K):
                start = center + k - K // 2
                sums[k] = sums[k] + jnp.sum(
                    (xs[start : start + 64, lane] * grad).reshape(8, 8, 128), axis=0
                )
                start = center - k + K // 2
                total = total + gd[start : start + 64, lane] * depth_ref[k : k + 1, lane]
            gs[r * 64 : (r + 1) * 64, lane] = total
        for k in range(K):
            gdk_ref[k, :, lane] = gdk_ref[k, :, lane] + sums[k]
        return carry

    lax.fori_loop(0, D // 128, column, 0)

    lane_head = lax.broadcasted_iota(jnp.int32, (1, 128), 1) // HD
    bias = jnp.where(inside, 0.0, -1e30).astype(F32)

    def pair(p, carry):
        def lanes(part):
            return pl.ds(pl.multiple_of(part * W + p * 128, 128), 128)

        q2, k2, v2 = (proj_ref[0, :, lanes(part)] for part in range(3))
        g2 = gctx_ref[0, :, lanes(0)]
        results = []
        for h in range(2):
            mine = lane_head == h
            scale = jnp.where(mine, 1.0 / math.sqrt(HD), 0.0).astype(BF16)
            scores = nt(k2, q2 * scale) + bias
            probs = jnp.exp(scores - lse_ref[0, pl.ds(p * 2 + h, 1)])
            grads = nt(v2 * jnp.where(mine, 1.0, 0.0).astype(BF16), g2)
            correction = jnp.sum(probs * grads, axis=0, keepdims=True)
            grad_scores = (probs * (grads - correction)).astype(BF16)
            dqt[h * HD : (h + 1) * HD] = tn(k2, grad_scores)[h * HD : (h + 1) * HD]
            results.append((nn(grad_scores, q2), nn(probs.astype(BF16), g2)))
        low = lane_head == 0
        scale = 1.0 / math.sqrt(HD)
        gproj_ref[0, :, lanes(0)] = (dqt[...].T * scale + gq[:, lanes(0)]).astype(BF16)
        gproj_ref[1, :, lanes(0)] = (jnp.where(low, results[0][0], results[1][0]) * scale).astype(BF16)
        gproj_ref[2, :, lanes(0)] = jnp.where(low, results[0][1], results[1][1]).astype(BF16)
        return carry

    lax.fori_loop(0, HEADS // 2, pair, 0)

    for b in range(4):
        gs[...] += nt(gproj_ref[b], (wa_ref, wb_ref)[b // 2][b % 2])
    gin_ref[0] = jnp.where(inside, gr1_ref[0] + gs[...], 0.0).astype(BF16)


def backward(lengths, x, proj, dl, kc, wt, lse, gctx, gr1, full, depth, kmt):
    rows = x.shape[0]

    def per_row(*shape):
        return pl.BlockSpec((1,) + shape, lambda r: (r, 0, 0))

    def out(dtype, *shape):
        return jax.ShapeDtypeStruct((rows,) + shape, dtype)

    return pl.pallas_call(
        backward_kernel,
        grid=(rows,),
        out_shape=(
            jax.ShapeDtypeStruct((4, rows * SEQ, W), BF16),
            out(BF16, SEQ, W),
            out(BF16, SEQ, D),
            jax.ShapeDtypeStruct((8 * K, W), F32),
            jax.ShapeDtypeStruct((K, 8, D), F32),
        ),
        in_specs=[
            pl.BlockSpec(memory_space=pltpu.SMEM),
            per_row(SEQ, D),
            per_row(SEQ, 4 * W),
            per_row(SEQ, D),
            per_row(SEQ, W),
            per_row(8 * K, SEQ),
            per_row(8, SEQ),
            per_row(SEQ, D),
            per_row(SEQ, D),
            pl.BlockSpec((2, D, W), lambda r: (5, 0, 0)),
            pl.BlockSpec((2, D, W), lambda r: (6, 0, 0)),
            pl.BlockSpec((1, D, W), lambda r: (14, 0, 0)),
            pl.BlockSpec((16, D), lambda r: (0, 0)),
            pl.BlockSpec((8 * K, W), lambda r: (0, 0)),
        ],
        out_specs=(
            pl.BlockSpec((4, SEQ, W), lambda r: (0, r, 0)),
            per_row(SEQ, W),
            per_row(SEQ, D),
            pl.BlockSpec((8 * K, W), lambda r: (0, 0)),
            pl.BlockSpec((K, 8, D), lambda r: (0, 0, 0)),
        ),
        scratch_shapes=[
            pltpu.VMEM((SEQ + 2 * PAD, W), F32),
            pltpu.VMEM((SEQ + 2 * PAD, W), F32),
            pltpu.VMEM((SEQ + 2 * PAD, D), F32),
            pltpu.VMEM((SEQ + 2 * PAD, D), F32),
            pltpu.VMEM((SEQ, D), F32),
            pltpu.VMEM((SEQ, W), F32),
            pltpu.VMEM((128, SEQ), F32),
            pltpu.VMEM((128, SEQ), F32),
        ],
        compiler_params=pltpu.CompilerParams(vmem_limit_bytes=56 * 1024 * 1024),
        name="mixer_backward",
    )(lengths, x, proj, dl, kc, wt, lse, gctx, gr1, full, full, full, depth, kmt)


def pack(in_weight, depth_kernel, point_weight, kernel_weight, out_weight, up_weight, down_weight, norm_gains, norm_biases):
    rows = in_weight.shape[0]

    def halves(grouped):
        return grouped.reshape(G * 2, rows, W)

    kernel = kernel_weight.reshape(K, rows, 3).transpose(1, 0, 2).reshape(rows, 3 * K)
    small = jnp.concatenate([depth_kernel.T, kernel, norm_gains.T, norm_biases.T], axis=1)
    small = jnp.pad(small, ((0, 0), (0, W - small.shape[1])))
    return jnp.concatenate(
        [
            halves(down_weight),
            halves(up_weight.transpose(0, 2, 1)),
            out_weight.reshape(rows, 2, W).transpose(1, 0, 2),
            in_weight.reshape(rows, 4, W).transpose(1, 0, 2),
            point_weight[None],
            small[None],
        ],
        axis=0,
    )


def unpack(shard):
    rows = shard.shape[1]
    small = shard[15]
    kernel = small[:, K : 4 * K].reshape(rows, K, 3).transpose(1, 0, 2).reshape(K, 3 * rows)
    return (
        shard[10:14].transpose(1, 0, 2).reshape(rows, 4 * W),
        small[:, :K].T,
        shard[14],
        kernel,
        shard[8:10].transpose(1, 0, 2).reshape(rows, 2 * W),
        shard[4:8].reshape(G, 2 * rows, W).transpose(0, 2, 1),
        shard[0:4].reshape(G, 2 * rows, W),
        small[:, 4 * K : 4 * K + 2].T,
        small[:, 4 * K + 2 : 4 * K + 4].T,
    )


def constants(full):
    small = full[15].astype(F32)
    depth = jnp.pad(small[:, :K].T, ((0, 16 - K), (0, 0)))
    kernel = small[:, K : 4 * K].reshape(D, K, 3).transpose(1, 0, 2).reshape(K, W, HEADS)
    kmt = jnp.pad(kernel.transpose(0, 2, 1), ((0, 0), (0, 8 - HEADS), (0, 0)))
    kmt = kmt.reshape(8 * K, W).astype(BF16)
    gb = jnp.pad(small[:, 4 * K : 4 * K + 4].T, ((0, 4), (0, 0)))
    return depth, kmt, gb


def layer(mesh, hidden, lengths, packed, out_grad):
    rows = hidden.shape[0]
    tokens = rows * SEQ
    if fused(mesh, rows):
        full, depth, kmt, gb, x, proj, dl, kc, wt, lse, ctx = gather_forward(
            mesh, lengths, packed, hidden
        )
    else:
        full = gather_all(packed, mesh)
        depth, kmt, gb = constants(full)
        x, proj, dl, kc, wt, lse, ctx = forward(lengths, hidden, full, depth, kmt)
    flat_x, flat_ctx = x.reshape(tokens, D), ctx.reshape(tokens, D)
    y, act, gpre, fb, gffn, gmix, gr1, gctx, stat = feed_forward(
        lengths, flat_ctx, flat_x, out_grad.reshape(tokens, D), full, gb
    )
    gctx, gr1 = gctx.reshape(rows, SEQ, D), gr1.reshape(rows, SEQ, D)
    if fused(mesh, rows):
        gin, shard, totals = backward_scatter(
            mesh, lengths, x, proj, dl, kc, wt, lse, gctx, gr1, full, depth, kmt, ctx, gmix, act, gffn, gpre, fb, stat
        )
        return y.reshape(rows, SEQ, D), gin, shard, totals
    gproj, gkc, gin, gkm, gdk = backward(
        lengths, x, proj, dl, kc, wt, lse, gctx, gr1, full, depth, kmt
    )
    stat = jnp.sum(stat, axis=1)
    grad_kernel = gkm.reshape(K, 8, W)[:, :HEADS].transpose(0, 2, 1).reshape(K, D, 3)
    small = jnp.concatenate(
        [
            jnp.sum(gdk, axis=1).T,
            grad_kernel.transpose(1, 0, 2).reshape(D, 3 * K),
            stat[4:8].T,
        ],
        axis=1,
    )
    small = jnp.pad(small, ((0, 0), (0, W - small.shape[1]))).astype(BF16)
    local = weight_grads(
        flat_x, dl.reshape(tokens, D), gproj, gkc.reshape(tokens, W), flat_ctx, gmix, act, gffn, gpre, fb, small
    )
    sums = jnp.concatenate([jnp.sum(stat[0:4], axis=1), jnp.sum(lengths).astype(F32)[None]])
    if mesh is None:
        return y.reshape(rows, SEQ, D), gin, local.astype(F32), sums[None]
    devices = mesh.shape["dp"] * mesh.shape["fsdp"]
    shard = lax.psum_scatter(
        local.reshape(BLOCKS, devices, D // devices, W),
        ("dp", "fsdp"),
        scatter_dimension=1,
        tiled=False,
    )
    return (
        y.reshape(rows, SEQ, D),
        gin,
        shard.astype(F32),
        lax.psum(sums, ("dp", "fsdp"))[None],
    )


def fused(mesh, rows):
    return mesh is not None and mesh.shape["fsdp"] == 2 and mesh.shape["dp"] % 4 == 0 and rows == 2


def weight_grads(x, dl, gproj, gkc, ctx, gmix, act, gffn, gpre, fb, small):
    pairs = [(act[s], gffn[s // 2]) for s in range(4)]
    pairs += [(gpre[s], fb[s // 2]) for s in range(4)]
    pairs += [(ctx, gmix[b]) for b in range(2)]
    pairs += [(x, gproj[b]) for b in range(4)]
    pairs += [(dl, gkc)]
    return jnp.stack([tn(a, b).astype(BF16) for a, b in pairs] + [small])


def picked(height, rule):
    row = lax.broadcasted_iota(jnp.int32, (height, 128), 0)
    lane = lax.broadcasted_iota(jnp.int32, (height, 128), 1)
    return rule(row, lane).astype(F32).astype(BF16)


def gather_engine(depth, g_ref, low, high, sems):
    dp, z, x, core, y = place()
    c_dev, x_dev, y_dev = partners(dp, x, core, y)
    up_dev, down_dev = (dp + 4, y), (dp - 4, y)
    steps = 2 * depth - 1
    size = (high - low) // 2
    every, halves = pl.ds(low, 2 * size), (pl.ds(low, size), pl.ds(low + size, size))

    def target(q):
        return z + ((q + 1) // 2) * (1 - 2 * (q % 2))

    def z_copy(j, way, device):
        slab = g_ref.at[every, j, x, core, y]
        return send(slab, slab, sems[0].at[way, j], sems[1].at[j], device)

    def x_copy(j):
        slab = g_ref.at[every, j, x, core, y]
        return send(slab, slab, sems[2].at[j], sems[3].at[j], x_dev)

    def y_copy(j):
        slab = g_ref.at[every, j, x, core, y]
        return send(slab, slab, sems[4].at[j], sems[5].at[j], y_dev)

    def d_copy(j, half):
        if half == 0:
            slab = g_ref.at[halves[0], j, 1 - x, core, y]
            return send(slab, slab, sems[6].at[0, j], sems[7].at[0, j], y_dev)
        slab = g_ref.at[halves[1], j, x, core, 1 - y]
        return send(slab, slab, sems[6].at[1, j], sems[7].at[1, j], x_dev)

    def c_copy(j, a, b):
        slab = g_ref.at[every, j, (x + a) % 2, core, (y + b) % 2]
        return send(slab, slab, sems[8].at[2 * a + b, j], sems[9].at[2 * a + b, j], c_dev)

    def c_arrival(j, a, b):
        slab = g_ref.at[every, j, (x + a) % 2, 1 - core, (y + b) % 2]
        return send(slab, slab, sems[8].at[2 * a + b, j], sems[9].at[2 * a + b, j], c_dev)

    def x_arrival(j):
        slab = g_ref.at[every, j, 1 - x, core, y]
        return send(slab, slab, sems[2].at[j], sems[3].at[j], x_dev)

    def y_arrival(j):
        slab = g_ref.at[every, j, x, core, 1 - y]
        return send(slab, slab, sems[4].at[j], sems[5].at[j], y_dev)

    def d_arrival(j, half):
        slab = g_ref.at[halves[half], j, 1 - x, core, 1 - y]
        return send(slab, slab, sems[6].at[half, j], sems[7].at[half, j], y_dev if half == 0 else x_dev)

    def first(j):
        @pl.when(j != z)
        def _():
            z_copy(j, 0, up_dev).wait_recv()

        @pl.when((j <= z) & (z + 1 < depth))
        def _():
            z_copy(j, 0, up_dev).start()

        @pl.when((j >= z) & (z > 0))
        def _():
            z_copy(j, 1, down_dev).start()

        x_copy(j).start()
        y_copy(j).start()
        c_copy(j, 0, 0).start()

    def second(j):
        x_arrival(j).wait_recv()
        d_copy(j, 0).start()
        c_copy(j, 1, 0).start()
        y_arrival(j).wait_recv()
        d_copy(j, 1).start()
        c_copy(j, 0, 1).start()

    def third(j):
        d_arrival(j, 0).wait_recv()
        d_arrival(j, 1).wait_recv()
        c_copy(j, 1, 1).start()

    def stage(q, work):
        j = target(q)

        @pl.when((q >= 0) & (q < steps) & (j >= 0) & (j < depth))
        def _():
            work(j)

    def arrive(j, carry):
        for a in range(2):
            for b in range(2):
                c_arrival(j, a, b).wait_recv()
        return carry

    def step(q, carry):
        stage(q, first)
        stage(q - 1, second)
        stage(q - 2, third)
        return carry

    def finish(j, carry):
        for a in range(2):
            for b in range(2):
                c_copy(j, a, b).wait_send()
        x_copy(j).wait_send()
        y_copy(j).wait_send()
        d_copy(j, 0).wait_send()
        d_copy(j, 1).wait_send()

        @pl.when((j <= z) & (z + 1 < depth))
        def _():
            z_copy(j, 0, up_dev).wait_send()

        @pl.when((j >= z) & (z > 0))
        def _():
            z_copy(j, 1, down_dev).wait_send()

        return carry

    return step, arrive, finish


def gather_forward_kernel(
    depth,
    len_ref,
    p_ref,
    hid_hbm,
    g_ref,
    taps_ref,
    kmt_ref,
    gb_ref,
    x_out,
    proj_out,
    dl_out,
    kc_out,
    wt_out,
    lse_out,
    ctx_out,
    hid_ref,
    x_ref,
    proj_ref,
    dl_ref,
    kc_ref,
    wt_ref,
    lse_ref,
    ctx_ref,
    win_ref,
    wpt_ref,
    small_ref,
    small,
    xs,
    sv,
    ot,
    own_sem,
    in_sem,
    out_sem,
    *sems,
):
    dp, z, x, core, y = place()
    rows = hid_ref.shape[0]
    depth_ref = taps_ref
    load = pltpu.make_async_copy(hid_hbm, hid_ref, in_sem.at[0])
    load.start()
    own = pltpu.make_async_copy(p_ref, g_ref.at[:, z, x, core, y], own_sem)
    own.start()
    xs[0:PAD] = jnp.zeros((PAD, D), F32)
    xs[PAD + SEQ :] = jnp.zeros((PAD, D), F32)
    sv[0:PAD] = jnp.zeros((PAD, W), F32)
    sv[PAD + SEQ :] = jnp.zeros((PAD, W), F32)
    meet(
        partners(dp, x, core, y),
        ((z + 1 < depth, (dp + 4, y)), (z > 0, (dp - 4, y))),
    )
    own.wait()
    count = len(sems) // 2
    soon = gather_engine(depth, g_ref, 10, 16, sems[:count])
    later = gather_engine(depth, g_ref, 0, 10, sems[count:])
    lax.fori_loop(0, 2 * depth + 1, soon[0], 0)
    lax.fori_loop(0, depth, soon[1], 0)
    inputs = [
        pltpu.make_async_copy(g_ref.at[pl.ds(first, size)], target, in_sem.at[1 + i])
        for i, (first, size, target) in enumerate(
            ((15, 1, small_ref), (10, 4, win_ref), (14, 1, wpt_ref))
        )
    ]
    for copy in inputs:
        copy.start()
    later[0](0, 0)
    load.wait()
    inputs[0].wait()
    values = small_ref[...].reshape(D, W)[:, 0:128]
    small[...] = values.astype(F32)
    taps_ref[...] = nt(picked(16, lambda row, lane: (row < K) & (lane == row)), values)
    gb_ref[...] = nt(picked(8, lambda row, lane: (row < 4) & (lane == row + 4 * K)), values)
    kernel = jnp.zeros((8 * K, W), F32)
    for odd in range(2):
        pick = picked(
            8 * K,
            lambda row, lane: (row % 8 >= 3 * odd)
            & (row % 8 < 3 * odd + 3)
            & (lane == K + row // 8 * 3 + row % 8 - 3 * odd),
        )
        kernel = kernel + nt(pick, small[pl.ds(odd, W, stride=2)].astype(BF16))
    kmt_ref[...] = kernel.astype(BF16)
    for copy in inputs[1:]:
        copy.wait()

    def inside_of(r):
        return lax.broadcasted_iota(jnp.int32, (SEQ, 1), 0) < len_ref[r]

    def piece_project(r):
        inside = inside_of(r)
        x = jnp.where(inside, hid_ref[r], jnp.zeros((), BF16))
        x_ref[r] = x
        xs[PAD : PAD + SEQ] = x.astype(F32)

        for b in range(4):
            part = nn(x_ref[r], win_ref[b].reshape(D, W)).astype(BF16)
            proj_ref[r, :, b * W : (b + 1) * W] = part
            if b == 3:
                sv[PAD : PAD + SEQ] = part.astype(F32)

    def piece_columns(r):
        def column(c, carry):
            lane = pl.ds(pl.multiple_of(c * 128, 128), 128)
            for n in range(8):
                total = jnp.zeros((64, 128), F32)
                for k in range(K):
                    start = PAD + n * 64 + k - K // 2
                    total = total + xs[start : start + 64, lane] * depth_ref[k : k + 1, lane]
                dl_ref[r, n * 64 : (n + 1) * 64, lane] = total.astype(BF16)
            return carry

        lax.fori_loop(0, D // 128, column, 0)

    def piece_span(r):
        kc_ref[r] = nn(dl_ref[r], wpt_ref[0].reshape(D, W))
        mk = (kc_ref[r] * proj_ref[r, :, 0:W].astype(F32)).astype(BF16)
        logits = nt(kmt_ref[...], mk)
        top = logits[0:8]
        for k in range(1, K):
            top = jnp.maximum(top, logits[k * 8 : k * 8 + 8])
        parts = [jnp.exp(logits[k * 8 : k * 8 + 8] - top) for k in range(K)]
        inverse = 1.0 / sum(parts)
        both = []
        for k in range(K):
            weight = parts[k] * inverse
            wt_ref[r, k * 8 : k * 8 + 8] = weight
            high = weight.astype(BF16).astype(F32)
            both.append(jnp.concatenate([high, weight - high], axis=0).astype(BF16))
        e16 = spread(16)
        for n in range(4):
            total = jnp.zeros((128, W), F32)
            for k in range(K):
                start = PAD + n * 128 + k - K // 2
                total = total + tn(both[k][:, n * 128 : (n + 1) * 128], e16) * sv[start : start + 128]
            ctx_ref[r, n * 128 : (n + 1) * 128, W:] = total.astype(BF16)

    def piece_pairs(r, first, stop):
        inside = inside_of(r)
        lane_head = lax.broadcasted_iota(jnp.int32, (1, 128), 1) // HD
        bias = jnp.where(inside, 0.0, -1e30).astype(F32)

        def pair(p, carry):
            def slab(part):
                return proj_ref[r, :, pl.ds(pl.multiple_of(part * W + p * 128, 128), 128)]

            q2, k2, v2 = slab(0), slab(1), slab(2)
            for h in range(2):
                scale = jnp.where(lane_head == h, 1.0 / math.sqrt(HD), 0.0).astype(BF16)
                scores = nt(k2, q2 * scale) + bias
                peak = jnp.max(scores, axis=0, keepdims=True)
                power = jnp.exp(scores - peak)
                total = jnp.sum(power, axis=0, keepdims=True)
                lse_ref[r, pl.ds(p * 2 + h, 1)] = peak + jnp.log(total)
                probs = (power * (1.0 / total)).astype(BF16)
                ot[h * HD : (h + 1) * HD] = tn(v2, probs)[h * HD : (h + 1) * HD]
            ctx_ref[r, :, pl.ds(pl.multiple_of(p * 128, 128), 128)] = ot[...].T.astype(BF16)
            return carry

        lax.fori_loop(first, stop, pair, 0)


    pairs = (
        (x_ref, x_out),
        (proj_ref, proj_out),
        (dl_ref, dl_out),
        (kc_ref, kc_out),
        (wt_ref, wt_out),
        (lse_ref, lse_out),
        (ctx_ref, ctx_out),
    )

    def store(r):
        return [
            pltpu.make_async_copy(source.at[r], target.at[r], out_sem.at[i, r])
            for i, (source, target) in enumerate(pairs)
        ]

    def tick(t, carry):
        row = t // 5

        def when(i, work):
            @pl.when(t % 5 == i)
            def _():
                work()

        when(0, lambda: piece_project(row))
        when(1, lambda: piece_columns(row))
        when(2, lambda: piece_span(row))
        when(3, lambda: piece_pairs(row, 0, 2))

        def close():
            piece_pairs(row, 2, 3)
            for copy in store(row):
                copy.start()

        when(4, close)

        @pl.when(t < 2 * depth)
        def _():
            later[0](t + 1, 0)

        return carry

    lax.fori_loop(0, 5 * rows, tick, 0)
    for t in range(5 * rows, 2 * depth):
        later[0](jnp.int32(t + 1), 0)
    lax.fori_loop(0, depth, later[1], 0)
    lax.fori_loop(0, depth, soon[2], 0)
    lax.fori_loop(0, depth, later[2], 0)

    def drain(r, carry):
        for copy in store(r):
            copy.wait()
        return carry

    lax.fori_loop(0, rows, drain, 0)


def gather_forward(mesh, lengths, packed, hidden):
    dp, fsdp = mesh.shape["dp"], mesh.shape["fsdp"]
    _, share, _ = packed.shape
    depth = dp // 4
    rows = hidden.shape[0]
    dma = pltpu.SemaphoreType.DMA
    anywhere = pl.BlockSpec(memory_space=pl.ANY)
    inside = pl.BlockSpec(memory_space=pltpu.VMEM)
    kinds = (
        (BF16, SEQ, D),
        (BF16, SEQ, 4 * W),
        (BF16, SEQ, D),
        (F32, SEQ, W),
        (F32, 8 * K, SEQ),
        (F32, 8, SEQ),
        (BF16, SEQ, D),
    )
    sems = [
        dma((2, depth)),
        dma((depth,)),
        dma((depth,)),
        dma((depth,)),
        dma((depth,)),
        dma((depth,)),
        dma((2, depth)),
        dma((2, depth)),
        dma((4, depth)),
        dma((4, depth)),
    ]
    outs = pl.pallas_call(
        functools.partial(gather_forward_kernel, depth),
        out_shape=(
            jax.ShapeDtypeStruct((BLOCKS, depth, 2, 2, 2, share, W), BF16),
            jax.ShapeDtypeStruct((16, D), F32),
            jax.ShapeDtypeStruct((8 * K, W), BF16),
            jax.ShapeDtypeStruct((8, D), F32),
        )
        + tuple(jax.ShapeDtypeStruct((rows, a, b), kind) for kind, a, b in kinds),
        in_specs=[pl.BlockSpec(memory_space=pltpu.SMEM), inside, anywhere],
        out_specs=(anywhere, inside, inside, inside) + (anywhere,) * 7,
        scratch_shapes=[pltpu.VMEM((rows, SEQ, D), BF16)]
        + [pltpu.VMEM((rows, a, b), kind) for kind, a, b in kinds]
        + [
            pltpu.VMEM((4, depth, 2, 2, 2, share, W), BF16),
            pltpu.VMEM((1, depth, 2, 2, 2, share, W), BF16),
            pltpu.VMEM((1, depth, 2, 2, 2, share, W), BF16),
            pltpu.VMEM((D, 128), F32),
            pltpu.VMEM((SEQ + 2 * PAD, D), F32),
            pltpu.VMEM((SEQ + 2 * PAD, W), F32),
            pltpu.VMEM((128, SEQ), F32),
            dma(()),
            dma((4,)),
            dma((7, rows)),
        ]
        + sems
        + sems,
        compiler_params=pltpu.CompilerParams(
            collective_id=0, has_side_effects=True, vmem_limit_bytes=56 * 1024 * 1024
        ),
        name="gather_forward",
    )(lengths, packed, hidden)
    return (outs[0].reshape(BLOCKS, D, W),) + tuple(outs[1:])


def backward_scatter_kernel(
    depth,
    len_ref,
    x_hbm,
    proj_hbm,
    dl_hbm,
    kc_hbm,
    wt_hbm,
    lse_hbm,
    gctx_hbm,
    gr1_hbm,
    full_hbm,
    depth_ref,
    kmt_ref,
    ctx_hbm,
    gmix_hbm,
    act_hbm,
    gffn_hbm,
    gpre_hbm,
    fb_hbm,
    stat_ref,
    gin_ref,
    o_ref,
    u_ref,
    x_ref,
    proj_ref,
    dl_ref,
    kc_ref,
    wt_ref,
    lse_ref,
    gctx_ref,
    gr1_ref,
    win_ref,
    wpt_ref,
    gproj_ref,
    gkc_ref,
    gkm,
    gdk,
    small,
    sv,
    gc,
    xs,
    gd,
    gs,
    gq,
    gt,
    dqt,
    left,
    right,
    part,
    rc,
    r1,
    r2,
    ru,
    rd,
    tiny,
    got,
    in_sem,
    left_sem,
    right_sem,
    cs,
    cr,
    s1,
    q1,
    s2,
    q2,
    us,
    ur,
    ds,
    dr,
    ts,
    tr,
):
    dp, z, x, core, y = place()
    c_dev, x_dev, y_dev = partners(dp, x, core, y)
    up_dev, down_dev = (dp + 4, y), (dp - 4, y)
    last = BLOCKS - 1
    rows = x_ref.shape[0]
    early = 5 * rows

    def fetch(t, act):
        def both(a, b):
            slot = t % 2
            for copy in (
                pltpu.make_async_copy(a, left.at[slot], left_sem.at[slot]),
                pltpu.make_async_copy(b, right.at[slot], right_sem.at[slot]),
            ):
                act(copy)

        @pl.when(t < 4)
        def _():
            both(act_hbm.at[t], gffn_hbm.at[t // 2])

        @pl.when((t >= 4) & (t < 8))
        def _():
            both(gpre_hbm.at[t - 4], fb_hbm.at[(t - 4) // 2])

        @pl.when((t >= 8) & (t < 10))
        def _():
            both(ctx_hbm, gmix_hbm.at[t - 8])

        @pl.when((t >= 10) & (t < 14))
        def _():
            both(x_hbm, gproj_ref.at[:, t - 10])

        @pl.when(t == 14)
        def _():
            both(dl_hbm, gkc_ref)

    def c_copy(t):
        return send(part.at[t, :, :, 1 - core], rc.at[t], cs.at[t], cr.at[t], c_dev)

    def first_copy(t, by_y):
        if by_y:
            return send(part.at[t, :, :, core, 1 - y], r1.at[t], s1.at[t], q1.at[t], y_dev)
        return send(part.at[t, :, 1 - x, core], r1.at[t], s1.at[t], q1.at[t], x_dev)

    def second_copy(t, by_y):
        if by_y:
            return send(part.at[t, :, 1 - x, core, y], r2.at[t], s2.at[t], q2.at[t], x_dev)
        return send(part.at[t, :, x, core, 1 - y], r2.at[t], s2.at[t], q2.at[t], y_dev)

    def up_copy(t, bottom):
        source = part.at[t, :, x, core, y] if bottom else ru.at[t]
        return send(source, ru.at[t], us.at[t], ur.at[t], up_dev)

    def down_copy(t, top):
        source = part.at[t, :, x, core, y] if top else rd.at[t]
        return send(source, rd.at[t], ds.at[t], dr.at[t], down_dev)

    def t_copy(k):
        return send(tiny.at[k], got.at[k], ts.at[k], tr.at[k], (c_dev, x_dev, y_dev)[k])

    def t_line(d, way):
        return send(
            tiny.at[3],
            got.at[3 + z],
            ts.at[2 + d if way > 0 else 1 + depth + d],
            tr.at[3 + z],
            (dp + 4 * d * way, y),
        )

    def t_arrival(level):
        return send(tiny.at[3], got.at[3 + level], ts.at[0], tr.at[3 + level], c_dev)

    def add(into, other):
        return (into.astype(F32) + other.astype(F32)).astype(BF16)

    def parity(t, work):
        @pl.when(t % 2 == 0)
        def _():
            work(True)

        @pl.when(t % 2 == 1)
        def _():
            work(False)


    def inside_of(r):
        return lax.broadcasted_iota(jnp.int32, (SEQ, 1), 0) < len_ref[r]

    def piece_span(r):
        sv[PAD : PAD + SEQ] = proj_ref[r, :, 3 * W :].astype(F32)
        gc[PAD : PAD + SEQ] = gctx_ref[r, :, W:].astype(F32)
        xs[PAD : PAD + SEQ] = x_ref[r].astype(F32)

        e16 = spread(16)
        place_row = lax.broadcasted_iota(jnp.int32, (W, 128), 0) // HD
        place_col = lax.broadcasted_iota(jnp.int32, (W, 128), 1)
        both = []
        for k in range(K):
            weight = pltpu.roll(wt_ref[r, k * 8 : k * 8 + 8], (k - K // 2) % SEQ, 1)
            high = weight.astype(BF16).astype(F32)
            both.append(jnp.concatenate([high, weight - high], axis=0).astype(BF16))
        for n in range(4):
            rows = slice(n * 128, (n + 1) * 128)
            spans = jnp.zeros((128, 128), F32)
            total = jnp.zeros((128, W), F32)
            for k in range(K):
                start = PAD + n * 128 + k - K // 2
                product_k = gc[PAD + n * 128 : PAD + (n + 1) * 128] * sv[start : start + 128]
                chosen = (place_col == place_row + 8 * k).astype(F32).astype(BF16)
                spans = spans + nn(product_k.astype(BF16), chosen)
                start = PAD + n * 128 - k + K // 2
                total = total + tn(both[k][:, rows], e16) * gc[start : start + 128]
            gt[:, rows] = spans.T
            gproj_ref[r, 3, rows] = total.astype(BF16)

    def piece_logits(r):
        center = jnp.zeros((8, SEQ), F32)
        for k in range(K):
            center = center + wt_ref[r, k * 8 : k * 8 + 8] * gt[k * 8 : k * 8 + 8]
        glt = jnp.concatenate(
            [
                wt_ref[r, k * 8 : k * 8 + 8] * (gt[k * 8 : k * 8 + 8] - center)
                for k in range(K)
            ],
            axis=0,
        ).astype(BF16)
        query = proj_ref[r, :, 0:W].astype(F32)
        mk = (kc_ref[r] * query).astype(BF16)
        gkm[...] += nn(glt, mk)
        mixed = tn(glt, kmt_ref[...])
        gkc_ref[r] = (mixed * query).astype(BF16)
        gq[...] = mixed * kc_ref[r]
        gd[PAD : PAD + SEQ] = nt(gkc_ref[r], wpt_ref[0])


    def piece_columns(r):
        def column(c, carry):
            lane = pl.ds(pl.multiple_of(c * 128, 128), 128)
            sums = [jnp.zeros((8, 128), F32)] * K
            for n in range(8):
                total = jnp.zeros((64, 128), F32)
                center = PAD + n * 64
                grad = gd[center : center + 64, lane]
                for k in range(K):
                    start = center + k - K // 2
                    sums[k] = sums[k] + jnp.sum(
                        (xs[start : start + 64, lane] * grad).reshape(8, 8, 128), axis=0
                    )
                    start = center - k + K // 2
                    total = total + gd[start : start + 64, lane] * depth_ref[k : k + 1, lane]
                gs[n * 64 : (n + 1) * 64, lane] = total
            for k in range(K):
                gdk[k, :, lane] = gdk[k, :, lane] + sums[k]
            return carry

        lax.fori_loop(0, D // 128, column, 0)


    def piece_pairs(r, first, stop):
        inside = inside_of(r)
        lane_head = lax.broadcasted_iota(jnp.int32, (1, 128), 1) // HD
        bias = jnp.where(inside, 0.0, -1e30).astype(F32)

        def pair(p, carry):
            def lanes(part):
                return pl.ds(pl.multiple_of(part * W + p * 128, 128), 128)

            q2, k2, v2 = (proj_ref[r, :, lanes(part)] for part in range(3))
            g2 = gctx_ref[r, :, lanes(0)]
            results = []
            for h in range(2):
                mine = lane_head == h
                scale = jnp.where(mine, 1.0 / math.sqrt(HD), 0.0).astype(BF16)
                scores = nt(k2, q2 * scale) + bias
                probs = jnp.exp(scores - lse_ref[r, pl.ds(p * 2 + h, 1)])
                grads = nt(v2 * jnp.where(mine, 1.0, 0.0).astype(BF16), g2)
                correction = jnp.sum(probs * grads, axis=0, keepdims=True)
                grad_scores = (probs * (grads - correction)).astype(BF16)
                dqt[h * HD : (h + 1) * HD] = tn(k2, grad_scores)[h * HD : (h + 1) * HD]
                results.append((nn(grad_scores, q2), nn(probs.astype(BF16), g2)))
            low = lane_head == 0
            scale = 1.0 / math.sqrt(HD)
            gproj_ref[r, 0, :, lanes(0)] = (dqt[...].T * scale + gq[:, lanes(0)]).astype(BF16)
            gproj_ref[r, 1, :, lanes(0)] = (jnp.where(low, results[0][0], results[1][0]) * scale).astype(BF16)
            gproj_ref[r, 2, :, lanes(0)] = jnp.where(low, results[0][1], results[1][1]).astype(BF16)
            return carry

        lax.fori_loop(first, stop, pair, 0)


    def piece_inputs(r):
        inside = inside_of(r)
        for b in range(4):
            gs[...] += nt(gproj_ref[r, b], win_ref[b])
        gin_ref[r] = jnp.where(inside, gr1_ref[r] + gs[...], 0.0).astype(BF16)


    def chosen(height, rule):
        row = lax.broadcasted_iota(jnp.int32, (height, 128), 0)
        lane = lax.broadcasted_iota(jnp.int32, (height, 128), 1)
        return rule(row, lane).astype(F32).astype(BF16)

    def gather_small():
        taps = jnp.concatenate(
            [jnp.sum(gdk[...], axis=1), jnp.zeros((16 - K, D), F32), jnp.sum(stat_ref[...], axis=1)]
        ).astype(BF16)
        pick = chosen(
            24,
            lambda row, lane: ((row < K) & (lane == row)) | ((row >= 20) & (lane == row - 20 + 4 * K)),
        )
        both = tn(taps, pick)
        low = gkm[...].astype(BF16)
        small[...] = both
        for odd in range(2):
            pick = chosen(
                8 * K,
                lambda row, lane: (row % 8 >= 3 * odd)
                & (row % 8 < 3 * odd + 3)
                & (lane == K + row // 8 * 3 + row % 8 - 3 * odd),
            )
            half = pl.ds(odd, W, stride=2)
            small[half] = small[half] + tn(low, pick)

    loads = (
        (x_hbm, x_ref),
        (proj_hbm, proj_ref),
        (dl_hbm, dl_ref),
        (kc_hbm, kc_ref),
        (wt_hbm, wt_ref),
        (lse_hbm, lse_ref),
        (gctx_hbm, gctx_ref),
        (gr1_hbm, gr1_ref),
        (full_hbm.at[pl.ds(10, 4)], win_ref),
        (full_hbm.at[pl.ds(14, 1)], wpt_ref),
    )
    inputs = [
        pltpu.make_async_copy(source, target, in_sem.at[i])
        for i, (source, target) in enumerate(loads)
    ]
    fetch(0, lambda copy: copy.start())
    for copy in inputs:
        copy.start()
    gkm[...] = jnp.zeros_like(gkm)
    gdk[...] = jnp.zeros_like(gdk)
    for ref, width in ((sv, W), (gc, W), (xs, D), (gd, D)):
        ref[0:PAD] = jnp.zeros((PAD, width), F32)
        ref[PAD + SEQ :] = jnp.zeros((PAD, width), F32)
    lines = tuple((z >= d, (dp - 4 * d, y)) for d in range(1, depth)) + tuple(
        (z + d < depth, (dp + 4 * d, y)) for d in range(1, depth)
    )
    meet((c_dev, x_dev, y_dev), lines)
    lane = lax.broadcasted_iota(jnp.int32, (8, 128), 1)
    mine = jnp.zeros((8, 128), F32)
    for k in range(4):
        mine = jnp.where(lane == k, jnp.sum(stat_ref[k]), mine)
    count = len_ref[0]
    for r in range(1, rows):
        count = count + len_ref[r]
    tiny[0] = jnp.where(lane == 4, count.astype(F32), mine)
    t_copy(0).start()

    def multiply(t):
        @pl.when(t == early)
        def _():
            fetch(t, lambda copy: copy.start())

        @pl.when((t + 1 < last) & (t + 1 != early))
        def _():
            fetch(t + 1, lambda copy: copy.start())

        @pl.when(t < last)
        def _():
            fetch(t, lambda copy: copy.wait())
            slot = t % 2
            for c in range(2):
                a = left[slot, :, :, c * W : (c + 1) * W].reshape(rows * SEQ, W)
                block = tn(a, right[slot].reshape(rows * SEQ, W))
                half = depth // 2
                part[t, c * half : (c + 1) * half] = block.reshape(
                    (half,) + part.shape[2:]
                ).astype(BF16)

        @pl.when(t == last)
        def _():
            gather_small()
            filled = jnp.concatenate([small[...], jnp.zeros((D, W - 128), F32)], axis=1)
            part[t] = filled.reshape(part.shape[1:]).astype(BF16)

        c_copy(t).start()

    def stage_core(t):
        c_copy(t).wait_recv()

        def level(j, carry):
            part[t, j, :, core] = add(part[t, j, :, core], rc[t, j])
            return carry

        lax.fori_loop(0, depth, level, 0)
        parity(t, lambda by_y: first_copy(t, by_y).start())

    def stage_first(t):
        def work(by_y):
            first_copy(t, by_y).wait_recv()
            if by_y:
                part[t, :, :, core, y] = add(part[t, :, :, core, y], r1[t])
            else:
                part[t, :, x, core] = add(part[t, :, x, core], r1[t])
            second_copy(t, by_y).start()

        parity(t, work)

    def stage_second(t):
        parity(t, lambda by_y: second_copy(t, by_y).wait_recv())
        part[t, :, x, core, y] = add(part[t, :, x, core, y], r2[t])
        o_ref[t] = part[t, z, x, core, y].astype(F32)

    def stage_up(t):
        @pl.when(z == 0)
        def _():
            up_copy(t, True).start()

        @pl.when(z > 0)
        def _():
            up_copy(t, False).wait_recv()
            o_ref[t] = o_ref[t] + ru[t, z].astype(F32)

        @pl.when((z > 0) & (z + 1 < depth))
        def _():
            ru[t] = add(ru[t], part[t, :, x, core, y])
            up_copy(t, False).start()

    def stage_down(t):
        @pl.when(z + 1 == depth)
        def _():
            down_copy(t, True).start()

        @pl.when(z + 1 < depth)
        def _():
            down_copy(t, False).wait_recv()
            o_ref[t] = o_ref[t] + rd[t, z].astype(F32)

        @pl.when((z > 0) & (z + 1 < depth))
        def _():
            rd[t] = add(rd[t], part[t, :, x, core, y])
            down_copy(t, False).start()

    def stage(t, work):
        @pl.when((t >= 0) & (t < BLOCKS))
        def _():
            work(t)

    def sums(t):
        for k in range(3):

            @pl.when(t == 3 * k + 3)
            def _():
                t_copy(k).wait_recv()
                tiny[k + 1] = tiny[k] + got[k]
                if k < 2:
                    t_copy(k + 1).start()

        @pl.when(t == 10)
        def _():
            for d in range(1, depth):

                @pl.when(z + d < depth)
                def _():
                    t_line(d, 1).start()

                @pl.when(z >= d)
                def _():
                    t_line(d, -1).start()

    def tick(t, carry):
        stage(t, multiply)
        stage(t - 1, stage_core)
        stage(t - 3, stage_first)
        stage(t - 5, stage_second)
        stage(t - 5 - z, stage_up)
        stage(t - 5 - (depth - 1 - z), stage_down)
        sums(t)
        row = t // 5

        def when(i, work):
            @pl.when((t < early) & (t % 5 == i))
            def _():
                work()

        @pl.when(t == 0)
        def _():
            for copy in inputs:
                copy.wait()

        when(0, lambda: piece_span(row))
        when(1, lambda: piece_logits(row))
        when(2, lambda: piece_columns(row))
        when(3, lambda: piece_pairs(row, 0, 2))

        def close():
            piece_pairs(row, 2, 3)
            piece_inputs(row)

        when(4, close)
        return carry

    lax.fori_loop(0, BLOCKS + 5 + depth, tick, 0)

    for level in range(depth):

        @pl.when(z == level)
        def _():
            got[3 + level] = tiny[3]

        @pl.when(z != level)
        def _():
            t_arrival(level).wait_recv()

    total = got[3]
    for level in range(1, depth):
        total = total + got[3 + level]
    u_ref[...] = total

    for d in range(1, depth):

        @pl.when(z + d < depth)
        def _():
            t_line(d, 1).wait_send()

        @pl.when(z >= d)
        def _():
            t_line(d, -1).wait_send()

    for k in range(3):
        t_copy(k).wait_send()

    def finish(t, carry):
        c_copy(t).wait_send()
        parity(t, lambda by_y: first_copy(t, by_y).wait_send())
        parity(t, lambda by_y: second_copy(t, by_y).wait_send())

        @pl.when(z + 1 < depth)
        def _():
            up_copy(t, False).wait_send()

        @pl.when(z > 0)
        def _():
            down_copy(t, False).wait_send()

        return carry

    lax.fori_loop(0, BLOCKS, finish, 0)


def backward_scatter(mesh, lengths, x, proj, dl, kc, wt, lse, gctx, gr1, full, depth_kernel, kmt, ctx, gmix, act, gffn, gpre, fb, stat):
    dp, fsdp = mesh.shape["dp"], mesh.shape["fsdp"]
    share = D // (dp * fsdp)
    depth = dp // 4
    rows = x.shape[0]
    dma = pltpu.SemaphoreType.DMA
    anywhere = pl.BlockSpec(memory_space=pl.ANY)
    inside = pl.BlockSpec(memory_space=pltpu.VMEM)

    def by_row(values):
        return values.reshape(values.shape[:-2] + (rows, SEQ, values.shape[-1]))

    return pl.pallas_call(
        functools.partial(backward_scatter_kernel, depth),
        out_shape=(
            jax.ShapeDtypeStruct((rows, SEQ, D), BF16),
            jax.ShapeDtypeStruct((BLOCKS, share, W), F32),
            jax.ShapeDtypeStruct((8, 128), F32),
        ),
        in_specs=[pl.BlockSpec(memory_space=pltpu.SMEM)]
        + [anywhere] * 9
        + [inside] * 2
        + [anywhere] * 6
        + [inside],
        out_specs=(inside, inside, inside),
        scratch_shapes=[
            pltpu.VMEM((rows, SEQ, D), BF16),
            pltpu.VMEM((rows, SEQ, 4 * W), BF16),
            pltpu.VMEM((rows, SEQ, D), BF16),
            pltpu.VMEM((rows, SEQ, W), F32),
            pltpu.VMEM((rows, 8 * K, SEQ), F32),
            pltpu.VMEM((rows, 8, SEQ), F32),
            pltpu.VMEM((rows, SEQ, D), BF16),
            pltpu.VMEM((rows, SEQ, D), F32),
            pltpu.VMEM((4, D, W), BF16),
            pltpu.VMEM((1, D, W), BF16),
            pltpu.VMEM((rows, 4, SEQ, W), BF16),
            pltpu.VMEM((rows, SEQ, W), BF16),
            pltpu.VMEM((8 * K, W), F32),
            pltpu.VMEM((K, 8, D), F32),
            pltpu.VMEM((D, 128), F32),
            pltpu.VMEM((SEQ + 2 * PAD, W), F32),
            pltpu.VMEM((SEQ + 2 * PAD, W), F32),
            pltpu.VMEM((SEQ + 2 * PAD, D), F32),
            pltpu.VMEM((SEQ + 2 * PAD, D), F32),
            pltpu.VMEM((SEQ, D), F32),
            pltpu.VMEM((SEQ, W), F32),
            pltpu.VMEM((128, SEQ), F32),
            pltpu.VMEM((128, SEQ), F32),
            pltpu.VMEM((2, rows, SEQ, D), BF16),
            pltpu.VMEM((2, rows, SEQ, W), BF16),
            pltpu.VMEM((BLOCKS, depth, 2, 2, 2, share, W), BF16),
            pltpu.VMEM((BLOCKS, depth, 2, 2, share, W), BF16),
            pltpu.VMEM((BLOCKS, depth, 2, share, W), BF16),
            pltpu.VMEM((BLOCKS, depth, share, W), BF16),
            pltpu.VMEM((BLOCKS, depth, share, W), BF16),
            pltpu.VMEM((BLOCKS, depth, share, W), BF16),
            pltpu.VMEM((4, 8, 128), F32),
            pltpu.VMEM((3 + depth, 8, 128), F32),
            dma((10,)),
            dma((2,)),
            dma((2,)),
        ]
        + [dma((BLOCKS,))] * 10
        + [dma((1 + 2 * depth,)), dma((3 + depth,))],
        compiler_params=pltpu.CompilerParams(
            collective_id=1, has_side_effects=True, vmem_limit_bytes=67_000_000
        ),
        name="backward_scatter",
    )(
        lengths,
        x,
        proj,
        dl,
        kc,
        wt,
        lse,
        gctx,
        gr1,
        full,
        depth_kernel,
        kmt,
        ctx,
        by_row(gmix),
        by_row(act),
        by_row(gffn),
        by_row(gpre),
        by_row(fb),
        stat,
    )


def body(
    mesh,
    hidden,
    lengths,
    in_weight,
    depth_kernel,
    point_weight,
    kernel_weight,
    out_weight,
    up_weight,
    down_weight,
    norm_gains,
    norm_biases,
    out_grad,
):
    packed = pack(
            in_weight,
            depth_kernel,
            point_weight,
            kernel_weight,
            out_weight,
            up_weight,
            down_weight,
            norm_gains,
            norm_biases,
    )
    output, input_grad, shard, totals = layer(mesh, hidden, lengths, packed, out_grad)
    rms = jnp.sqrt(totals[0, :4] / (totals[0, 4] * D))
    return (output, input_grad) + unpack(shard) + (rms,)


def solution(mesh):
    in_specs = (
        P(("dp", "fsdp"), None, None),
        P(("dp", "fsdp")),
        P(("dp", "fsdp"), None),
        P(None, ("dp", "fsdp")),
        P(("dp", "fsdp"), None),
        P(None, ("dp", "fsdp")),
        P(("dp", "fsdp"), None),
        P(None, None, ("dp", "fsdp")),
        P(None, ("dp", "fsdp"), None),
        P(None, ("dp", "fsdp")),
        P(None, ("dp", "fsdp")),
        P(("dp", "fsdp"), None, None),
    )
    out_specs = (
        P(("dp", "fsdp"), None, None),
        P(("dp", "fsdp"), None, None),
        P(("dp", "fsdp"), None),
        P(None, ("dp", "fsdp")),
        P(("dp", "fsdp"), None),
        P(None, ("dp", "fsdp")),
        P(("dp", "fsdp"), None),
        P(None, None, ("dp", "fsdp")),
        P(None, ("dp", "fsdp"), None),
        P(None, ("dp", "fsdp")),
        P(None, ("dp", "fsdp")),
        P(),
    )
    return jax.shard_map(functools.partial(body, mesh), mesh=mesh, in_specs=in_specs, out_specs=out_specs, check_vma=False)
```

```python
import functools
import math

import jax
import jax.numpy as jnp
from jax import lax
from jax.experimental import pallas as pl
from jax.experimental.pallas import tpu as pltpu
from jax.sharding import PartitionSpec as P

D = 768
HEADS = 6
HD = 64
G = 2
K = 9
SEQ = 512


EPSILON = 1e-06
MESH = pl.DeviceIdType.MESH
BLOCKS = 16
HALF = BLOCKS // 2


def place():
    dp, y = lax.axis_index("dp"), lax.axis_index("fsdp")
    return dp, dp // 4, (dp // 2) % 2, dp % 2, y


def partners(dp, x, core, y):
    return (dp + 1 - 2 * core, y), (dp + 2 - 4 * x, y), (dp, 1 - y)


def meet(peers, others):
    barrier = pltpu.get_barrier_semaphore()
    for peer in peers:
        pl.semaphore_signal(barrier, inc=1, device_id=peer, device_id_type=MESH)
    count = len(peers)
    for there, peer in others:

        @pl.when(there)
        def _():
            pl.semaphore_signal(barrier, inc=1, device_id=peer, device_id_type=MESH)

        count = count + there.astype(jnp.int32)
    pl.semaphore_wait(barrier, count)


def send(src, dst, send_sem, recv_sem, device):
    return pltpu.make_async_remote_copy(
        src_ref=src,
        dst_ref=dst,
        send_sem=send_sem,
        recv_sem=recv_sem,
        device_id=device,
        device_id_type=MESH,
    )


def gather_all(packed, mesh):
    if mesh is None:
        return packed
    full = lax.all_gather(packed, ("dp", "fsdp"), axis=1, tiled=False)
    return full.reshape(BLOCKS, D, packed.shape[2])


W = D // G
F32, BF16 = jnp.float32, jnp.bfloat16
PAD = 8


def nn(a, b):
    return lax.dot_general(a, b, (((1,), (0,)), ((), ())), preferred_element_type=F32)


def nt(a, b):
    return lax.dot_general(a, b, (((1,), (1,)), ((), ())), preferred_element_type=F32)


def tn(a, b):
    return lax.dot_general(a, b, (((0,), (0,)), ((), ())), preferred_element_type=F32)


def spread(rows):
    head = lax.broadcasted_iota(jnp.int32, (rows, W), 0) % 8
    channel = lax.broadcasted_iota(jnp.int32, (rows, W), 1) // HD
    return (head == channel).astype(F32).astype(BF16)


def forward_kernel(
    len_ref,
    hid_ref,
    wa_ref,
    wb_ref,
    wpt_ref,
    depth_ref,
    kmt_ref,
    x_ref,
    proj_ref,
    dl_ref,
    kc_ref,
    wt_ref,
    lse_ref,
    ctx_ref,
    xs,
    sv,
    ot,
):
    length = len_ref[pl.program_id(0)]
    inside = lax.broadcasted_iota(jnp.int32, (SEQ, 1), 0) < length
    x = jnp.where(inside, hid_ref[0], jnp.zeros((), BF16))
    x_ref[0] = x
    xs[0:PAD] = jnp.zeros((PAD, D), F32)
    xs[PAD + SEQ :] = jnp.zeros((PAD, D), F32)
    xs[PAD : PAD + SEQ] = x.astype(F32)
    sv[0:PAD] = jnp.zeros((PAD, W), F32)
    sv[PAD + SEQ :] = jnp.zeros((PAD, W), F32)

    for b in range(4):
        part = nn(x_ref[0], (wa_ref, wb_ref)[b // 2][b % 2]).astype(BF16)
        proj_ref[0, :, b * W : (b + 1) * W] = part
        if b == 3:
            sv[PAD : PAD + SEQ] = part.astype(F32)

    def column(c, carry):
        lane = pl.ds(pl.multiple_of(c * 128, 128), 128)
        for r in range(8):
            total = jnp.zeros((64, 128), F32)
            for k in range(K):
                start = PAD + r * 64 + k - K // 2
                total = total + xs[start : start + 64, lane] * depth_ref[k : k + 1, lane]
            dl_ref[0, r * 64 : (r + 1) * 64, lane] = total.astype(BF16)
        return carry

    lax.fori_loop(0, D // 128, column, 0)
    kc_ref[0] = nn(dl_ref[0], wpt_ref[0])
    mk = (kc_ref[0] * proj_ref[0, :, 0:W].astype(F32)).astype(BF16)
    logits = nt(kmt_ref[...], mk)
    top = logits[0:8]
    for k in range(1, K):
        top = jnp.maximum(top, logits[k * 8 : k * 8 + 8])
    parts = [jnp.exp(logits[k * 8 : k * 8 + 8] - top) for k in range(K)]
    inverse = 1.0 / sum(parts)
    both = []
    for k in range(K):
        weight = parts[k] * inverse
        wt_ref[0, k * 8 : k * 8 + 8] = weight
        high = weight.astype(BF16).astype(F32)
        both.append(jnp.concatenate([high, weight - high], axis=0).astype(BF16))
    e16 = spread(16)
    for r in range(4):
        total = jnp.zeros((128, W), F32)
        for k in range(K):
            start = PAD + r * 128 + k - K // 2
            total = total + tn(both[k][:, r * 128 : (r + 1) * 128], e16) * sv[start : start + 128]
        ctx_ref[0, r * 128 : (r + 1) * 128, W:] = total.astype(BF16)

    lane_head = lax.broadcasted_iota(jnp.int32, (1, 128), 1) // HD
    bias = jnp.where(inside, 0.0, -1e30).astype(F32)

    def pair(p, carry):
        def slab(part):
            return proj_ref[0, :, pl.ds(pl.multiple_of(part * W + p * 128, 128), 128)]

        q2, k2, v2 = slab(0), slab(1), slab(2)
        for h in range(2):
            scale = jnp.where(lane_head == h, 1.0 / math.sqrt(HD), 0.0).astype(BF16)
            scores = nt(k2, q2 * scale) + bias
            peak = jnp.max(scores, axis=0, keepdims=True)
            power = jnp.exp(scores - peak)
            total = jnp.sum(power, axis=0, keepdims=True)
            lse_ref[0, pl.ds(p * 2 + h, 1)] = peak + jnp.log(total)
            probs = (power * (1.0 / total)).astype(BF16)
            ot[h * HD : (h + 1) * HD] = tn(v2, probs)[h * HD : (h + 1) * HD]
        ctx_ref[0, :, pl.ds(pl.multiple_of(p * 128, 128), 128)] = ot[...].T.astype(BF16)
        return carry

    lax.fori_loop(0, HEADS // 2, pair, 0)


def forward(lengths, hidden, full, depth, kmt):
    rows = hidden.shape[0]

    def per_row(*shape):
        return pl.BlockSpec((1,) + shape, lambda r: (r, 0, 0))

    def out(dtype, *shape):
        return jax.ShapeDtypeStruct((rows,) + shape, dtype)

    return pl.pallas_call(
        forward_kernel,
        grid=(rows,),
        out_shape=(
            out(BF16, SEQ, D),
            out(BF16, SEQ, 4 * W),
            out(BF16, SEQ, D),
            out(F32, SEQ, W),
            out(F32, 8 * K, SEQ),
            out(F32, 8, SEQ),
            out(BF16, SEQ, D),
        ),
        in_specs=[
            pl.BlockSpec(memory_space=pltpu.SMEM),
            per_row(SEQ, D),
            pl.BlockSpec((2, D, W), lambda r: (5, 0, 0)),
            pl.BlockSpec((2, D, W), lambda r: (6, 0, 0)),
            pl.BlockSpec((1, D, W), lambda r: (14, 0, 0)),
            pl.BlockSpec((16, D), lambda r: (0, 0)),
            pl.BlockSpec((8 * K, W), lambda r: (0, 0)),
        ],
        out_specs=(
            per_row(SEQ, D),
            per_row(SEQ, 4 * W),
            per_row(SEQ, D),
            per_row(SEQ, W),
            per_row(8 * K, SEQ),
            per_row(8, SEQ),
            per_row(SEQ, D),
        ),
        scratch_shapes=[
            pltpu.VMEM((SEQ + 2 * PAD, D), F32),
            pltpu.VMEM((SEQ + 2 * PAD, W), F32),
            pltpu.VMEM((128, SEQ), F32),
        ],
        compiler_params=pltpu.CompilerParams(vmem_limit_bytes=56 * 1024 * 1024),
        name="mixer_forward",
    )(lengths, hidden, full, full, full, depth, kmt)


TILE = 256
CHUNK = 256
PART = 256


def ffn_kernel(
    len_ref,
    ctx_ref,
    x_ref,
    og_ref,
    wout_ref,
    wdn_ref,
    wup_ref,
    gb_ref,
    y_ref,
    act_ref,
    gpre_ref,
    fb_ref,
    gffn_ref,
    gmix_ref,
    gr1_ref,
    gctx_ref,
    stat_ref,
    mix,
    first,
    n1,
    inv,
    ffn,
    pre,
    dg,
    gr2,
):
    step = pl.program_id(0)
    row = step // (SEQ // TILE)
    base = (step % (SEQ // TILE)) * TILE
    left = len_ref[row] - base

    @pl.when(step == 0)
    def _():
        stat_ref[...] = jnp.zeros_like(stat_ref)

    for b in range(2):
        mix[:, b * W : (b + 1) * W] = nn(ctx_ref[...], wout_ref[b])

    def mask_of(i):
        return (lax.broadcasted_iota(jnp.int32, (CHUNK, 1), 0) + i * CHUNK < left).astype(F32)

    def fold(values):
        return jnp.sum(values.reshape(CHUNK // 8, 8, D), axis=0)

    def tally(k, values):
        stat_ref[k] = stat_ref[k] + fold(values)

    def rows_of(i):
        return pl.ds(pl.multiple_of(i * CHUNK, CHUNK), CHUNK)

    def norm(values):
        average = jnp.mean(values, axis=-1, keepdims=True)
        centered = values - average
        inverse = lax.rsqrt(jnp.mean(centered * centered, axis=-1, keepdims=True) + EPSILON)
        return centered * inverse, inverse

    def norm_back(grad, normed, inverse, gain):
        scaled = grad * gain
        mean = jnp.mean(scaled, axis=-1, keepdims=True)
        other = jnp.mean(scaled * normed, axis=-1, keepdims=True)
        return inverse * (scaled - mean - normed * other)

    def norm_one(i, carry):
        rows = rows_of(i)
        xf, mixed = x_ref[rows].astype(F32), mix[rows]
        normed, inverse = norm(xf + mixed)
        result = normed * gb_ref[0:1] + gb_ref[2:3]
        n1[rows] = normed
        inv[rows] = jnp.broadcast_to(inverse, (CHUNK, 128))
        first[rows] = result
        for g in range(G):
            fb_ref[g, rows] = result[:, g * W : (g + 1) * W].astype(BF16)
        tally(0, xf * xf)
        tally(1, mixed * mixed * mask_of(i))
        return carry

    lax.fori_loop(0, TILE // CHUNK, norm_one, 0)

    def part_of(c):
        return c // 3, pl.ds(c % 3 * PART, PART)

    def expand(c):
        s, units = part_of(c)
        pre[c % 2] = nt(fb_ref[s // 2], wup_ref[s, units])

    def gelu(c):
        s, units = part_of(c)
        for r in range(TILE // 32):
            rows = slice(r * 32, (r + 1) * 32)
            v = pre[c % 2, rows]
            phi = 0.5 + 0.5 * lax.erf(v * math.sqrt(0.5))
            act_ref[s, rows, units] = (v * phi).astype(BF16)
            dg[s, rows, units] = phi + v * jnp.exp(v * v * -0.5) * (1.0 / math.sqrt(2.0 * math.pi))

    def contract(s):
        g = s // 2
        part = nn(act_ref[s], wdn_ref[s])
        lanes = slice(g * W, (g + 1) * W)
        if s % 2 == 0:
            ffn[:, lanes] = part
        else:
            ffn[:, lanes] += part

    parts = 4 * D // PART
    expand(0)
    for c in range(parts):
        if c + 1 < parts:
            expand(c + 1)
        if c % 3 == 0 and c > 0:
            contract(c // 3 - 1)
        gelu(c)
    contract(3)

    def norm_two(i, carry):
        rows = rows_of(i)
        mask = mask_of(i)
        out = ffn[rows]
        normed, inverse = norm(first[rows] + out)
        y = (normed * gb_ref[1:2] + gb_ref[3:4]) * mask
        y_ref[rows] = y.astype(BF16)
        grad = og_ref[rows].astype(F32) * mask
        back = norm_back(grad, normed, inverse, gb_ref[1:2])
        gr2[rows] = back
        for g in range(G):
            gffn_ref[g, rows] = back[:, g * W : (g + 1) * W].astype(BF16)
        tally(2, out * out * mask)
        tally(3, y * y)
        tally(5, grad * normed)
        tally(7, grad)
        return carry

    lax.fori_loop(0, TILE // CHUNK, norm_two, 0)

    for c in range(parts):
        s, units = part_of(c)
        gpre_ref[s, :, units] = (nt(gffn_ref[s // 2], wdn_ref[s, units]) * dg[s, :, units]).astype(BF16)
        if c % 3 == 2:
            lanes = slice(s // 2 * W, (s // 2 + 1) * W)
            gr2[:, lanes] += nn(gpre_ref[s], wup_ref[s])

    def norm_one_back(i, carry):
        rows = rows_of(i)
        grad, normed = gr2[rows], n1[rows]
        back = norm_back(grad, normed, inv[rows, 0:1], gb_ref[0:1])
        gr1_ref[rows] = back
        for g in range(2):
            gmix_ref[g, rows] = back[:, g * W : (g + 1) * W].astype(BF16)
        tally(4, grad * normed)
        tally(6, grad)
        return carry

    lax.fori_loop(0, TILE // CHUNK, norm_one_back, 0)
    gctx_ref[...] = (
        nt(gmix_ref[0], wout_ref[0]) + nt(gmix_ref[1], wout_ref[1])
    ).astype(BF16)


def feed_forward(lengths, ctx, x, out_grad, full, gb):
    tokens = x.shape[0]

    def per_tile(width):
        return pl.BlockSpec((TILE, width), lambda i: (i, 0))

    def out(dtype, width):
        return jax.ShapeDtypeStruct((tokens, width), dtype)

    def slabs(count, width):
        return pl.BlockSpec((count, TILE, width), lambda i: (0, i, 0))

    def slabs_out(count, width):
        return jax.ShapeDtypeStruct((count, tokens, width), BF16)

    return pl.pallas_call(
        ffn_kernel,
        grid=(tokens // TILE,),
        out_shape=(
            out(BF16, D),
            slabs_out(4, D),
            slabs_out(4, D),
            slabs_out(G, W),
            slabs_out(G, W),
            slabs_out(2, W),
            out(F32, D),
            out(BF16, D),
            jax.ShapeDtypeStruct((8, 8, D), F32),
        ),
        in_specs=[
            pl.BlockSpec(memory_space=pltpu.SMEM),
            per_tile(D),
            per_tile(D),
            per_tile(D),
            pl.BlockSpec((2, D, W), lambda i: (4, 0, 0)),
            pl.BlockSpec((4, D, W), lambda i: (0, 0, 0)),
            pl.BlockSpec((4, D, W), lambda i: (1, 0, 0)),
            pl.BlockSpec((8, D), lambda i: (0, 0)),
        ],
        out_specs=(
            per_tile(D),
            slabs(4, D),
            slabs(4, D),
            slabs(G, W),
            slabs(G, W),
            slabs(2, W),
            per_tile(D),
            per_tile(D),
            pl.BlockSpec((8, 8, D), lambda i: (0, 0, 0)),
        ),
        scratch_shapes=[
            pltpu.VMEM((TILE, D), F32),
            pltpu.VMEM((TILE, D), F32),
            pltpu.VMEM((TILE, D), F32),
            pltpu.VMEM((TILE, 128), F32),
            pltpu.VMEM((TILE, D), F32),
            pltpu.VMEM((2, TILE, PART), F32),
            pltpu.VMEM((4, TILE, D), F32),
            pltpu.VMEM((TILE, D), F32),
        ],
        compiler_params=pltpu.CompilerParams(vmem_limit_bytes=56 * 1024 * 1024),
        name="feed_forward",
    )(lengths, ctx, x, out_grad, full, full, full, gb)


def backward_kernel(
    len_ref,
    x_ref,
    proj_ref,
    dl_ref,
    kc_ref,
    wt_ref,
    lse_ref,
    gctx_ref,
    gr1_ref,
    wa_ref,
    wb_ref,
    wpt_ref,
    depth_ref,
    kmt_ref,
    gproj_ref,
    gkc_ref,
    gin_ref,
    gkm_ref,
    gdk_ref,
    sv,
    gc,
    xs,
    gd,
    gs,
    gq,
    gt,
    dqt,
):
    row = pl.program_id(0)
    length = len_ref[row]
    inside = lax.broadcasted_iota(jnp.int32, (SEQ, 1), 0) < length

    @pl.when(row == 0)
    def _():
        gkm_ref[...] = jnp.zeros_like(gkm_ref)
        gdk_ref[...] = jnp.zeros_like(gdk_ref)

    for ref, width in ((sv, W), (gc, W), (xs, D), (gd, D)):
        ref[0:PAD] = jnp.zeros((PAD, width), F32)
        ref[PAD + SEQ :] = jnp.zeros((PAD, width), F32)
    sv[PAD : PAD + SEQ] = proj_ref[0, :, 3 * W :].astype(F32)
    gc[PAD : PAD + SEQ] = gctx_ref[0, :, W:].astype(F32)
    xs[PAD : PAD + SEQ] = x_ref[0].astype(F32)

    e16 = spread(16)
    place_row = lax.broadcasted_iota(jnp.int32, (W, 128), 0) // HD
    place_col = lax.broadcasted_iota(jnp.int32, (W, 128), 1)
    both = []
    for k in range(K):
        weight = pltpu.roll(wt_ref[0, k * 8 : k * 8 + 8], (k - K // 2) % SEQ, 1)
        high = weight.astype(BF16).astype(F32)
        both.append(jnp.concatenate([high, weight - high], axis=0).astype(BF16))
    for r in range(4):
        rows = slice(r * 128, (r + 1) * 128)
        spans = jnp.zeros((128, 128), F32)
        total = jnp.zeros((128, W), F32)
        for k in range(K):
            start = PAD + r * 128 + k - K // 2
            product_k = gc[PAD + r * 128 : PAD + (r + 1) * 128] * sv[start : start + 128]
            chosen = (place_col == place_row + 8 * k).astype(F32).astype(BF16)
            spans = spans + nn(product_k.astype(BF16), chosen)
            start = PAD + r * 128 - k + K // 2
            total = total + tn(both[k][:, rows], e16) * gc[start : start + 128]
        gt[:, rows] = spans.T
        gproj_ref[3, rows] = total.astype(BF16)
    center = jnp.zeros((8, SEQ), F32)
    for k in range(K):
        center = center + wt_ref[0, k * 8 : k * 8 + 8] * gt[k * 8 : k * 8 + 8]
    glt = jnp.concatenate(
        [
            wt_ref[0, k * 8 : k * 8 + 8] * (gt[k * 8 : k * 8 + 8] - center)
            for k in range(K)
        ],
        axis=0,
    ).astype(BF16)
    query = proj_ref[0, :, 0:W].astype(F32)
    mk = (kc_ref[0] * query).astype(BF16)
    gkm_ref[...] += nn(glt, mk)
    mixed = tn(glt, kmt_ref[...])
    gkc_ref[0] = (mixed * query).astype(BF16)
    gq[...] = mixed * kc_ref[0]
    gd[PAD : PAD + SEQ] = nt(gkc_ref[0], wpt_ref[0])

    def column(c, carry):
        lane = pl.ds(pl.multiple_of(c * 128, 128), 128)
        sums = [jnp.zeros((8, 128), F32)] * K
        for r in range(8):
            total = jnp.zeros((64, 128), F32)
            center = PAD + r * 64
            grad = gd[center : center + 64, lane]
            for k in range(K):
                start = center + k - K // 2
                sums[k] = sums[k] + jnp.sum(
                    (xs[start : start + 64, lane] * grad).reshape(8, 8, 128), axis=0
                )
                start = center - k + K // 2
                total = total + gd[start : start + 64, lane] * depth_ref[k : k + 1, lane]
            gs[r * 64 : (r + 1) * 64, lane] = total
        for k in range(K):
            gdk_ref[k, :, lane] = gdk_ref[k, :, lane] + sums[k]
        return carry

    lax.fori_loop(0, D // 128, column, 0)

    lane_head = lax.broadcasted_iota(jnp.int32, (1, 128), 1) // HD
    bias = jnp.where(inside, 0.0, -1e30).astype(F32)

    def pair(p, carry):
        def lanes(part):
            return pl.ds(pl.multiple_of(part * W + p * 128, 128), 128)

        q2, k2, v2 = (proj_ref[0, :, lanes(part)] for part in range(3))
        g2 = gctx_ref[0, :, lanes(0)]
        results = []
        for h in range(2):
            mine = lane_head == h
            scale = jnp.where(mine, 1.0 / math.sqrt(HD), 0.0).astype(BF16)
            scores = nt(k2, q2 * scale) + bias
            probs = jnp.exp(scores - lse_ref[0, pl.ds(p * 2 + h, 1)])
            grads = nt(v2 * jnp.where(mine, 1.0, 0.0).astype(BF16), g2)
            correction = jnp.sum(probs * grads, axis=0, keepdims=True)
            grad_scores = (probs * (grads - correction)).astype(BF16)
            dqt[h * HD : (h + 1) * HD] = tn(k2, grad_scores)[h * HD : (h + 1) * HD]
            results.append((nn(grad_scores, q2), nn(probs.astype(BF16), g2)))
        low = lane_head == 0
        scale = 1.0 / math.sqrt(HD)
        gproj_ref[0, :, lanes(0)] = (dqt[...].T * scale + gq[:, lanes(0)]).astype(BF16)
        gproj_ref[1, :, lanes(0)] = (jnp.where(low, results[0][0], results[1][0]) * scale).astype(BF16)
        gproj_ref[2, :, lanes(0)] = jnp.where(low, results[0][1], results[1][1]).astype(BF16)
        return carry

    lax.fori_loop(0, HEADS // 2, pair, 0)

    for b in range(4):
        gs[...] += nt(gproj_ref[b], (wa_ref, wb_ref)[b // 2][b % 2])
    gin_ref[0] = jnp.where(inside, gr1_ref[0] + gs[...], 0.0).astype(BF16)


def backward(lengths, x, proj, dl, kc, wt, lse, gctx, gr1, full, depth, kmt):
    rows = x.shape[0]

    def per_row(*shape):
        return pl.BlockSpec((1,) + shape, lambda r: (r, 0, 0))

    def out(dtype, *shape):
        return jax.ShapeDtypeStruct((rows,) + shape, dtype)

    return pl.pallas_call(
        backward_kernel,
        grid=(rows,),
        out_shape=(
            jax.ShapeDtypeStruct((4, rows * SEQ, W), BF16),
            out(BF16, SEQ, W),
            out(BF16, SEQ, D),
            jax.ShapeDtypeStruct((8 * K, W), F32),
            jax.ShapeDtypeStruct((K, 8, D), F32),
        ),
        in_specs=[
            pl.BlockSpec(memory_space=pltpu.SMEM),
            per_row(SEQ, D),
            per_row(SEQ, 4 * W),
            per_row(SEQ, D),
            per_row(SEQ, W),
            per_row(8 * K, SEQ),
            per_row(8, SEQ),
            per_row(SEQ, D),
            per_row(SEQ, D),
            pl.BlockSpec((2, D, W), lambda r: (5, 0, 0)),
            pl.BlockSpec((2, D, W), lambda r: (6, 0, 0)),
            pl.BlockSpec((1, D, W), lambda r: (14, 0, 0)),
            pl.BlockSpec((16, D), lambda r: (0, 0)),
            pl.BlockSpec((8 * K, W), lambda r: (0, 0)),
        ],
        out_specs=(
            pl.BlockSpec((4, SEQ, W), lambda r: (0, r, 0)),
            per_row(SEQ, W),
            per_row(SEQ, D),
            pl.BlockSpec((8 * K, W), lambda r: (0, 0)),
            pl.BlockSpec((K, 8, D), lambda r: (0, 0, 0)),
        ),
        scratch_shapes=[
            pltpu.VMEM((SEQ + 2 * PAD, W), F32),
            pltpu.VMEM((SEQ + 2 * PAD, W), F32),
            pltpu.VMEM((SEQ + 2 * PAD, D), F32),
            pltpu.VMEM((SEQ + 2 * PAD, D), F32),
            pltpu.VMEM((SEQ, D), F32),
            pltpu.VMEM((SEQ, W), F32),
            pltpu.VMEM((128, SEQ), F32),
            pltpu.VMEM((128, SEQ), F32),
        ],
        compiler_params=pltpu.CompilerParams(vmem_limit_bytes=56 * 1024 * 1024),
        name="mixer_backward",
    )(lengths, x, proj, dl, kc, wt, lse, gctx, gr1, full, full, full, depth, kmt)


def pack(in_weight, depth_kernel, point_weight, kernel_weight, out_weight, up_weight, down_weight, norm_gains, norm_biases):
    rows = in_weight.shape[0]

    def halves(grouped):
        return grouped.reshape(G * 2, rows, W)

    kernel = kernel_weight.reshape(K, rows, 3).transpose(1, 0, 2).reshape(rows, 3 * K)
    small = jnp.concatenate([depth_kernel.T, kernel, norm_gains.T, norm_biases.T], axis=1)
    small = jnp.pad(small, ((0, 0), (0, W - small.shape[1])))
    return jnp.concatenate(
        [
            halves(down_weight),
            halves(up_weight.transpose(0, 2, 1)),
            out_weight.reshape(rows, 2, W).transpose(1, 0, 2),
            in_weight.reshape(rows, 4, W).transpose(1, 0, 2),
            point_weight[None],
            small[None],
        ],
        axis=0,
    )


def unpack(shard):
    rows = shard.shape[1]
    small = shard[15]
    kernel = small[:, K : 4 * K].reshape(rows, K, 3).transpose(1, 0, 2).reshape(K, 3 * rows)
    return (
        shard[10:14].transpose(1, 0, 2).reshape(rows, 4 * W),
        small[:, :K].T,
        shard[14],
        kernel,
        shard[8:10].transpose(1, 0, 2).reshape(rows, 2 * W),
        shard[4:8].reshape(G, 2 * rows, W).transpose(0, 2, 1),
        shard[0:4].reshape(G, 2 * rows, W),
        small[:, 4 * K : 4 * K + 2].T,
        small[:, 4 * K + 2 : 4 * K + 4].T,
    )


def constants(full):
    small = full[15].astype(F32)
    depth = jnp.pad(small[:, :K].T, ((0, 16 - K), (0, 0)))
    kernel = small[:, K : 4 * K].reshape(D, K, 3).transpose(1, 0, 2).reshape(K, W, HEADS)
    kmt = jnp.pad(kernel.transpose(0, 2, 1), ((0, 0), (0, 8 - HEADS), (0, 0)))
    kmt = kmt.reshape(8 * K, W).astype(BF16)
    gb = jnp.pad(small[:, 4 * K : 4 * K + 4].T, ((0, 4), (0, 0)))
    return depth, kmt, gb


def layer(mesh, hidden, lengths, packed, out_grad):
    rows = hidden.shape[0]
    tokens = rows * SEQ
    if fused(mesh, rows):
        full, depth, kmt, gb, x, proj, dl, kc, wt, lse, ctx = gather_forward(
            mesh, lengths, packed, hidden
        )
    else:
        full = gather_all(packed, mesh)
        depth, kmt, gb = constants(full)
        x, proj, dl, kc, wt, lse, ctx = forward(lengths, hidden, full, depth, kmt)
    flat_x, flat_ctx = x.reshape(tokens, D), ctx.reshape(tokens, D)
    y, act, gpre, fb, gffn, gmix, gr1, gctx, stat = feed_forward(
        lengths, flat_ctx, flat_x, out_grad.reshape(tokens, D), full, gb
    )
    gctx, gr1 = gctx.reshape(rows, SEQ, D), gr1.reshape(rows, SEQ, D)
    if fused(mesh, rows):
        gin, shard, totals = backward_scatter(
            mesh, lengths, x, proj, dl, kc, wt, lse, gctx, gr1, full, depth, kmt, ctx, gmix, act, gffn, gpre, fb, stat
        )
        return y.reshape(rows, SEQ, D), gin, shard, totals
    gproj, gkc, gin, gkm, gdk = backward(
        lengths, x, proj, dl, kc, wt, lse, gctx, gr1, full, depth, kmt
    )
    stat = jnp.sum(stat, axis=1)
    grad_kernel = gkm.reshape(K, 8, W)[:, :HEADS].transpose(0, 2, 1).reshape(K, D, 3)
    small = jnp.concatenate(
        [
            jnp.sum(gdk, axis=1).T,
            grad_kernel.transpose(1, 0, 2).reshape(D, 3 * K),
            stat[4:8].T,
        ],
        axis=1,
    )
    small = jnp.pad(small, ((0, 0), (0, W - small.shape[1]))).astype(BF16)
    local = weight_grads(
        flat_x, dl.reshape(tokens, D), gproj, gkc.reshape(tokens, W), flat_ctx, gmix, act, gffn, gpre, fb, small
    )
    sums = jnp.concatenate([jnp.sum(stat[0:4], axis=1), jnp.sum(lengths).astype(F32)[None]])
    if mesh is None:
        return y.reshape(rows, SEQ, D), gin, local.astype(F32), sums[None]
    devices = mesh.shape["dp"] * mesh.shape["fsdp"]
    shard = lax.psum_scatter(
        local.reshape(BLOCKS, devices, D // devices, W),
        ("dp", "fsdp"),
        scatter_dimension=1,
        tiled=False,
    )
    return (
        y.reshape(rows, SEQ, D),
        gin,
        shard.astype(F32),
        lax.psum(sums, ("dp", "fsdp"))[None],
    )


def fused(mesh, rows):
    return mesh is not None and mesh.shape["fsdp"] == 2 and mesh.shape["dp"] % 4 == 0 and rows == 2


def weight_grads(x, dl, gproj, gkc, ctx, gmix, act, gffn, gpre, fb, small):
    pairs = [(act[s], gffn[s // 2]) for s in range(4)]
    pairs += [(gpre[s], fb[s // 2]) for s in range(4)]
    pairs += [(ctx, gmix[b]) for b in range(2)]
    pairs += [(x, gproj[b]) for b in range(4)]
    pairs += [(dl, gkc)]
    return jnp.stack([tn(a, b).astype(BF16) for a, b in pairs] + [small])


def picked(height, rule):
    row = lax.broadcasted_iota(jnp.int32, (height, 128), 0)
    lane = lax.broadcasted_iota(jnp.int32, (height, 128), 1)
    return rule(row, lane).astype(F32).astype(BF16)


def gather_engine(depth, g_ref, low, high, sems):
    dp, z, x, core, y = place()
    c_dev, x_dev, y_dev = partners(dp, x, core, y)
    up_dev, down_dev = (dp + 4, y), (dp - 4, y)
    steps = 2 * depth - 1
    size = (high - low) // 2
    every, halves = pl.ds(low, 2 * size), (pl.ds(low, size), pl.ds(low + size, size))

    def target(q):
        return z + ((q + 1) // 2) * (1 - 2 * (q % 2))

    def z_copy(j, way, device):
        slab = g_ref.at[every, j, x, core, y]
        return send(slab, slab, sems[0].at[way, j], sems[1].at[j], device)

    def x_copy(j):
        slab = g_ref.at[every, j, x, core, y]
        return send(slab, slab, sems[2].at[j], sems[3].at[j], x_dev)

    def y_copy(j):
        slab = g_ref.at[every, j, x, core, y]
        return send(slab, slab, sems[4].at[j], sems[5].at[j], y_dev)

    def d_copy(j, half):
        if half == 0:
            slab = g_ref.at[halves[0], j, 1 - x, core, y]
            return send(slab, slab, sems[6].at[0, j], sems[7].at[0, j], y_dev)
        slab = g_ref.at[halves[1], j, x, core, 1 - y]
        return send(slab, slab, sems[6].at[1, j], sems[7].at[1, j], x_dev)

    def c_copy(j, a, b):
        slab = g_ref.at[every, j, (x + a) % 2, core, (y + b) % 2]
        return send(slab, slab, sems[8].at[2 * a + b, j], sems[9].at[2 * a + b, j], c_dev)

    def c_arrival(j, a, b):
        slab = g_ref.at[every, j, (x + a) % 2, 1 - core, (y + b) % 2]
        return send(slab, slab, sems[8].at[2 * a + b, j], sems[9].at[2 * a + b, j], c_dev)

    def x_arrival(j):
        slab = g_ref.at[every, j, 1 - x, core, y]
        return send(slab, slab, sems[2].at[j], sems[3].at[j], x_dev)

    def y_arrival(j):
        slab = g_ref.at[every, j, x, core, 1 - y]
        return send(slab, slab, sems[4].at[j], sems[5].at[j], y_dev)

    def d_arrival(j, half):
        slab = g_ref.at[halves[half], j, 1 - x, core, 1 - y]
        return send(slab, slab, sems[6].at[half, j], sems[7].at[half, j], y_dev if half == 0 else x_dev)

    def first(j):
        @pl.when(j != z)
        def _():
            z_copy(j, 0, up_dev).wait_recv()

        @pl.when((j <= z) & (z + 1 < depth))
        def _():
            z_copy(j, 0, up_dev).start()

        @pl.when((j >= z) & (z > 0))
        def _():
            z_copy(j, 1, down_dev).start()

        x_copy(j).start()
        y_copy(j).start()
        c_copy(j, 0, 0).start()

    def second(j):
        x_arrival(j).wait_recv()
        d_copy(j, 0).start()
        c_copy(j, 1, 0).start()
        y_arrival(j).wait_recv()
        d_copy(j, 1).start()
        c_copy(j, 0, 1).start()

    def third(j):
        d_arrival(j, 0).wait_recv()
        d_arrival(j, 1).wait_recv()
        c_copy(j, 1, 1).start()

    def stage(q, work):
        j = target(q)

        @pl.when((q >= 0) & (q < steps) & (j >= 0) & (j < depth))
        def _():
            work(j)

    def arrive(j, carry):
        for a in range(2):
            for b in range(2):
                c_arrival(j, a, b).wait_recv()
        return carry

    def step(q, carry):
        stage(q, first)
        stage(q - 1, second)
        stage(q - 2, third)
        return carry

    def finish(j, carry):
        for a in range(2):
            for b in range(2):
                c_copy(j, a, b).wait_send()
        x_copy(j).wait_send()
        y_copy(j).wait_send()
        d_copy(j, 0).wait_send()
        d_copy(j, 1).wait_send()

        @pl.when((j <= z) & (z + 1 < depth))
        def _():
            z_copy(j, 0, up_dev).wait_send()

        @pl.when((j >= z) & (z > 0))
        def _():
            z_copy(j, 1, down_dev).wait_send()

        return carry

    return step, arrive, finish


def gather_forward_kernel(
    depth,
    len_ref,
    p_ref,
    hid_hbm,
    g_ref,
    taps_ref,
    kmt_ref,
    gb_ref,
    x_out,
    proj_out,
    dl_out,
    kc_out,
    wt_out,
    lse_out,
    ctx_out,
    hid_ref,
    x_ref,
    proj_ref,
    dl_ref,
    kc_ref,
    wt_ref,
    lse_ref,
    ctx_ref,
    win_ref,
    wpt_ref,
    small_ref,
    small,
    xs,
    sv,
    ot,
    own_sem,
    in_sem,
    out_sem,
    *sems,
):
    dp, z, x, core, y = place()
    rows = hid_ref.shape[0]
    depth_ref = taps_ref
    load = pltpu.make_async_copy(hid_hbm, hid_ref, in_sem.at[0])
    load.start()
    own = pltpu.make_async_copy(p_ref, g_ref.at[:, z, x, core, y], own_sem)
    own.start()
    xs[0:PAD] = jnp.zeros((PAD, D), F32)
    xs[PAD + SEQ :] = jnp.zeros((PAD, D), F32)
    sv[0:PAD] = jnp.zeros((PAD, W), F32)
    sv[PAD + SEQ :] = jnp.zeros((PAD, W), F32)
    meet(
        partners(dp, x, core, y),
        ((z + 1 < depth, (dp + 4, y)), (z > 0, (dp - 4, y))),
    )
    own.wait()
    count = len(sems) // 2
    soon = gather_engine(depth, g_ref, 10, 16, sems[:count])
    later = gather_engine(depth, g_ref, 0, 10, sems[count:])
    lax.fori_loop(0, 2 * depth - 1, soon[0], 0)
    later[0](0, 0)
    lax.fori_loop(2 * depth - 1, 2 * depth + 1, soon[0], 0)
    lax.fori_loop(0, depth, soon[1], 0)
    inputs = [
        pltpu.make_async_copy(g_ref.at[pl.ds(first, size)], target, in_sem.at[1 + i])
        for i, (first, size, target) in enumerate(
            ((15, 1, small_ref), (10, 4, win_ref), (14, 1, wpt_ref))
        )
    ]
    for copy in inputs:
        copy.start()
    load.wait()
    inputs[0].wait()
    values = small_ref[...].reshape(D, W)[:, 0:128]
    small[...] = values.astype(F32)
    taps_ref[...] = nt(picked(16, lambda row, lane: (row < K) & (lane == row)), values)
    gb_ref[...] = nt(picked(8, lambda row, lane: (row < 4) & (lane == row + 4 * K)), values)
    kernel = jnp.zeros((8 * K, W), F32)
    for odd in range(2):
        pick = picked(
            8 * K,
            lambda row, lane: (row % 8 >= 3 * odd)
            & (row % 8 < 3 * odd + 3)
            & (lane == K + row // 8 * 3 + row % 8 - 3 * odd),
        )
        kernel = kernel + nt(pick, small[pl.ds(odd, W, stride=2)].astype(BF16))
    kmt_ref[...] = kernel.astype(BF16)
    for copy in inputs[1:]:
        copy.wait()

    def inside_of(r):
        return lax.broadcasted_iota(jnp.int32, (SEQ, 1), 0) < len_ref[r]

    def piece_project(r):
        inside = inside_of(r)
        x = jnp.where(inside, hid_ref[r], jnp.zeros((), BF16))
        x_ref[r] = x
        xs[PAD : PAD + SEQ] = x.astype(F32)

        for b in range(4):
            part = nn(x_ref[r], win_ref[b].reshape(D, W)).astype(BF16)
            proj_ref[r, :, b * W : (b + 1) * W] = part
            if b == 3:
                sv[PAD : PAD + SEQ] = part.astype(F32)

    def piece_columns(r):
        def column(c, carry):
            lane = pl.ds(pl.multiple_of(c * 128, 128), 128)
            for n in range(8):
                total = jnp.zeros((64, 128), F32)
                for k in range(K):
                    start = PAD + n * 64 + k - K // 2
                    total = total + xs[start : start + 64, lane] * depth_ref[k : k + 1, lane]
                dl_ref[r, n * 64 : (n + 1) * 64, lane] = total.astype(BF16)
            return carry

        lax.fori_loop(0, D // 128, column, 0)

    def piece_span(r):
        kc_ref[r] = nn(dl_ref[r], wpt_ref[0].reshape(D, W))
        mk = (kc_ref[r] * proj_ref[r, :, 0:W].astype(F32)).astype(BF16)
        logits = nt(kmt_ref[...], mk)
        top = logits[0:8]
        for k in range(1, K):
            top = jnp.maximum(top, logits[k * 8 : k * 8 + 8])
        parts = [jnp.exp(logits[k * 8 : k * 8 + 8] - top) for k in range(K)]
        inverse = 1.0 / sum(parts)
        both = []
        for k in range(K):
            weight = parts[k] * inverse
            wt_ref[r, k * 8 : k * 8 + 8] = weight
            high = weight.astype(BF16).astype(F32)
            both.append(jnp.concatenate([high, weight - high], axis=0).astype(BF16))
        e16 = spread(16)
        for n in range(4):
            total = jnp.zeros((128, W), F32)
            for k in range(K):
                start = PAD + n * 128 + k - K // 2
                total = total + tn(both[k][:, n * 128 : (n + 1) * 128], e16) * sv[start : start + 128]
            ctx_ref[r, n * 128 : (n + 1) * 128, W:] = total.astype(BF16)

    def piece_pairs(r, first, stop):
        inside = inside_of(r)
        lane_head = lax.broadcasted_iota(jnp.int32, (1, 128), 1) // HD
        bias = jnp.where(inside, 0.0, -1e30).astype(F32)

        def pair(p, carry):
            def slab(part):
                return proj_ref[r, :, pl.ds(pl.multiple_of(part * W + p * 128, 128), 128)]

            q2, k2, v2 = slab(0), slab(1), slab(2)
            for h in range(2):
                scale = jnp.where(lane_head == h, 1.0 / math.sqrt(HD), 0.0).astype(BF16)
                scores = nt(k2, q2 * scale) + bias
                peak = jnp.max(scores, axis=0, keepdims=True)
                power = jnp.exp(scores - peak)
                total = jnp.sum(power, axis=0, keepdims=True)
                lse_ref[r, pl.ds(p * 2 + h, 1)] = peak + jnp.log(total)
                probs = (power * (1.0 / total)).astype(BF16)
                ot[h * HD : (h + 1) * HD] = tn(v2, probs)[h * HD : (h + 1) * HD]
            ctx_ref[r, :, pl.ds(pl.multiple_of(p * 128, 128), 128)] = ot[...].T.astype(BF16)
            return carry

        lax.fori_loop(first, stop, pair, 0)


    pairs = (
        (x_ref, x_out),
        (proj_ref, proj_out),
        (dl_ref, dl_out),
        (kc_ref, kc_out),
        (wt_ref, wt_out),
        (lse_ref, lse_out),
        (ctx_ref, ctx_out),
    )

    def store(r):
        return [
            pltpu.make_async_copy(source.at[r], target.at[r], out_sem.at[i, r])
            for i, (source, target) in enumerate(pairs)
        ]

    def tick(t, carry):
        row = t // 5

        def when(i, work):
            @pl.when(t % 5 == i)
            def _():
                work()

        when(0, lambda: piece_project(row))
        when(1, lambda: piece_columns(row))
        when(2, lambda: piece_span(row))
        when(3, lambda: piece_pairs(row, 0, 2))

        def close():
            piece_pairs(row, 2, 3)
            for copy in store(row):
                copy.start()

        when(4, close)

        @pl.when(t < 2 * depth)
        def _():
            later[0](t + 1, 0)

        return carry

    lax.fori_loop(0, 5 * rows, tick, 0)
    for t in range(5 * rows, 2 * depth):
        later[0](jnp.int32(t + 1), 0)
    lax.fori_loop(0, depth, later[1], 0)
    lax.fori_loop(0, depth, soon[2], 0)
    lax.fori_loop(0, depth, later[2], 0)

    def drain(r, carry):
        for copy in store(r):
            copy.wait()
        return carry

    lax.fori_loop(0, rows, drain, 0)


def gather_forward(mesh, lengths, packed, hidden):
    dp, fsdp = mesh.shape["dp"], mesh.shape["fsdp"]
    _, share, _ = packed.shape
    depth = dp // 4
    rows = hidden.shape[0]
    dma = pltpu.SemaphoreType.DMA
    anywhere = pl.BlockSpec(memory_space=pl.ANY)
    inside = pl.BlockSpec(memory_space=pltpu.VMEM)
    kinds = (
        (BF16, SEQ, D),
        (BF16, SEQ, 4 * W),
        (BF16, SEQ, D),
        (F32, SEQ, W),
        (F32, 8 * K, SEQ),
        (F32, 8, SEQ),
        (BF16, SEQ, D),
    )
    sems = [
        dma((2, depth)),
        dma((depth,)),
        dma((depth,)),
        dma((depth,)),
        dma((depth,)),
        dma((depth,)),
        dma((2, depth)),
        dma((2, depth)),
        dma((4, depth)),
        dma((4, depth)),
    ]
    outs = pl.pallas_call(
        functools.partial(gather_forward_kernel, depth),
        out_shape=(
            jax.ShapeDtypeStruct((BLOCKS, depth, 2, 2, 2, share, W), BF16),
            jax.ShapeDtypeStruct((16, D), F32),
            jax.ShapeDtypeStruct((8 * K, W), BF16),
            jax.ShapeDtypeStruct((8, D), F32),
        )
        + tuple(jax.ShapeDtypeStruct((rows, a, b), kind) for kind, a, b in kinds),
        in_specs=[pl.BlockSpec(memory_space=pltpu.SMEM), inside, anywhere],
        out_specs=(anywhere, inside, inside, inside) + (anywhere,) * 7,
        scratch_shapes=[pltpu.VMEM((rows, SEQ, D), BF16)]
        + [pltpu.VMEM((rows, a, b), kind) for kind, a, b in kinds]
        + [
            pltpu.VMEM((4, depth, 2, 2, 2, share, W), BF16),
            pltpu.VMEM((1, depth, 2, 2, 2, share, W), BF16),
            pltpu.VMEM((1, depth, 2, 2, 2, share, W), BF16),
            pltpu.VMEM((D, 128), F32),
            pltpu.VMEM((SEQ + 2 * PAD, D), F32),
            pltpu.VMEM((SEQ + 2 * PAD, W), F32),
            pltpu.VMEM((128, SEQ), F32),
            dma(()),
            dma((4,)),
            dma((7, rows)),
        ]
        + sems
        + sems,
        compiler_params=pltpu.CompilerParams(
            collective_id=0, has_side_effects=True, vmem_limit_bytes=56 * 1024 * 1024
        ),
        name="gather_forward",
    )(lengths, packed, hidden)
    return (outs[0].reshape(BLOCKS, D, W),) + tuple(outs[1:])


def backward_scatter_kernel(
    depth,
    len_ref,
    x_hbm,
    proj_hbm,
    dl_hbm,
    kc_hbm,
    wt_hbm,
    lse_hbm,
    gctx_hbm,
    gr1_hbm,
    full_hbm,
    depth_ref,
    kmt_ref,
    ctx_hbm,
    gmix_hbm,
    act_hbm,
    gffn_hbm,
    gpre_hbm,
    fb_hbm,
    stat_ref,
    gin_ref,
    o_ref,
    u_ref,
    x_ref,
    proj_ref,
    dl_ref,
    kc_ref,
    wt_ref,
    lse_ref,
    gctx_ref,
    gr1_ref,
    win_ref,
    wpt_ref,
    gproj_ref,
    gkc_ref,
    gkm,
    gdk,
    small,
    sv,
    gc,
    xs,
    gd,
    gs,
    gq,
    gt,
    dqt,
    left,
    right,
    part,
    rc,
    r1,
    r2,
    ru,
    rd,
    tiny,
    got,
    in_sem,
    left_sem,
    right_sem,
    cs,
    cr,
    s1,
    q1,
    s2,
    q2,
    us,
    ur,
    ds,
    dr,
    ts,
    tr,
):
    dp, z, x, core, y = place()
    c_dev, x_dev, y_dev = partners(dp, x, core, y)
    up_dev, down_dev = (dp + 4, y), (dp - 4, y)
    last = BLOCKS - 1
    rows = x_ref.shape[0]
    early = 5 * rows

    def fetch(t, act):
        def both(a, b):
            slot = t % 2
            for copy in (
                pltpu.make_async_copy(a, left.at[slot], left_sem.at[slot]),
                pltpu.make_async_copy(b, right.at[slot], right_sem.at[slot]),
            ):
                act(copy)

        @pl.when(t < 4)
        def _():
            both(act_hbm.at[t], gffn_hbm.at[t // 2])

        @pl.when((t >= 4) & (t < 8))
        def _():
            both(gpre_hbm.at[t - 4], fb_hbm.at[(t - 4) // 2])

        @pl.when((t >= 8) & (t < 10))
        def _():
            both(ctx_hbm, gmix_hbm.at[t - 8])

        @pl.when((t >= 10) & (t < 14))
        def _():
            both(x_hbm, gproj_ref.at[:, t - 10])

        @pl.when(t == 14)
        def _():
            both(dl_hbm, gkc_ref)

    def c_copy(t):
        return send(part.at[t, :, :, 1 - core], rc.at[t], cs.at[t], cr.at[t], c_dev)

    def first_copy(t, by_y):
        if by_y:
            return send(part.at[t, :, :, core, 1 - y], r1.at[t], s1.at[t], q1.at[t], y_dev)
        return send(part.at[t, :, 1 - x, core], r1.at[t], s1.at[t], q1.at[t], x_dev)

    def second_copy(t, by_y):
        if by_y:
            return send(part.at[t, :, 1 - x, core, y], r2.at[t], s2.at[t], q2.at[t], x_dev)
        return send(part.at[t, :, x, core, 1 - y], r2.at[t], s2.at[t], q2.at[t], y_dev)

    def up_copy(t, bottom):
        source = part.at[t, :, x, core, y] if bottom else ru.at[t]
        return send(source, ru.at[t], us.at[t], ur.at[t], up_dev)

    def down_copy(t, top):
        source = part.at[t, :, x, core, y] if top else rd.at[t]
        return send(source, rd.at[t], ds.at[t], dr.at[t], down_dev)

    def t_copy(k):
        return send(tiny.at[k], got.at[k], ts.at[k], tr.at[k], (c_dev, x_dev, y_dev)[k])

    def t_line(d, way):
        return send(
            tiny.at[3],
            got.at[3 + z],
            ts.at[2 + d if way > 0 else 1 + depth + d],
            tr.at[3 + z],
            (dp + 4 * d * way, y),
        )

    def t_arrival(level):
        return send(tiny.at[3], got.at[3 + level], ts.at[0], tr.at[3 + level], c_dev)

    def add(into, other):
        return (into.astype(F32) + other.astype(F32)).astype(BF16)

    def parity(t, work):
        @pl.when(t % 2 == 0)
        def _():
            work(True)

        @pl.when(t % 2 == 1)
        def _():
            work(False)


    def inside_of(r):
        return lax.broadcasted_iota(jnp.int32, (SEQ, 1), 0) < len_ref[r]

    def piece_span(r):
        sv[PAD : PAD + SEQ] = proj_ref[r, :, 3 * W :].astype(F32)
        gc[PAD : PAD + SEQ] = gctx_ref[r, :, W:].astype(F32)
        xs[PAD : PAD + SEQ] = x_ref[r].astype(F32)

        e16 = spread(16)
        place_row = lax.broadcasted_iota(jnp.int32, (W, 128), 0) // HD
        place_col = lax.broadcasted_iota(jnp.int32, (W, 128), 1)
        both = []
        for k in range(K):
            weight = pltpu.roll(wt_ref[r, k * 8 : k * 8 + 8], (k - K // 2) % SEQ, 1)
            high = weight.astype(BF16).astype(F32)
            both.append(jnp.concatenate([high, weight - high], axis=0).astype(BF16))
        for n in range(4):
            rows = slice(n * 128, (n + 1) * 128)
            spans = jnp.zeros((128, 128), F32)
            total = jnp.zeros((128, W), F32)
            for k in range(K):
                start = PAD + n * 128 + k - K // 2
                product_k = gc[PAD + n * 128 : PAD + (n + 1) * 128] * sv[start : start + 128]
                chosen = (place_col == place_row + 8 * k).astype(F32).astype(BF16)
                spans = spans + nn(product_k.astype(BF16), chosen)
                start = PAD + n * 128 - k + K // 2
                total = total + tn(both[k][:, rows], e16) * gc[start : start + 128]
            gt[:, rows] = spans.T
            gproj_ref[r, 3, rows] = total.astype(BF16)

    def piece_logits(r):
        center = jnp.zeros((8, SEQ), F32)
        for k in range(K):
            center = center + wt_ref[r, k * 8 : k * 8 + 8] * gt[k * 8 : k * 8 + 8]
        glt = jnp.concatenate(
            [
                wt_ref[r, k * 8 : k * 8 + 8] * (gt[k * 8 : k * 8 + 8] - center)
                for k in range(K)
            ],
            axis=0,
        ).astype(BF16)
        query = proj_ref[r, :, 0:W].astype(F32)
        mk = (kc_ref[r] * query).astype(BF16)
        gkm[...] += nn(glt, mk)
        mixed = tn(glt, kmt_ref[...])
        gkc_ref[r] = (mixed * query).astype(BF16)
        gq[...] = mixed * kc_ref[r]
        gd[PAD : PAD + SEQ] = nt(gkc_ref[r], wpt_ref[0])


    def piece_columns(r):
        def column(c, carry):
            lane = pl.ds(pl.multiple_of(c * 128, 128), 128)
            sums = [jnp.zeros((8, 128), F32)] * K
            for n in range(8):
                total = jnp.zeros((64, 128), F32)
                center = PAD + n * 64
                grad = gd[center : center + 64, lane]
                for k in range(K):
                    start = center + k - K // 2
                    sums[k] = sums[k] + jnp.sum(
                        (xs[start : start + 64, lane] * grad).reshape(8, 8, 128), axis=0
                    )
                    start = center - k + K // 2
                    total = total + gd[start : start + 64, lane] * depth_ref[k : k + 1, lane]
                gs[n * 64 : (n + 1) * 64, lane] = total
            for k in range(K):
                gdk[k, :, lane] = gdk[k, :, lane] + sums[k]
            return carry

        lax.fori_loop(0, D // 128, column, 0)


    def piece_pairs(r, first, stop):
        inside = inside_of(r)
        lane_head = lax.broadcasted_iota(jnp.int32, (1, 128), 1) // HD
        bias = jnp.where(inside, 0.0, -1e30).astype(F32)

        def pair(p, carry):
            def lanes(part):
                return pl.ds(pl.multiple_of(part * W + p * 128, 128), 128)

            q2, k2, v2 = (proj_ref[r, :, lanes(part)] for part in range(3))
            g2 = gctx_ref[r, :, lanes(0)]
            results = []
            for h in range(2):
                mine = lane_head == h
                scale = jnp.where(mine, 1.0 / math.sqrt(HD), 0.0).astype(BF16)
                scores = nt(k2, q2 * scale) + bias
                probs = jnp.exp(scores - lse_ref[r, pl.ds(p * 2 + h, 1)])
                grads = nt(v2 * jnp.where(mine, 1.0, 0.0).astype(BF16), g2)
                correction = jnp.sum(probs * grads, axis=0, keepdims=True)
                grad_scores = (probs * (grads - correction)).astype(BF16)
                dqt[h * HD : (h + 1) * HD] = tn(k2, grad_scores)[h * HD : (h + 1) * HD]
                results.append((nn(grad_scores, q2), nn(probs.astype(BF16), g2)))
            low = lane_head == 0
            scale = 1.0 / math.sqrt(HD)
            gproj_ref[r, 0, :, lanes(0)] = (dqt[...].T * scale + gq[:, lanes(0)]).astype(BF16)
            gproj_ref[r, 1, :, lanes(0)] = (jnp.where(low, results[0][0], results[1][0]) * scale).astype(BF16)
            gproj_ref[r, 2, :, lanes(0)] = jnp.where(low, results[0][1], results[1][1]).astype(BF16)
            return carry

        lax.fori_loop(first, stop, pair, 0)


    def piece_inputs(r):
        inside = inside_of(r)
        for b in range(4):
            gs[...] += nt(gproj_ref[r, b], win_ref[b])
        gin_ref[r] = jnp.where(inside, gr1_ref[r] + gs[...], 0.0).astype(BF16)


    def chosen(height, rule):
        row = lax.broadcasted_iota(jnp.int32, (height, 128), 0)
        lane = lax.broadcasted_iota(jnp.int32, (height, 128), 1)
        return rule(row, lane).astype(F32).astype(BF16)

    def gather_small():
        taps = jnp.concatenate(
            [jnp.sum(gdk[...], axis=1), jnp.zeros((16 - K, D), F32), jnp.sum(stat_ref[...], axis=1)]
        ).astype(BF16)
        pick = chosen(
            24,
            lambda row, lane: ((row < K) & (lane == row)) | ((row >= 20) & (lane == row - 20 + 4 * K)),
        )
        both = tn(taps, pick)
        low = gkm[...].astype(BF16)
        small[...] = both
        for odd in range(2):
            pick = chosen(
                8 * K,
                lambda row, lane: (row % 8 >= 3 * odd)
                & (row % 8 < 3 * odd + 3)
                & (lane == K + row // 8 * 3 + row % 8 - 3 * odd),
            )
            half = pl.ds(odd, W, stride=2)
            small[half] = small[half] + tn(low, pick)

    loads = (
        (x_hbm, x_ref),
        (proj_hbm, proj_ref),
        (dl_hbm, dl_ref),
        (kc_hbm, kc_ref),
        (wt_hbm, wt_ref),
        (lse_hbm, lse_ref),
        (gctx_hbm, gctx_ref),
        (gr1_hbm, gr1_ref),
        (full_hbm.at[pl.ds(10, 4)], win_ref),
        (full_hbm.at[pl.ds(14, 1)], wpt_ref),
    )
    inputs = [
        pltpu.make_async_copy(source, target, in_sem.at[i])
        for i, (source, target) in enumerate(loads)
    ]
    fetch(0, lambda copy: copy.start())
    for copy in inputs:
        copy.start()
    gkm[...] = jnp.zeros_like(gkm)
    gdk[...] = jnp.zeros_like(gdk)
    for ref, width in ((sv, W), (gc, W), (xs, D), (gd, D)):
        ref[0:PAD] = jnp.zeros((PAD, width), F32)
        ref[PAD + SEQ :] = jnp.zeros((PAD, width), F32)
    lines = tuple((z >= d, (dp - 4 * d, y)) for d in range(1, depth)) + tuple(
        (z + d < depth, (dp + 4 * d, y)) for d in range(1, depth)
    )
    meet((c_dev, x_dev, y_dev), lines)
    lane = lax.broadcasted_iota(jnp.int32, (8, 128), 1)
    mine = jnp.zeros((8, 128), F32)
    for k in range(4):
        mine = jnp.where(lane == k, jnp.sum(stat_ref[k]), mine)
    count = len_ref[0]
    for r in range(1, rows):
        count = count + len_ref[r]
    tiny[0] = jnp.where(lane == 4, count.astype(F32), mine)
    t_copy(0).start()

    def multiply(t):
        @pl.when(t == early)
        def _():
            fetch(t, lambda copy: copy.start())

        @pl.when((t + 1 < last) & (t + 1 != early))
        def _():
            fetch(t + 1, lambda copy: copy.start())

        @pl.when(t < last)
        def _():
            fetch(t, lambda copy: copy.wait())
            slot = t % 2
            for c in range(2):
                a = left[slot, :, :, c * W : (c + 1) * W].reshape(rows * SEQ, W)
                block = tn(a, right[slot].reshape(rows * SEQ, W))
                half = depth // 2
                part[t, c * half : (c + 1) * half] = block.reshape(
                    (half,) + part.shape[2:]
                ).astype(BF16)

        @pl.when(t == last)
        def _():
            gather_small()
            filled = jnp.concatenate([small[...], jnp.zeros((D, W - 128), F32)], axis=1)
            part[t] = filled.reshape(part.shape[1:]).astype(BF16)

        c_copy(t).start()

    def stage_core(t):
        c_copy(t).wait_recv()

        def level(j, carry):
            part[t, j, :, core] = add(part[t, j, :, core], rc[t, j])
            return carry

        lax.fori_loop(0, depth, level, 0)
        parity(t, lambda by_y: first_copy(t, by_y).start())

    def stage_first(t):
        def work(by_y):
            first_copy(t, by_y).wait_recv()
            if by_y:
                part[t, :, :, core, y] = add(part[t, :, :, core, y], r1[t])
            else:
                part[t, :, x, core] = add(part[t, :, x, core], r1[t])
            second_copy(t, by_y).start()

        parity(t, work)

    def stage_second(t):
        parity(t, lambda by_y: second_copy(t, by_y).wait_recv())
        part[t, :, x, core, y] = add(part[t, :, x, core, y], r2[t])
        o_ref[t] = part[t, z, x, core, y].astype(F32)

    def stage_up(t):
        @pl.when(z == 0)
        def _():
            up_copy(t, True).start()

        @pl.when(z > 0)
        def _():
            up_copy(t, False).wait_recv()
            o_ref[t] = o_ref[t] + ru[t, z].astype(F32)

        @pl.when((z > 0) & (z + 1 < depth))
        def _():
            ru[t] = add(ru[t], part[t, :, x, core, y])
            up_copy(t, False).start()

    def stage_down(t):
        @pl.when(z + 1 == depth)
        def _():
            down_copy(t, True).start()

        @pl.when(z + 1 < depth)
        def _():
            down_copy(t, False).wait_recv()
            o_ref[t] = o_ref[t] + rd[t, z].astype(F32)

        @pl.when((z > 0) & (z + 1 < depth))
        def _():
            rd[t] = add(rd[t], part[t, :, x, core, y])
            down_copy(t, False).start()

    def stage(t, work):
        @pl.when((t >= 0) & (t < BLOCKS))
        def _():
            work(t)

    def sums(t):
        for k in range(3):

            @pl.when(t == 3 * k + 3)
            def _():
                t_copy(k).wait_recv()
                tiny[k + 1] = tiny[k] + got[k]
                if k < 2:
                    t_copy(k + 1).start()

        @pl.when(t == 10)
        def _():
            for d in range(1, depth):

                @pl.when(z + d < depth)
                def _():
                    t_line(d, 1).start()

                @pl.when(z >= d)
                def _():
                    t_line(d, -1).start()

    def tick(t, carry):
        stage(t, multiply)
        stage(t - 1, stage_core)
        stage(t - 3, stage_first)
        stage(t - 5, stage_second)
        stage(t - 5 - z, stage_up)
        stage(t - 5 - (depth - 1 - z), stage_down)
        sums(t)
        row = t // 5

        def when(i, work):
            @pl.when((t < early) & (t % 5 == i))
            def _():
                work()

        @pl.when(t == 0)
        def _():
            for copy in inputs:
                copy.wait()

        when(0, lambda: piece_span(row))
        when(1, lambda: piece_logits(row))
        when(2, lambda: piece_columns(row))
        when(3, lambda: piece_pairs(row, 0, 2))

        def close():
            piece_pairs(row, 2, 3)
            piece_inputs(row)

        when(4, close)
        return carry

    lax.fori_loop(0, BLOCKS + 5 + depth, tick, 0)

    for level in range(depth):

        @pl.when(z == level)
        def _():
            got[3 + level] = tiny[3]

        @pl.when(z != level)
        def _():
            t_arrival(level).wait_recv()

    total = got[3]
    for level in range(1, depth):
        total = total + got[3 + level]
    u_ref[...] = total

    for d in range(1, depth):

        @pl.when(z + d < depth)
        def _():
            t_line(d, 1).wait_send()

        @pl.when(z >= d)
        def _():
            t_line(d, -1).wait_send()

    for k in range(3):
        t_copy(k).wait_send()

    def finish(t, carry):
        c_copy(t).wait_send()
        parity(t, lambda by_y: first_copy(t, by_y).wait_send())
        parity(t, lambda by_y: second_copy(t, by_y).wait_send())

        @pl.when(z + 1 < depth)
        def _():
            up_copy(t, False).wait_send()

        @pl.when(z > 0)
        def _():
            down_copy(t, False).wait_send()

        return carry

    lax.fori_loop(0, BLOCKS, finish, 0)


def backward_scatter(mesh, lengths, x, proj, dl, kc, wt, lse, gctx, gr1, full, depth_kernel, kmt, ctx, gmix, act, gffn, gpre, fb, stat):
    dp, fsdp = mesh.shape["dp"], mesh.shape["fsdp"]
    share = D // (dp * fsdp)
    depth = dp // 4
    rows = x.shape[0]
    dma = pltpu.SemaphoreType.DMA
    anywhere = pl.BlockSpec(memory_space=pl.ANY)
    inside = pl.BlockSpec(memory_space=pltpu.VMEM)

    def by_row(values):
        return values.reshape(values.shape[:-2] + (rows, SEQ, values.shape[-1]))

    return pl.pallas_call(
        functools.partial(backward_scatter_kernel, depth),
        out_shape=(
            jax.ShapeDtypeStruct((rows, SEQ, D), BF16),
            jax.ShapeDtypeStruct((BLOCKS, share, W), F32),
            jax.ShapeDtypeStruct((8, 128), F32),
        ),
        in_specs=[pl.BlockSpec(memory_space=pltpu.SMEM)]
        + [anywhere] * 9
        + [inside] * 2
        + [anywhere] * 6
        + [inside],
        out_specs=(inside, inside, inside),
        scratch_shapes=[
            pltpu.VMEM((rows, SEQ, D), BF16),
            pltpu.VMEM((rows, SEQ, 4 * W), BF16),
            pltpu.VMEM((rows, SEQ, D), BF16),
            pltpu.VMEM((rows, SEQ, W), F32),
            pltpu.VMEM((rows, 8 * K, SEQ), F32),
            pltpu.VMEM((rows, 8, SEQ), F32),
            pltpu.VMEM((rows, SEQ, D), BF16),
            pltpu.VMEM((rows, SEQ, D), F32),
            pltpu.VMEM((4, D, W), BF16),
            pltpu.VMEM((1, D, W), BF16),
            pltpu.VMEM((rows, 4, SEQ, W), BF16),
            pltpu.VMEM((rows, SEQ, W), BF16),
            pltpu.VMEM((8 * K, W), F32),
            pltpu.VMEM((K, 8, D), F32),
            pltpu.VMEM((D, 128), F32),
            pltpu.VMEM((SEQ + 2 * PAD, W), F32),
            pltpu.VMEM((SEQ + 2 * PAD, W), F32),
            pltpu.VMEM((SEQ + 2 * PAD, D), F32),
            pltpu.VMEM((SEQ + 2 * PAD, D), F32),
            pltpu.VMEM((SEQ, D), F32),
            pltpu.VMEM((SEQ, W), F32),
            pltpu.VMEM((128, SEQ), F32),
            pltpu.VMEM((128, SEQ), F32),
            pltpu.VMEM((2, rows, SEQ, D), BF16),
            pltpu.VMEM((2, rows, SEQ, W), BF16),
            pltpu.VMEM((BLOCKS, depth, 2, 2, 2, share, W), BF16),
            pltpu.VMEM((BLOCKS, depth, 2, 2, share, W), BF16),
            pltpu.VMEM((BLOCKS, depth, 2, share, W), BF16),
            pltpu.VMEM((BLOCKS, depth, share, W), BF16),
            pltpu.VMEM((BLOCKS, depth, share, W), BF16),
            pltpu.VMEM((BLOCKS, depth, share, W), BF16),
            pltpu.VMEM((4, 8, 128), F32),
            pltpu.VMEM((3 + depth, 8, 128), F32),
            dma((10,)),
            dma((2,)),
            dma((2,)),
        ]
        + [dma((BLOCKS,))] * 10
        + [dma((1 + 2 * depth,)), dma((3 + depth,))],
        compiler_params=pltpu.CompilerParams(
            collective_id=1, has_side_effects=True, vmem_limit_bytes=67_000_000
        ),
        name="backward_scatter",
    )(
        lengths,
        x,
        proj,
        dl,
        kc,
        wt,
        lse,
        gctx,
        gr1,
        full,
        depth_kernel,
        kmt,
        ctx,
        by_row(gmix),
        by_row(act),
        by_row(gffn),
        by_row(gpre),
        by_row(fb),
        stat,
    )


def body(
    mesh,
    hidden,
    lengths,
    in_weight,
    depth_kernel,
    point_weight,
    kernel_weight,
    out_weight,
    up_weight,
    down_weight,
    norm_gains,
    norm_biases,
    out_grad,
):
    packed = pack(
            in_weight,
            depth_kernel,
            point_weight,
            kernel_weight,
            out_weight,
            up_weight,
            down_weight,
            norm_gains,
            norm_biases,
    )
    output, input_grad, shard, totals = layer(mesh, hidden, lengths, packed, out_grad)
    rms = jnp.sqrt(totals[0, :4] / (totals[0, 4] * D))
    return (output, input_grad) + unpack(shard) + (rms,)


def solution(mesh):
    in_specs = (
        P(("dp", "fsdp"), None, None),
        P(("dp", "fsdp")),
        P(("dp", "fsdp"), None),
        P(None, ("dp", "fsdp")),
        P(("dp", "fsdp"), None),
        P(None, ("dp", "fsdp")),
        P(("dp", "fsdp"), None),
        P(None, None, ("dp", "fsdp")),
        P(None, ("dp", "fsdp"), None),
        P(None, ("dp", "fsdp")),
        P(None, ("dp", "fsdp")),
        P(("dp", "fsdp"), None, None),
    )
    out_specs = (
        P(("dp", "fsdp"), None, None),
        P(("dp", "fsdp"), None, None),
        P(("dp", "fsdp"), None),
        P(None, ("dp", "fsdp")),
        P(("dp", "fsdp"), None),
        P(None, ("dp", "fsdp")),
        P(("dp", "fsdp"), None),
        P(None, None, ("dp", "fsdp")),
        P(None, ("dp", "fsdp"), None),
        P(None, ("dp", "fsdp")),
        P(None, ("dp", "fsdp")),
        P(),
    )
    return jax.shard_map(functools.partial(body, mesh), mesh=mesh, in_specs=in_specs, out_specs=out_specs, check_vma=False)
```
